16 devices in a mesh: dp: 4 (over z, y), tp: 4 (over x, core).
Axes of the slice: x: 2, y: 2, z: 2, core: 2. Of those that a mesh axis runs over, the one named last changes fastest.
Arguments:
- tokens: bfloat16 [8, 128, 5120], P('dp'), parts along dimension 0
- seq_lens: int32 [8], P('dp'), parts along dimension 0
- w_q: bfloat16 [5120, 5120], P(None, 'tp')
- w_k: bfloat16 [5120, 5120], P(None, 'tp')
- w_v: bfloat16 [5120, 5120], P(None, 'tp')
- w_o: bfloat16 [5120, 5120], P('tp')
- g_q: bfloat16 [5120], P('tp')
- g_k: bfloat16 [5120], P('tp')
- g_attn: bfloat16 [5120], replicated
- g_mlp: bfloat16 [5120], replicated
- w_gate: bfloat16 [5120, 13824], P(None, 'tp')
- w_up: bfloat16 [5120, 13824], P(None, 'tp')
- w_down: bfloat16 [13824, 5120], P('tp')
Outputs:
- output 1: bfloat16 [8, 128, 5120], P('dp'), parts along dimension 0
- output 2: bfloat16 [8, 40, 128, 128], P('dp', 'tp'), parts along dimension 0
- output 3: bfloat16 [8, 40, 128, 128], P('dp', 'tp'), parts along dimension 0
There are 4 independent parts. The reference program is written for one: setup_inputs(seed, part) draws one part's arguments, and reference() takes and returns one part's arrays. A program takes and returns all parts, laid end to end along the dimension named above; an argument that names none is the same for every part.
All inputs are finite; a program needn't handle non-finite values.
Results may differ from the reference program's by a relative error of at most 0.0163826.
Values are sent between devices in bfloat16 or wider.
A program may use at most 1 GiB of HBM per device.

```python
import jax
import jax.numpy as jnp
from jax import lax

PROMPTS = 2
SEQ_LEN = 128
D_MODEL = 5120
Q_HEADS = 40
KV_HEADS = 40
HEAD_DIM = 128
FF_DIM = 13824

ROPE_BASE = 500000.0
NORM_EPS = 1e-6


def setup_inputs(seed: int = 0, part: int = 0) -> dict:
    part_key = jax.random.fold_in(jax.random.key(seed), part)
    key_tok, key_len, key_slot = jax.random.split(part_key, 3)
    weight_keys = jax.random.split(jax.random.key(seed + 1), 13)
    q_width = Q_HEADS * HEAD_DIM
    kv_width = KV_HEADS * HEAD_DIM
    in_scale = D_MODEL ** -0.5
    tokens = jax.random.normal(key_tok, (PROMPTS, SEQ_LEN, D_MODEL), jnp.float32)
    seq_lens = jax.random.randint(key_len, (PROMPTS,), SEQ_LEN // 8, SEQ_LEN + 1, jnp.int32)
    full_slot = jax.random.randint(key_slot, (), 0, PROMPTS, jnp.int32)
    seq_lens = jnp.where(jnp.arange(PROMPTS) == full_slot, SEQ_LEN, seq_lens).astype(jnp.int32)
    q_head_scale = 2.0 ** jax.random.uniform(weight_keys[0], (Q_HEADS, 1), jnp.float32, -1.0, 1.0)
    k_head_scale = 2.0 ** jax.random.uniform(weight_keys[1], (KV_HEADS, 1), jnp.float32, -1.0, 1.0)
    w_q = (jax.random.normal(weight_keys[2], (D_MODEL, Q_HEADS, HEAD_DIM), jnp.float32) * q_head_scale * in_scale).reshape(D_MODEL, q_width)
    w_k = (jax.random.normal(weight_keys[3], (D_MODEL, KV_HEADS, HEAD_DIM), jnp.float32) * k_head_scale * in_scale).reshape(D_MODEL, kv_width)
    w_v = jax.random.normal(weight_keys[4], (D_MODEL, kv_width), jnp.float32) * in_scale
    w_o = jax.random.normal(weight_keys[5], (q_width, D_MODEL), jnp.float32) * q_width ** -0.5
    g_q = jax.random.uniform(weight_keys[6], (q_width,), jnp.float32, 0.5, 1.5)
    g_k = jax.random.uniform(weight_keys[7], (kv_width,), jnp.float32, 0.5, 1.5)
    g_attn = jax.random.uniform(weight_keys[8], (D_MODEL,), jnp.float32, 0.5, 1.5)
    g_mlp = jax.random.uniform(weight_keys[9], (D_MODEL,), jnp.float32, 0.5, 1.5)
    w_gate = jax.random.normal(weight_keys[10], (D_MODEL, FF_DIM), jnp.float32) * in_scale
    w_up = jax.random.normal(weight_keys[11], (D_MODEL, FF_DIM), jnp.float32) * in_scale
    w_down = jax.random.normal(weight_keys[12], (FF_DIM, D_MODEL), jnp.float32) * FF_DIM ** -0.5
    return dict(tokens=tokens.astype(jnp.bfloat16), seq_lens=seq_lens, w_q=w_q.astype(jnp.bfloat16), w_k=w_k.astype(jnp.bfloat16), w_v=w_v.astype(jnp.bfloat16), w_o=w_o.astype(jnp.bfloat16), g_q=g_q.astype(jnp.bfloat16), g_k=g_k.astype(jnp.bfloat16), g_attn=g_attn.astype(jnp.bfloat16), g_mlp=g_mlp.astype(jnp.bfloat16), w_gate=w_gate.astype(jnp.bfloat16), w_up=w_up.astype(jnp.bfloat16), w_down=w_down.astype(jnp.bfloat16))


def rope_tables(seq_len, head_dim):
    half_dim = head_dim // 2
    inv_freq = ROPE_BASE ** (-2.0 * jnp.arange(half_dim, dtype=jnp.float32) / head_dim)
    angles = jnp.arange(seq_len, dtype=jnp.float32)[:, None] * inv_freq[None, :]
    angles = jnp.concatenate([angles, angles], axis=-1)
    return jnp.cos(angles), jnp.sin(angles)


def apply_rope(vecs, cos_tab, sin_tab, head_axes):
    half_dim = vecs.shape[-1] // 2
    table_shape = (cos_tab.shape[0],) + (1,) * head_axes + (cos_tab.shape[1],)
    rotated = jnp.concatenate([-vecs[..., half_dim:], vecs[..., :half_dim]], axis=-1)
    return vecs * cos_tab.reshape(table_shape) + rotated * sin_tab.reshape(table_shape)


def rms_scale(vals):
    return lax.rsqrt(jnp.mean(vals * vals, axis=-1, keepdims=True) + NORM_EPS)


def post_norm(base, branch, gain):
    branch32 = branch.astype(jnp.float32)
    return (base.astype(jnp.float32) + branch32 * rms_scale(branch32) * gain.astype(jnp.float32)).astype(jnp.bfloat16)


def reference(tokens, seq_lens, w_q, w_k, w_v, w_o, g_q, g_k, g_attn, g_mlp, w_gate, w_up, w_down):
    group_size = Q_HEADS // KV_HEADS
    cos_tab, sin_tab = rope_tables(SEQ_LEN, HEAD_DIM)
    positions = jnp.arange(SEQ_LEN)
    causal = positions[None, :] <= positions[:, None]

    def one_prompt(item):
        prompt, length = item
        q_raw = jnp.dot(prompt, w_q, preferred_element_type=jnp.float32)
        k_raw = jnp.dot(prompt, w_k, preferred_element_type=jnp.float32)
        v_new = jnp.dot(prompt, w_v, preferred_element_type=jnp.float32).astype(jnp.bfloat16)
        q_norm = q_raw * rms_scale(q_raw) * g_q.astype(jnp.float32)
        k_norm = k_raw * rms_scale(k_raw) * g_k.astype(jnp.float32)
        queries = apply_rope(q_norm.reshape(SEQ_LEN, KV_HEADS, group_size, HEAD_DIM), cos_tab, sin_tab, 2).astype(jnp.bfloat16)
        keys_new = apply_rope(k_norm.reshape(SEQ_LEN, KV_HEADS, HEAD_DIM), cos_tab, sin_tab, 1).astype(jnp.bfloat16)
        v_heads = v_new.reshape(SEQ_LEN, KV_HEADS, HEAD_DIM)
        scores = jnp.einsum('sgrd,tgd->grst', queries.astype(jnp.float32), keys_new.astype(jnp.float32)) * HEAD_DIM ** -0.5
        allowed = causal & (positions[None, :] < length)
        scores = jnp.where(allowed, scores, -1e30)
        attn_probs = jax.nn.softmax(scores, axis=-1).astype(jnp.bfloat16)
        attn_out = jnp.einsum('grst,tgd->sgrd', attn_probs.astype(jnp.float32), v_heads.astype(jnp.float32)).astype(jnp.bfloat16)
        attn_proj = jnp.dot(attn_out.reshape(SEQ_LEN, Q_HEADS * HEAD_DIM), w_o, preferred_element_type=jnp.float32).astype(jnp.bfloat16)
        hidden = post_norm(prompt, attn_proj, g_attn)
        gate_pre = jnp.dot(hidden, w_gate, preferred_element_type=jnp.float32)
        up_proj = jnp.dot(hidden, w_up, preferred_element_type=jnp.float32)
        act_out = (jax.nn.silu(gate_pre) * up_proj).astype(jnp.bfloat16)
        mlp_out = jnp.dot(act_out, w_down, preferred_element_type=jnp.float32).astype(jnp.bfloat16)
        new_hidden = post_norm(hidden, mlp_out, g_mlp)
        return new_hidden, jnp.transpose(keys_new, (1, 0, 2)), jnp.transpose(v_heads, (1, 0, 2))

    out_hidden, k_cache, v_cache = lax.map(one_prompt, (tokens, seq_lens))
    return out_hidden, k_cache, v_cache
```

```python
import functools

import numpy as np
import jax
import jax.numpy as jnp
from jax import lax
from jax.experimental import pallas as pl
from jax.experimental.pallas import tpu as pltpu
from jax.sharding import PartitionSpec as P

HEAD_DIM = 128
ROPE_BASE = 500000.0
NORM_EPS = 1e-6
SLOTS = 13
F32 = jnp.float32
BF16 = jnp.bfloat16


def rope_tables(seq_len):
    half = HEAD_DIM // 2
    inv_freq = (ROPE_BASE ** (-2.0 * np.arange(half) / HEAD_DIM)).astype(np.float32)
    angles = np.arange(seq_len, dtype=np.float32)[:, None] * inv_freq[None, :]
    cos, sin = np.cos(angles), np.sin(angles)
    return (np.concatenate([cos, cos], -1).astype(np.float32), np.concatenate([-sin, sin], -1).astype(np.float32))


def layer_kernel(seq_ref, cos_ref, sin_ref, gq_ref, gk_ref, ga_ref, gm_ref,
                 x_hbm, wq, wk, wv, wo, wg, wu, wd,
                 y_hbm, kc_hbm, vc_hbm,
                 pool, x, qraw, kraw, kb, vb, o, act, ssq_acc, rsc, ssq_send, ssq_recv,
                 rs_send, rs_recv, xs_send, xs_recv, full,
                 wsem, xsem, csem, ysem, ssq_s, ssq_r, arsem):
    dp = lax.axis_index("dp")
    t = lax.axis_index("tp")
    core = lax.rem(t, 2)
    sib = t + 1 - 2 * core
    xpeer = lax.rem(t + 2, 4)
    diag = 3 - t
    width = 5120

    B_V, B_O, B_G, B_D, B_END = 10, 15, 20, 47, 67

    def half_col(step, per):
        return lax.rem(step, per) + per * lax.rem(step // per + 1 + core, 2)

    def cols(start, size):
        return pl.ds(pl.multiple_of(start, size), size)

    def issue(n, lo, hi):
        slot = lax.rem(n, SLOTS)
        sem = wsem.at[slot]

        def copy(src, dst):
            pltpu.make_async_copy(src, dst, sem).start()

        def do_qk():
            @pl.when(lax.rem(n, 2) == 0)
            def _():
                copy(wq.at[:, cols((n // 2) * 256, 256)], pool.at[slot])

            @pl.when(lax.rem(n, 2) == 1)
            def _():
                copy(wk.at[:, cols((n // 2) * 256, 256)], pool.at[slot])

        def do_v():
            copy(wv.at[:, cols((n - B_V) * 256, 256)], pool.at[slot])

        def do_o():
            for k in range(4):
                step = 2 * (n - B_O) + k // 2
                copy(wo.at[:, cols(half_col(step, 5) * 512 + (k % 2) * 256, 256)], pool.at[slot, pl.ds(k * 1280, 1280), :])

        def do_g():
            r = n - B_G

            @pl.when(jnp.logical_and(lax.rem(r, 2) == 0, r < 26))
            def _():
                copy(wg.at[:, cols((r // 2) * 256, 256)], pool.at[slot])

            @pl.when(lax.rem(r, 2) == 1)
            def _():
                copy(wu.at[:, cols((r // 2) * 256, 256)], pool.at[slot])

            @pl.when(r == 26)
            def _():
                copy(wg.at[:, pl.ds(3328, 128)], pool.at[slot, :, pl.ds(0, 128)])
                copy(wu.at[:, pl.ds(3328, 128)], pool.at[slot, :, pl.ds(128, 128)])

        def do_d():
            copy(wd.at[:, cols(half_col(n - B_D, 10) * 256, 256)], pool.at[slot, pl.ds(0, 3456), :])

        for start, end, fn in ((0, B_V, do_qk), (B_V, B_O, do_v), (B_O, B_G, do_o), (B_G, B_D, do_g), (B_D, B_END, do_d)):
            if hi < start or lo >= end:
                continue
            if lo >= start and hi < end:
                fn()
            else:
                pl.when(jnp.logical_and(n >= start, n < end))(fn)

    def wait_chunk(n, rows=5120):
        slot = lax.rem(n, SLOTS)
        src = wq if rows == 5120 else wd
        pltpu.make_async_copy(src.at[:, pl.ds(0, 256)], pool.at[slot, pl.ds(0, rows), :], wsem.at[slot]).wait()
        return slot

    def dot(a, b):
        return jnp.dot(a, b, preferred_element_type=F32)

    xcopy = pltpu.make_async_copy(x_hbm, x, xsem)
    xcopy.start()
    for n in range(SLOTS):
        issue(jnp.int32(n), n, n)

    barrier = pltpu.get_barrier_semaphore()
    for peer in (sib, xpeer, diag):
        pl.semaphore_signal(barrier, inc=1, device_id={"tp": peer}, device_id_type=pl.DeviceIdType.MESH)
    pl.semaphore_wait(barrier, 3)

    def remote(src, dst, ssem, rsem, peer):
        return pltpu.make_async_remote_copy(src_ref=src, dst_ref=dst, send_sem=ssem, recv_sem=rsem,
                                            device_id={"tp": peer}, device_id_type=pl.DeviceIdType.MESH)

    xcopy.wait()
    ssq_acc[...] = jnp.zeros_like(ssq_acc)

    def qk_step(i, carry):
        n = 2 * i
        s0 = wait_chunk(n)
        s1 = wait_chunk(n + 1)
        q = dot(x[...], pool[s0])
        k = dot(x[...], pool[s1])
        for b in range(2):
            for hh in range(2):
                qraw[b, 2 * i + hh] = q[b * 128:(b + 1) * 128, hh * 128:(hh + 1) * 128]
                kraw[b, 2 * i + hh] = k[b * 128:(b + 1) * 128, hh * 128:(hh + 1) * 128]
        ssq_acc[0] += q[:, :128] * q[:, :128] + q[:, 128:] * q[:, 128:]
        ssq_acc[1] += k[:, :128] * k[:, :128] + k[:, 128:] * k[:, 128:]
        issue(n + SLOTS, SLOTS, SLOTS + 8)
        issue(n + 1 + SLOTS, SLOTS + 1, SLOTS + 9)
        return carry

    lax.fori_loop(0, 5, qk_step, 0)

    for r in range(2):
        ssq_send[r:r + 1, :] = jnp.sum(jnp.transpose(ssq_acc[r]), axis=0, keepdims=True)
    ssq_send[2:8, :] = jnp.zeros((6, 256), F32)
    ssq_copies = [remote(ssq_send, ssq_recv.at[j], ssq_s.at[j], ssq_r.at[j], peer) for j, peer in enumerate((sib, xpeer, diag))]
    for c in ssq_copies:
        c.start()

    for group in ((10, 11), (12, 13), (14,)):
        slots = [wait_chunk(jnp.int32(n)) for n in group]
        vals = [dot(x[...], pool[s]).astype(BF16) for s in slots]
        for n, v in zip(group, vals):
            for b in range(2):
                for hh in range(2):
                    vb[b, 2 * (n - B_V) + hh] = v[b * 128:(b + 1) * 128, hh * 128:(hh + 1) * 128]
        for n in group:
            issue(jnp.int32(n + SLOTS), n + SLOTS, n + SLOTS)
    vcopy = pltpu.make_async_copy(vb, vc_hbm, csem.at[0])
    vcopy.start()

    for c in ssq_copies:
        c.wait()
    total = ssq_send[...] + ssq_recv[0] + ssq_recv[1] + ssq_recv[2]
    scale = lax.rsqrt(total * (1.0 / width) + NORM_EPS)
    for r in range(2):
        rsc[r] = jnp.transpose(jnp.broadcast_to(scale[r:r + 1, :], (128, 256)))

    row = lax.broadcasted_iota(jnp.int32, (128, 128), 0)
    col = lax.broadcasted_iota(jnp.int32, (128, 128), 1)

    def rope(v):
        return (v * cos_ref[...] + pltpu.roll(v, 64, 1) * sin_ref[...]).astype(BF16)

    for b in range(2):
        allowed = jnp.logical_and(col <= row, col < seq_ref[b])

        def attn_step(i, carry, b=b, allowed=allowed):
            for u in range(5):
                h = i * 5 + u
                hs = cols(h * 128, 128)
                q = rope(qraw[b, h] * rsc[0, b * 128:(b + 1) * 128, :] * gq_ref[:, hs])
                k = rope(kraw[b, h] * rsc[1, b * 128:(b + 1) * 128, :] * gk_ref[:, hs])
                kb[b, h] = k
                s = lax.dot_general(q, k, (((1,), (1,)), ((), ())), preferred_element_type=F32) * HEAD_DIM ** -0.5
                s = jnp.where(allowed, s, -1e30)
                e = jnp.exp(s - jnp.max(s, axis=-1, keepdims=True))
                p = (e / jnp.sum(e, axis=-1, keepdims=True)).astype(BF16)
                o[b * 128:(b + 1) * 128, hs] = dot(p, vb[b, h]).astype(BF16)
            return carry

        lax.fori_loop(0, 2, attn_step, 0)
    kcopy = pltpu.make_async_copy(kb, kc_hbm, csem.at[1])
    kcopy.start()

    def rs_copy(p, j):
        return remote(rs_send.at[p, j], rs_recv.at[p, j], arsem.at[p, 0, j], arsem.at[p, 1, j], sib)

    def xs_copy(p, j):
        return remote(xs_send.at[p, j], xs_recv.at[p, j], arsem.at[p, 2, j], arsem.at[p, 3, j], xpeer)

    def ag_copy(p, j, owner):
        blk = full.at[p, owner * 5 + j]
        return remote(blk, blk, arsem.at[p, 4, j], arsem.at[p, 5, j], sib)

    def reduce_columns(p, partial):
        def sib_step(j, carry):
            rs_send[p, j] = partial(j).astype(BF16)
            rs_copy(p, j).start()
            return carry

        lax.fori_loop(0, 5, sib_step, 0)

        def own_step(j, carry):
            val = partial(j + 5)
            rs_copy(p, j).wait()
            xs_send[p, j] = (val + rs_recv[p, j].astype(F32)).astype(BF16)
            xs_copy(p, j).start()
            return carry

        lax.fori_loop(0, 5, own_step, 0)

        def gather_step(j, carry):
            xs_copy(p, j).wait()
            full[p, core * 5 + j] = (xs_send[p, j].astype(F32) + xs_recv[p, j].astype(F32)).astype(BF16)
            ag_copy(p, j, core).start()
            return carry

        lax.fori_loop(0, 5, gather_step, 0)

        def arrive_step(j, carry):
            ag_copy(p, j, core).wait_send()
            ag_copy(p, j, 1 - core).wait_recv()
            return carry

        lax.fori_loop(0, 5, arrive_step, 0)

    def post_norm(p, gain):
        def sq(c, acc):
            v = full[p, c].astype(F32)
            return acc + v[:, :128] * v[:, :128] + v[:, 128:256] * v[:, 128:256] + v[:, 256:384] * v[:, 256:384] + v[:, 384:] * v[:, 384:]

        acc = lax.fori_loop(0, 10, sq, jnp.zeros((256, 128), F32))
        rs = lax.rsqrt(jnp.sum(acc, axis=-1, keepdims=True) * (1.0 / width) + NORM_EPS)

        def apply(c, carry):
            cs = cols(c * 512, 512)
            x[:, cs] = (x[:, cs].astype(F32) + full[p, c].astype(F32) * rs * gain[:, cs]).astype(BF16)
            return carry

        lax.fori_loop(0, 10, apply, 0)

    def o_partial(step):
        n = B_O + step // 2
        slot = lax.rem(n, SLOTS)

        @pl.when(lax.rem(step, 2) == 0)
        def _():
            wait_chunk(n)

        base = lax.rem(step, 2) * 2560
        parts = [dot(o[...], pool[slot, pl.ds(pl.multiple_of(base + k * 1280, 1280), 1280), :]) for k in range(2)]

        @pl.when(lax.rem(step, 2) == 1)
        def _():
            issue(n + SLOTS, B_O + SLOTS, B_O + SLOTS + 4)

        return jnp.concatenate(parts, axis=1)

    reduce_columns(0, o_partial)
    post_norm(0, ga_ref)

    def gu_step(i, carry):
        n = B_G + 2 * i
        s0 = wait_chunk(n)
        s1 = wait_chunk(n + 1)
        g = dot(x[...], pool[s0])
        u = dot(x[...], pool[s1])
        act[:, cols(i * 256, 256)] = (g * jax.nn.sigmoid(g) * u).astype(BF16)
        issue(n + SLOTS, B_G + SLOTS, B_D + SLOTS - 2)
        issue(n + 1 + SLOTS, B_G + 1 + SLOTS, B_D + SLOTS - 2)
        return carry

    lax.fori_loop(0, 13, gu_step, 0)
    s0 = wait_chunk(jnp.int32(B_D - 1))
    gu = dot(x[...], pool[s0])
    act[:, 3328:3456] = (gu[:, :128] * jax.nn.sigmoid(gu[:, :128]) * gu[:, 128:]).astype(BF16)
    issue(jnp.int32(B_D - 1 + SLOTS), B_D - 1 + SLOTS, B_D - 1 + SLOTS)

    def d_partial(step):
        n = B_D + 2 * step
        s0 = wait_chunk(n, 3456)
        s1 = wait_chunk(n + 1, 3456)
        parts = [dot(act[...], pool[s, pl.ds(0, 3456), :]) for s in (s0, s1)]
        for q in (n, n + 1):
            @pl.when(q + SLOTS < B_END)
            def _(q=q):
                issue(q + SLOTS, B_D + SLOTS, B_END - 1)
        return jnp.concatenate(parts, axis=1)

    reduce_columns(1, d_partial)
    post_norm(1, gm_ref)
    ycopy = pltpu.make_async_copy(x, y_hbm, ysem)
    ycopy.start()
    vcopy.wait()
    kcopy.wait()
    ycopy.wait()


def solution(mesh):
    def local_layer(tokens, seq_lens, w_q, w_k, w_v, w_o, g_q, g_k, g_attn, g_mlp, w_gate, w_up, w_down):
        cos_tab, sin_tab = rope_tables(128)
        vmem = pl.BlockSpec(memory_space=pltpu.VMEM)
        hbm = pl.BlockSpec(memory_space=pl.ANY)
        gain = lambda g: g.astype(F32).reshape(1, -1)
        dma = pltpu.SemaphoreType.DMA
        y, kc, vc = pl.pallas_call(
            layer_kernel,
            out_shape=(jax.ShapeDtypeStruct((256, 5120), BF16), jax.ShapeDtypeStruct((2, 10, 128, 128), BF16), jax.ShapeDtypeStruct((2, 10, 128, 128), BF16)),
            in_specs=[pl.BlockSpec(memory_space=pltpu.SMEM)] + [vmem] * 6 + [hbm] * 8,
            out_specs=(hbm, hbm, hbm),
            scratch_shapes=[
                pltpu.VMEM((SLOTS, 5120, 256), BF16),
                pltpu.VMEM((256, 5120), BF16),
                pltpu.VMEM((2, 10, 128, 128), F32),
                pltpu.VMEM((2, 10, 128, 128), F32),
                pltpu.VMEM((2, 10, 128, 128), BF16),
                pltpu.VMEM((2, 10, 128, 128), BF16),
                pltpu.VMEM((256, 1280), BF16),
                pltpu.VMEM((256, 3456), BF16),
                pltpu.VMEM((2, 256, 128), F32),
                pltpu.VMEM((2, 256, 128), F32),
                pltpu.VMEM((8, 256), F32),
                pltpu.VMEM((3, 8, 256), F32),
                pltpu.VMEM((2, 5, 256, 512), BF16),
                pltpu.VMEM((2, 5, 256, 512), BF16),
                pltpu.VMEM((2, 5, 256, 512), BF16),
                pltpu.VMEM((2, 5, 256, 512), BF16),
                pltpu.VMEM((2, 10, 256, 512), BF16),
                dma((SLOTS,)), dma, dma((2,)), dma, dma((3,)), dma((3,)), dma((2, 6, 5)),
            ],
            compiler_params=pltpu.CompilerParams(collective_id=0, has_side_effects=True, vmem_limit_bytes=67043328),
        )(seq_lens, jnp.asarray(cos_tab), jnp.asarray(sin_tab), gain(g_q), gain(g_k), gain(g_attn), gain(g_mlp),
          tokens.reshape(256, 5120), w_q, w_k, w_v, w_o, w_gate, w_up, w_down)
        return y.reshape(2, 128, 5120), kc, vc

    return jax.shard_map(local_layer, mesh=mesh, in_specs=(P('dp', None, None), P('dp'), P(None, 'tp'), P(None, 'tp'), P(None, 'tp'), P('tp', None), P('tp'), P('tp'), P(), P(), P(None, 'tp'), P(None, 'tp'), P('tp', None)), out_specs=(P('dp', None, None), P('dp', 'tp', None, None), P('dp', 'tp', None, None)), check_vma=False)
```

```python
import functools

import numpy as np
import jax
import jax.numpy as jnp
from jax import lax
from jax.experimental import pallas as pl
from jax.experimental.pallas import tpu as pltpu
from jax.sharding import PartitionSpec as P

HEAD_DIM = 128
ROPE_BASE = 500000.0
NORM_EPS = 1e-6
SLOTS = 13
F32 = jnp.float32
BF16 = jnp.bfloat16


def rope_tables(seq_len):
    half = HEAD_DIM // 2
    inv_freq = (ROPE_BASE ** (-2.0 * np.arange(half) / HEAD_DIM)).astype(np.float32)
    angles = np.arange(seq_len, dtype=np.float32)[:, None] * inv_freq[None, :]
    cos, sin = np.cos(angles), np.sin(angles)
    return (np.concatenate([cos, cos], -1).astype(np.float32), np.concatenate([-sin, sin], -1).astype(np.float32))


def layer_kernel(seq_ref, cos_hbm, sin_hbm, gq_hbm, gk_hbm, ga_hbm,
                 x_hbm, wq, wk, wv, wo, wg, wu, wd,
                 h_hbm, m_hbm, rs_hbm, kc_hbm, vc_hbm,
                 pool, x, qraw, kraw, kb, vb, o, act, ssq_acc, rsc, ssq_send, ssq_recv,
                 rs_send, rs_recv, xs_send, xs_recv, full,
                 cos_ref, sin_ref, gq16, gk16, ga16, gq_ref, gk_ref, ga_ref, sq_acc, rs_out,
                 wsem, xsem, csem, ysem, ssq_s, ssq_r, arsem, tsem):
    dp = lax.axis_index("dp")
    t = lax.axis_index("tp")
    core = lax.rem(t, 2)
    sib = t + 1 - 2 * core
    xpeer = lax.rem(t + 2, 4)
    diag = 3 - t
    width = 5120

    B_V, B_O, B_G, B_D, B_END = 10, 15, 20, 47, 67

    def half_col(step, per):
        return lax.rem(step, per) + per * lax.rem(step // per + 1 + core, 2)

    def cols(start, size):
        return pl.ds(pl.multiple_of(start, size), size)

    def issue(n, lo, hi):
        slot = lax.rem(n, SLOTS)
        sem = wsem.at[slot]

        def copy(src, dst):
            pltpu.make_async_copy(src, dst, sem).start()

        def do_qk():
            @pl.when(lax.rem(n, 2) == 0)
            def _():
                copy(wq.at[:, cols((n // 2) * 256, 256)], pool.at[slot])

            @pl.when(lax.rem(n, 2) == 1)
            def _():
                copy(wk.at[:, cols((n // 2) * 256, 256)], pool.at[slot])

        def do_v():
            copy(wv.at[:, cols((n - B_V) * 256, 256)], pool.at[slot])

        def do_o():
            for k in range(4):
                step = 2 * (n - B_O) + k // 2
                copy(wo.at[:, cols(half_col(step, 5) * 512 + (k % 2) * 256, 256)], pool.at[slot, pl.ds(k * 1280, 1280), :])

        def do_g():
            r = n - B_G

            @pl.when(jnp.logical_and(lax.rem(r, 2) == 0, r < 26))
            def _():
                copy(wg.at[:, cols((r // 2) * 256, 256)], pool.at[slot])

            @pl.when(lax.rem(r, 2) == 1)
            def _():
                copy(wu.at[:, cols((r // 2) * 256, 256)], pool.at[slot])

            @pl.when(r == 26)
            def _():
                copy(wg.at[:, pl.ds(3328, 128)], pool.at[slot, :, pl.ds(0, 128)])
                copy(wu.at[:, pl.ds(3328, 128)], pool.at[slot, :, pl.ds(128, 128)])

        def do_d():
            copy(wd.at[:, cols(half_col(n - B_D, 10) * 256, 256)], pool.at[slot, pl.ds(0, 3456), :])

        for start, end, fn in ((0, B_V, do_qk), (B_V, B_O, do_v), (B_O, B_G, do_o), (B_G, B_D, do_g), (B_D, B_END, do_d)):
            if hi < start or lo >= end:
                continue
            if lo >= start and hi < end:
                fn()
            else:
                pl.when(jnp.logical_and(n >= start, n < end))(fn)

    def wait_chunk(n, rows=5120):
        slot = lax.rem(n, SLOTS)
        src = wq if rows == 5120 else wd
        pltpu.make_async_copy(src.at[:, pl.ds(0, 256)], pool.at[slot, pl.ds(0, rows), :], wsem.at[slot]).wait()
        return slot

    def dot(a, b):
        return jnp.dot(a, b, preferred_element_type=F32)

    xcopy = pltpu.make_async_copy(x_hbm, x, xsem)
    xcopy.start()
    for n in range(SLOTS):
        issue(jnp.int32(n), n, n)
    small = [pltpu.make_async_copy(src, dst, tsem.at[i]) for i, (src, dst) in enumerate(
        ((cos_hbm, cos_ref), (sin_hbm, sin_ref), (gq_hbm, gq16), (gk_hbm, gk16), (ga_hbm, ga16)))]
    for c in small:
        c.start()

    barrier = pltpu.get_barrier_semaphore()
    for peer in (sib, xpeer, diag):
        pl.semaphore_signal(barrier, inc=1, device_id={"tp": peer}, device_id_type=pl.DeviceIdType.MESH)
    with jax.named_scope("barrier"):
        pl.semaphore_wait(barrier, 3)

    def remote(src, dst, ssem, rsem, peer):
        return pltpu.make_async_remote_copy(src_ref=src, dst_ref=dst, send_sem=ssem, recv_sem=rsem,
                                            device_id={"tp": peer}, device_id_type=pl.DeviceIdType.MESH)

    for c in small:
        c.wait()
    for src, dst in ((gq16, gq_ref), (gk16, gk_ref), (ga16, ga_ref)):
        dst[...] = src[...].astype(F32)
    xcopy.wait()
    ssq_acc[...] = jnp.zeros_like(ssq_acc)

    def qk_step(i, carry):
        n = 2 * i
        s0 = wait_chunk(n)
        s1 = wait_chunk(n + 1)
        q = dot(x[...], pool[s0])
        k = dot(x[...], pool[s1])
        for b in range(2):
            for hh in range(2):
                qraw[b, 2 * i + hh] = q[b * 128:(b + 1) * 128, hh * 128:(hh + 1) * 128]
                kraw[b, 2 * i + hh] = k[b * 128:(b + 1) * 128, hh * 128:(hh + 1) * 128]
        ssq_acc[0] += q[:, :128] * q[:, :128] + q[:, 128:] * q[:, 128:]
        ssq_acc[1] += k[:, :128] * k[:, :128] + k[:, 128:] * k[:, 128:]
        issue(n + SLOTS, SLOTS, SLOTS + 8)
        issue(n + 1 + SLOTS, SLOTS + 1, SLOTS + 9)
        return carry

    with jax.named_scope("qk"):
        lax.fori_loop(0, 5, qk_step, 0)

    for r in range(2):
        ssq_send[r:r + 1, :] = jnp.sum(jnp.transpose(ssq_acc[r]), axis=0, keepdims=True)
    ssq_send[2:8, :] = jnp.zeros((6, 256), F32)
    ssq_copies = [remote(ssq_send, ssq_recv.at[j], ssq_s.at[j], ssq_r.at[j], peer) for j, peer in enumerate((sib, xpeer, diag))]
    for c in ssq_copies:
        c.start()

    for group in ((10, 11), (12, 13), (14,)):
        slots = [wait_chunk(jnp.int32(n)) for n in group]
        vals = [dot(x[...], pool[s]).astype(BF16) for s in slots]
        for n, v in zip(group, vals):
            for b in range(2):
                for hh in range(2):
                    vb[b, 2 * (n - B_V) + hh] = v[b * 128:(b + 1) * 128, hh * 128:(hh + 1) * 128]
        for n in group:
            issue(jnp.int32(n + SLOTS), n + SLOTS, n + SLOTS)
    vcopy = pltpu.make_async_copy(vb, vc_hbm, csem.at[0])
    vcopy.start()

    with jax.named_scope("ssqwait"):
        for c in ssq_copies:
            c.wait()
    total = ssq_send[...] + ssq_recv[0] + ssq_recv[1] + ssq_recv[2]
    scale = lax.rsqrt(total * (1.0 / width) + NORM_EPS)
    for r in range(2):
        rsc[r] = jnp.transpose(jnp.broadcast_to(scale[r:r + 1, :], (128, 256)))

    row = lax.broadcasted_iota(jnp.int32, (128, 128), 0)
    col = lax.broadcasted_iota(jnp.int32, (128, 128), 1)

    def rope(v):
        return (v * cos_ref[...] + pltpu.roll(v, 64, 1) * sin_ref[...]).astype(BF16)

    for b in range(2):
        allowed = jnp.logical_and(col <= row, col < seq_ref[b])

        def attn_step(i, carry, b=b, allowed=allowed):
            for u in range(5):
                h = i * 5 + u
                hs = cols(h * 128, 128)
                q = rope(qraw[b, h] * rsc[0, b * 128:(b + 1) * 128, :] * gq_ref[pl.ds(h, 1), :])
                k = rope(kraw[b, h] * rsc[1, b * 128:(b + 1) * 128, :] * gk_ref[pl.ds(h, 1), :])
                kb[b, h] = k
                s = lax.dot_general(q, k, (((1,), (1,)), ((), ())), preferred_element_type=F32) * HEAD_DIM ** -0.5
                s = jnp.where(allowed, s, -1e30)
                e = jnp.exp(s - jnp.max(s, axis=-1, keepdims=True))
                p = (e / jnp.sum(e, axis=-1, keepdims=True)).astype(BF16)
                o[b * 128:(b + 1) * 128, hs] = dot(p, vb[b, h]).astype(BF16)
            return carry

        with jax.named_scope("attn"):
            lax.fori_loop(0, 2, attn_step, 0)
    kcopy = pltpu.make_async_copy(kb, kc_hbm, csem.at[1])
    kcopy.start()

    def rs_copy(p, j):
        return remote(rs_send.at[p, j], rs_recv.at[p, j], arsem.at[p, 0, j], arsem.at[p, 1, j], sib)

    def xs_copy(p, j):
        return remote(xs_send.at[p, j], xs_recv.at[p, j], arsem.at[p, 2, j], arsem.at[p, 3, j], xpeer)

    def ag_copy(p, j, owner):
        blk = full.at[p, owner * 5 + j]
        return remote(blk, blk, arsem.at[p, 4, j], arsem.at[p, 5, j], sib)

    def reduce_columns(p, partial):
        def sib_step(j, carry):
            rs_send[p, j] = partial(j).astype(BF16)
            rs_copy(p, j).start()
            return carry

        with jax.named_scope(f"sib{p}"):
            lax.fori_loop(0, 5, sib_step, 0)

        def own_step(j, carry):
            val = partial(j + 5)
            rs_copy(p, j).wait()
            xs_send[p, j] = (val + rs_recv[p, j].astype(F32)).astype(BF16)
            xs_copy(p, j).start()
            return carry

        with jax.named_scope(f"own{p}"):
            lax.fori_loop(0, 5, own_step, 0)

        def squares(c):
            v = full[p, c].astype(F32)
            return v[:, :128] * v[:, :128] + v[:, 128:256] * v[:, 128:256] + v[:, 256:384] * v[:, 256:384] + v[:, 384:] * v[:, 384:]

        sq_acc[...] = jnp.zeros_like(sq_acc)

        def gather_step(j, carry):
            with jax.named_scope(f"xwait{p}"):
                xs_copy(p, j).wait()
            full[p, core * 5 + j] = (xs_send[p, j].astype(F32) + xs_recv[p, j].astype(F32)).astype(BF16)
            ag_copy(p, j, core).start()
            sq_acc[0] += squares(core * 5 + j)
            return carry

        with jax.named_scope(f"gather{p}"):
            lax.fori_loop(0, 5, gather_step, 0)

        def arrive_step(j, carry):
            ag_copy(p, j, core).wait_send()
            ag_copy(p, j, 1 - core).wait_recv()
            sq_acc[1] += squares((1 - core) * 5 + j)
            return carry

        with jax.named_scope(f"arrive{p}"):
            lax.fori_loop(0, 5, arrive_step, 0)
        return lax.rsqrt(jnp.sum(sq_acc[0] + sq_acc[1], axis=-1, keepdims=True) * (1.0 / width) + NORM_EPS)

    def post_norm(rs, gain):
        rsb = jnp.broadcast_to(rs, (256, 128))

        def apply(c, carry):
            for w in range(4):
                cs = cols(c * 512 + w * 128, 128)
                x[:, cs] = (x[:, cs].astype(F32) + full[0, c, :, pl.ds(w * 128, 128)].astype(F32) * rsb * gain[pl.ds(c * 4 + w, 1), :]).astype(BF16)
            return carry

        lax.fori_loop(0, 10, apply, 0)

    def o_partial(step):
        n = B_O + step // 2
        slot = lax.rem(n, SLOTS)

        @pl.when(lax.rem(step, 2) == 0)
        def _():
            wait_chunk(n)

        base = lax.rem(step, 2) * 2560
        parts = [dot(o[...], pool[slot, pl.ds(pl.multiple_of(base + k * 1280, 1280), 1280), :]) for k in range(2)]

        @pl.when(lax.rem(step, 2) == 1)
        def _():
            issue(n + SLOTS, B_O + SLOTS, B_O + SLOTS + 4)

        return jnp.concatenate(parts, axis=1)

    with jax.named_scope("ar1"):
        rs = reduce_columns(0, o_partial)
    with jax.named_scope("norm1"):
        post_norm(rs, ga_ref)
    hcopy = pltpu.make_async_copy(x, h_hbm, ysem.at[0])
    hcopy.start()

    def gu_step(i, carry):
        n = B_G + 2 * i
        s0 = wait_chunk(n)
        s1 = wait_chunk(n + 1)
        g = dot(x[...], pool[s0])
        u = dot(x[...], pool[s1])
        act[:, cols(i * 256, 256)] = (g * jax.nn.sigmoid(g) * u).astype(BF16)
        issue(n + SLOTS, B_G + SLOTS, B_D + SLOTS - 2)
        issue(n + 1 + SLOTS, B_G + 1 + SLOTS, B_D + SLOTS - 2)
        return carry

    with jax.named_scope("gu"):
        lax.fori_loop(0, 13, gu_step, 0)
    s0 = wait_chunk(jnp.int32(B_D - 1))
    gu = dot(x[...], pool[s0])
    act[:, 3328:3456] = (gu[:, :128] * jax.nn.sigmoid(gu[:, :128]) * gu[:, 128:]).astype(BF16)
    issue(jnp.int32(B_D - 1 + SLOTS), B_D - 1 + SLOTS, B_D - 1 + SLOTS)

    def d_partial(step):
        n = B_D + 2 * step
        s0 = wait_chunk(n, 3456)
        s1 = wait_chunk(n + 1, 3456)
        parts = [dot(act[...], pool[s, pl.ds(0, 3456), :]) for s in (s0, s1)]
        for q in (n, n + 1):
            @pl.when(q + SLOTS < B_END)
            def _(q=q):
                issue(q + SLOTS, B_D + SLOTS, B_END - 1)
        return jnp.concatenate(parts, axis=1)

    with jax.named_scope("ar2"):
        rs = reduce_columns(1, d_partial)
    with jax.named_scope("tail"):
        rs_out[...] = jnp.broadcast_to(rs, (256, 128))
        mcopy = pltpu.make_async_copy(full.at[1], m_hbm, ysem.at[1])
        mcopy.start()
        rcopy = pltpu.make_async_copy(rs_out, rs_hbm, ysem.at[2])
        rcopy.start()
        for c in (vcopy, kcopy, hcopy, mcopy, rcopy):
            c.wait()


def finish_kernel(rs_hbm, gm_hbm, h_hbm, m_hbm, k_in, v_in, y_hbm, k_out, v_out, rs, gm, h, m, kb, vb, isem, msem, hsem, osem, ysem):
    copies = [pltpu.make_async_copy(src, dst, isem.at[i]) for i, (src, dst) in enumerate(((rs_hbm, rs), (gm_hbm, gm), (k_in, kb), (v_in, vb)))]
    for c in copies[:2]:
        c.start()

    def halves(c):
        return [pltpu.make_async_copy(m_hbm.at[c], m.at[c], msem.at[c]), pltpu.make_async_copy(h_hbm.at[:, pl.ds(c * 512, 512)], h.at[:, pl.ds(c * 512, 512)], hsem.at[c])]

    for c in range(10):
        for d in halves(c):
            d.start()
    for c in copies[2:]:
        c.start()
    copies[0].wait()
    copies[1].wait()
    out = []
    for c in range(10):
        for d in halves(c):
            d.wait()
        for w in range(4):
            cs = pl.ds(c * 512 + w * 128, 128)
            g = gm[c * 4 + w:c * 4 + w + 1, :].astype(F32)
            h[:, cs] = (h[:, cs].astype(F32) + m[c, :, pl.ds(w * 128, 128)].astype(F32) * rs[...] * g).astype(BF16)
        cs = pl.ds(c * 512, 512)
        out.append(pltpu.make_async_copy(h.at[:, cs], y_hbm.at[:, cs], ysem.at[c]))
        out[-1].start()
    for i, (src, dst) in enumerate(((kb, k_out), (vb, v_out))):
        copies[2 + i].wait()
        out.append(pltpu.make_async_copy(src, dst, osem.at[i]))
        out[-1].start()
    for d in out:
        d.wait()


def solution(mesh):
    def local_layer(tokens, seq_lens, w_q, w_k, w_v, w_o, g_q, g_k, g_attn, g_mlp, w_gate, w_up, w_down):
        cos_tab, sin_tab = rope_tables(128)
        hbm = pl.BlockSpec(memory_space=pl.ANY)
        gain = lambda g: g.reshape(-1, 128)
        dma = pltpu.SemaphoreType.DMA
        cache = jax.ShapeDtypeStruct((2, 10, 128, 128), BF16)
        hidden = jax.ShapeDtypeStruct((256, 5120), BF16)
        h, m, rs, kc, vc = pl.pallas_call(
            layer_kernel,
            out_shape=(hidden, jax.ShapeDtypeStruct((10, 256, 512), BF16), jax.ShapeDtypeStruct((256, 128), F32), cache, cache),
            in_specs=[pl.BlockSpec(memory_space=pltpu.SMEM)] + [hbm] * 13,
            out_specs=(hbm,) * 5,
            scratch_shapes=[
                pltpu.VMEM((SLOTS, 5120, 256), BF16),
                pltpu.VMEM((256, 5120), BF16),
                pltpu.VMEM((2, 10, 128, 128), F32),
                pltpu.VMEM((2, 10, 128, 128), F32),
                pltpu.VMEM((2, 10, 128, 128), BF16),
                pltpu.VMEM((2, 10, 128, 128), BF16),
                pltpu.VMEM((256, 1280), BF16),
                pltpu.VMEM((256, 3456), BF16),
                pltpu.VMEM((2, 256, 128), F32),
                pltpu.VMEM((2, 256, 128), F32),
                pltpu.VMEM((8, 256), F32),
                pltpu.VMEM((3, 8, 256), F32),
                pltpu.VMEM((2, 5, 256, 512), BF16),
                pltpu.VMEM((2, 5, 256, 512), BF16),
                pltpu.VMEM((2, 5, 256, 512), BF16),
                pltpu.VMEM((2, 5, 256, 512), BF16),
                pltpu.VMEM((2, 10, 256, 512), BF16),
                pltpu.VMEM((128, 128), F32),
                pltpu.VMEM((128, 128), F32),
                pltpu.VMEM((10, 128), BF16),
                pltpu.VMEM((10, 128), BF16),
                pltpu.VMEM((40, 128), BF16),
                pltpu.VMEM((10, 128), F32),
                pltpu.VMEM((10, 128), F32),
                pltpu.VMEM((40, 128), F32),
                pltpu.VMEM((2, 256, 128), F32),
                pltpu.VMEM((256, 128), F32),
                dma((SLOTS,)), dma, dma((2,)), dma((3,)), dma((3,)), dma((3,)), dma((2, 6, 5)), dma((6,)),
            ],
            compiler_params=pltpu.CompilerParams(collective_id=0, has_side_effects=True, vmem_limit_bytes=67043328),
        )(seq_lens, jnp.asarray(cos_tab), jnp.asarray(sin_tab), gain(g_q), gain(g_k), gain(g_attn),
          tokens.reshape(256, 5120), w_q, w_k, w_v, w_o, w_gate, w_up, w_down)
        y, kc, vc = pl.pallas_call(
            finish_kernel,
            out_shape=(hidden, cache, cache),
            in_specs=[hbm] * 6,
            out_specs=(hbm,) * 3,
            scratch_shapes=[
                pltpu.VMEM((256, 128), F32),
                pltpu.VMEM((40, 128), BF16),
                pltpu.VMEM((256, 5120), BF16),
                pltpu.VMEM((10, 256, 512), BF16),
                pltpu.VMEM((2, 10, 128, 128), BF16),
                pltpu.VMEM((2, 10, 128, 128), BF16),
                dma((4,)), dma((10,)), dma((10,)), dma((2,)), dma((10,)),
            ],
            compiler_params=pltpu.CompilerParams(vmem_limit_bytes=60000000),
        )(rs, gain(g_mlp), h, m, kc, vc)
        return y.reshape(2, 128, 5120), kc, vc

    return jax.shard_map(local_layer, mesh=mesh, in_specs=(P('dp', None, None), P('dp'), P(None, 'tp'), P(None, 'tp'), P(None, 'tp'), P('tp', None), P('tp'), P('tp'), P(), P(), P(None, 'tp'), P(None, 'tp'), P('tp', None)), out_specs=(P('dp', None, None), P('dp', 'tp', None, None), P('dp', 'tp', None, None)), check_vma=False)
```

```python
import jax
import jax.numpy as jnp
import numpy as np
from jax import lax
from jax.experimental import pallas as pl
from jax.experimental.pallas import tpu as pltpu
from jax.sharding import PartitionSpec as P

HEAD_DIM = 128
ROPE_BASE = 500000.0
NORM_EPS = 1e-6
F32 = jnp.float32
BF16 = jnp.bfloat16

WIDTH = 5120
RING = 8
KEEP = 8
N_V, N_QKV = 10, 15
N_G = 27
N_RG = N_G - KEEP
N_MLP = N_RG + 20


def rope_tables(seq_len):
    half = HEAD_DIM // 2
    inv_freq = (ROPE_BASE ** (-2.0 * np.arange(half) / HEAD_DIM)).astype(np.float32)
    angles = np.arange(seq_len, dtype=np.float32)[:, None] * inv_freq[None, :]
    cos, sin = np.cos(angles), np.sin(angles)
    return (np.concatenate([cos, cos], -1).astype(np.float32), np.concatenate([-sin, sin], -1).astype(np.float32))


def cols(start, size):
    return pl.ds(pl.multiple_of(start, size), size)


def dot(a, b):
    return jnp.dot(a, b, preferred_element_type=F32)


def layer_kernel(seq_ref, cos_hbm, sin_hbm, gq_hbm, gk_hbm, ga_hbm,
                 x_hbm, wq, wk, wv, wo, wg, wu, wd,
                 h_hbm, m_hbm, rs_hbm, kc_hbm, vc_hbm,
                 pool, x, qraw, kraw, kb, vb, qb, o, act, own32, ssq_acc, rsc, ssq_send, ssq_recv,
                 rs_send, rs_recv, xs_send, xs_recv, full, sq_acc, rs_out,
                 cos_ref, sin_ref, gq16, gk16, ga16, gq_ref, gk_ref, ga_ref,
                 wsem, xsem, csem, ysem, ssq_s, ssq_r, arsem, tsem):
    t = lax.axis_index("tp")
    core = lax.rem(t, 2)
    sib = t + 1 - 2 * core
    xpeer = lax.rem(t + 2, 4)
    diag = 3 - t

    def load(src, dst, slot):
        pltpu.make_async_copy(src, dst, wsem.at[slot]).start()

    def load_qk(n):
        slot = lax.rem(n, RING)

        @pl.when(lax.rem(n, 2) == 0)
        def _():
            load(wq.at[:, cols((n // 2) * 256, 256)], pool.at[slot], slot)

        @pl.when(lax.rem(n, 2) == 1)
        def _():
            load(wk.at[:, cols((n // 2) * 256, 256)], pool.at[slot], slot)

    def load_v(n):
        slot = lax.rem(n, RING)
        load(wv.at[:, cols((n - N_V) * 256, 256)], pool.at[slot], slot)

    def load_o(j):
        slot = RING + j
        for k in range(4):
            half = core if k // 2 else 1 - core
            load(wo.at[:, cols(half * 2560 + j * 512 + (k % 2) * 256, 256)], pool.at[slot, pl.ds(k * 1280, 1280), :], slot)

    def load_g(k, slot):
        @pl.when(jnp.logical_and(lax.rem(k, 2) == 0, k < N_G - 1))
        def _():
            load(wg.at[:, cols((k // 2) * 256, 256)], pool.at[slot], slot)

        @pl.when(lax.rem(k, 2) == 1)
        def _():
            load(wu.at[:, cols((k // 2) * 256, 256)], pool.at[slot], slot)

        @pl.when(k == N_G - 1)
        def _():
            load(wg.at[:, pl.ds(3328, 128)], pool.at[slot, :, pl.ds(0, 128)], slot)
            load(wu.at[:, pl.ds(3328, 128)], pool.at[slot, :, pl.ds(128, 128)], slot)

    def keep_slot(k):
        return RING + lax.rem(k + 5, KEEP)

    def ring_slot(b, l):
        return lax.rem(N_QKV + N_MLP * b + l, RING)

    def load_ring(b, l, lo, hi):
        slot = ring_slot(b, l)

        def g():
            load_g(KEEP + l, slot)

        def d():
            q = l - N_RG
            half = lax.rem(lax.rem(q, 4) // 2 + 1 + core, 2)
            load(wd.at[:, cols(half * 2560 + (q // 4) * 512 + lax.rem(q, 2) * 256, 256)], pool.at[slot, pl.ds(0, 3456), :], slot)

        def nxt():
            load_g(KEEP + l - N_MLP, slot)

        for start, end, fn in ((0, N_RG, g), (N_RG, N_MLP, d), (N_MLP, 2 * N_MLP, nxt if b == 0 else None)):
            if fn is None or hi < start or lo >= end:
                continue
            if lo >= start and hi < end:
                fn()
            else:
                pl.when(jnp.logical_and(l >= start, l < end))(fn)

    def wait_slot(slot, rows=WIDTH):
        src = wq if rows == WIDTH else wd
        pltpu.make_async_copy(src.at[:, pl.ds(0, 256)], pool.at[slot, pl.ds(0, rows), :], wsem.at[slot]).wait()

    def i32(v):
        return jnp.int32(v)

    xcopy = pltpu.make_async_copy(x_hbm, x, xsem)
    xcopy.start()
    for n in range(2):
        load_qk(i32(n))
    small = [pltpu.make_async_copy(src, dst, tsem.at[i]) for i, (src, dst) in enumerate(
        ((cos_hbm, cos_ref), (sin_hbm, sin_ref), (gq_hbm, gq16), (gk_hbm, gk16), (ga_hbm, ga16)))]
    for c in small:
        c.start()
    for n in range(2, 4):
        load_qk(i32(n))

    barrier = pltpu.get_barrier_semaphore()
    for peer in (sib, xpeer, diag):
        pl.semaphore_signal(barrier, inc=1, device_id={"tp": peer}, device_id_type=pl.DeviceIdType.MESH)

    def remote(src, dst, ssem, rsem, peer):
        return pltpu.make_async_remote_copy(src_ref=src, dst_ref=dst, send_sem=ssem, recv_sem=rsem,
                                            device_id={"tp": peer}, device_id_type=pl.DeviceIdType.MESH)

    ssq_acc[...] = jnp.zeros_like(ssq_acc)
    xcopy.wait()

    def qk_step(i, carry):
        n = 2 * i
        s0, s1 = lax.rem(n, RING), lax.rem(n + 1, RING)
        wait_slot(s0)
        wait_slot(s1)
        for m in (n + 4, n + 5):
            pl.when(m < N_V)(lambda m=m: load_qk(m))
            pl.when(m >= N_V)(lambda m=m: load_v(m))
        q = dot(x[...], pool[s0])
        k = dot(x[...], pool[s1])
        for b in range(2):
            for hh in range(2):
                qraw[b, 2 * i + hh] = q[b * 128:(b + 1) * 128, hh * 128:(hh + 1) * 128]
                kraw[b, 2 * i + hh] = k[b * 128:(b + 1) * 128, hh * 128:(hh + 1) * 128]
        ssq_acc[0] += q[:, :128] * q[:, :128] + q[:, 128:] * q[:, 128:]
        ssq_acc[1] += k[:, :128] * k[:, :128] + k[:, 128:] * k[:, 128:]
        return carry

    with jax.named_scope("qk"):
        lax.fori_loop(0, 5, qk_step, 0)

    for r in range(2):
        ssq_send[r:r + 1, :] = jnp.sum(jnp.transpose(ssq_acc[r]), axis=0, keepdims=True)
    ssq_send[2:8, :] = jnp.zeros((6, 256), F32)
    with jax.named_scope("barrier"):
        pl.semaphore_wait(barrier, 3)
    ssq_copies = [remote(ssq_send, ssq_recv.at[j], ssq_s.at[j], ssq_r.at[j], peer) for j, peer in enumerate((sib, xpeer, diag))]
    for c in ssq_copies:
        c.start()

    with jax.named_scope("v"):
        for group in ((10, 11), (12, 13), (14,)):
            for n in group:
                wait_slot(n % RING)
            if group[0] == 10:
                load_v(i32(14))
                load_o(0)
                load_o(1)
            elif group[0] == 12:
                load_o(2)
                load_o(3)
                load_o(4)
            else:
                for k in range(KEEP - 5):
                    load_g(i32(k), keep_slot(i32(k)))
            vals = [dot(x[...], pool[n % RING]).astype(BF16) for n in group]
            for n, v in zip(group, vals):
                for b in range(2):
                    for hh in range(2):
                        vb[b, 2 * (n - N_V) + hh] = v[b * 128:(b + 1) * 128, hh * 128:(hh + 1) * 128]
    vcopy = pltpu.make_async_copy(vb, vc_hbm, csem.at[0])
    vcopy.start()
    for l in range(RING):
        load_ring(0, i32(l), l, l)

    with jax.named_scope("ssqwait"):
        for c in ssq_copies:
            c.wait()
    for c in small:
        c.wait()
    for src, dst in ((gq16, gq_ref), (gk16, gk_ref), (ga16, ga_ref)):
        dst[...] = src[...].astype(F32)
    total = ssq_send[...] + ssq_recv[0] + ssq_recv[1] + ssq_recv[2]
    scale = lax.rsqrt(total * (1.0 / WIDTH) + NORM_EPS)
    for r in range(2):
        rsc[r] = jnp.transpose(jnp.broadcast_to(scale[r:r + 1, :], (128, 256)))

    def rope(v):
        return (v * cos_ref[...] + pltpu.roll(v, 64, 1) * sin_ref[...]).astype(BF16)

    def attention(b):
        rows = pl.ds(b * 128, 128)
        row = lax.broadcasted_iota(jnp.int32, (128, 128), 0)
        col = lax.broadcasted_iota(jnp.int32, (128, 128), 1)
        allowed = jnp.logical_and(col <= row, col < seq_ref[b])
        for h in range(10):
            qb[h] = rope(qraw[b, h] * rsc[0, rows, :] * gq_ref[h:h + 1, :])
            kb[b, h] = rope(kraw[b, h] * rsc[1, rows, :] * gk_ref[h:h + 1, :])
        for h in range(10):
            qraw[b, h] = lax.dot_general(qb[h], kb[b, h], (((1,), (1,)), ((), ())), preferred_element_type=F32)
        for h in range(10):
            s = jnp.where(allowed, qraw[b, h] * HEAD_DIM ** -0.5, -1e30)
            e = jnp.exp(s - jnp.max(s, axis=-1, keepdims=True))
            qb[h] = (e / jnp.sum(e, axis=-1, keepdims=True)).astype(BF16)
        for h in range(10):
            o[rows, pl.ds(h * 128, 128)] = dot(qb[h], vb[b, h]).astype(BF16)

    def rs_copy(p, b, j):
        return remote(rs_send.at[b, j], rs_recv.at[b, j], arsem.at[p, b, 0, j], arsem.at[p, b, 1, j], sib)

    def xs_copy(p, b, j):
        return remote(xs_send.at[b, j], xs_recv.at[p, b, j], arsem.at[p, b, 2, j], arsem.at[p, b, 3, j], xpeer)

    def ag_copy(p, b, j, owner):
        blk = full.at[b, owner * 5 + j]
        return remote(blk, blk, arsem.at[p, b, 4, j], arsem.at[p, b, 5, j], sib)

    def reduce_half(p, b, partial):
        def finish(j):
            rs_copy(p, b, j).wait()
            xs_send[b, j] = (own32[lax.rem(j, 2)] + rs_recv[b, j].astype(F32)).astype(BF16)
            xs_copy(p, b, j).start()

        def step(j, carry):
            parts = partial(j)
            for k in range(2):
                rs_send[b, j, :, pl.ds(k * 256, 256)] = parts[k].astype(BF16)
                own32[lax.rem(j, 2), :, pl.ds(k * 256, 256)] = parts[2 + k]
            rs_copy(p, b, j).start()
            pl.when(j > 0)(lambda: finish(j - 1))
            return carry

        lax.fori_loop(0, 5, step, 0)
        finish(i32(4))

    def squares(b, c):
        v = full[b, c].astype(F32)
        return v[:, :128] * v[:, :128] + v[:, 128:256] * v[:, 128:256] + v[:, 256:384] * v[:, 256:384] + v[:, 384:] * v[:, 384:]

    def gather(p, b):
        sq_acc[b] = jnp.zeros((2, 128, 128), F32)

        def step(j, carry):
            with jax.named_scope(f"xwait{p}{b}"):
                xs_copy(p, b, j).wait()
            full[b, core * 5 + j] = (xs_send[b, j].astype(F32) + xs_recv[p, b, j].astype(F32)).astype(BF16)
            ag_copy(p, b, j, core).start()
            sq_acc[b, 0] += squares(b, core * 5 + j)
            return carry

        lax.fori_loop(0, 5, step, 0)

    def arrive(p, b):
        def step(j, carry):
            ag_copy(p, b, j, core).wait_send()
            ag_copy(p, b, j, 1 - core).wait_recv()
            sq_acc[b, 1] += squares(b, (1 - core) * 5 + j)
            return carry

        lax.fori_loop(0, 5, step, 0)
        rs = lax.rsqrt(jnp.sum(sq_acc[b, 0] + sq_acc[b, 1], axis=-1, keepdims=True) * (1.0 / WIDTH) + NORM_EPS)
        rs_out[p, pl.ds(b * 128, 128), :] = jnp.broadcast_to(rs, (128, 128))

    def norm_hidden(b):
        rows = pl.ds(b * 128, 128)

        def apply(c, carry):
            for w in range(4):
                cs = cols(c * 512 + w * 128, 128)
                x[rows, cs] = (x[rows, cs].astype(F32) + full[b, c, :, pl.ds(w * 128, 128)].astype(F32) * rs_out[0, rows, :] * ga_ref[pl.ds(c * 4 + w, 1), :]).astype(BF16)
            return carry

        lax.fori_loop(0, 10, apply, 0)
        pltpu.make_async_copy(x.at[rows], h_hbm.at[rows], ysem.at[b]).start()

    def o_partial(b):
        def partial(j):
            slot = RING + j
            if b == 0:
                wait_slot(slot)
            return [dot(o[pl.ds(b * 128, 128), :], pool[slot, pl.ds(k * 1280, 1280), :]) for k in range(4)]
        return partial

    for b in range(2):
        with jax.named_scope(f"attn{b}"):
            attention(b)
        with jax.named_scope(f"o{b}"):
            reduce_half(0, b, o_partial(b))
    kcopy = pltpu.make_async_copy(kb, kc_hbm, csem.at[1])
    kcopy.start()
    for k in range(KEEP - 5, KEEP):
        load_g(i32(k), keep_slot(i32(k)))

    def gu_store(i, g, u):
        act[:, cols(i * 256, 256)] = (g * jax.nn.sigmoid(g) * u).astype(BF16)

    def gu_keep(b):
        def step(i, carry):
            s0, s1 = keep_slot(2 * i), keep_slot(2 * i + 1)
            if b == 0:
                wait_slot(s0)
                wait_slot(s1)
            xb = x[pl.ds(b * 128, 128), :]
            gu_store(i, dot(xb, pool[s0]), dot(xb, pool[s1]))
            return carry

        with jax.named_scope(f"gukeep{b}"):
            lax.fori_loop(0, KEEP // 2, step, 0)

    def gu_ring(b):
        def step(i, carry):
            l = 2 * i
            s0, s1 = ring_slot(b, l), ring_slot(b, l + 1)
            wait_slot(s0)
            wait_slot(s1)
            xb = x[pl.ds(b * 128, 128), :]
            gu_store(i + KEEP // 2, dot(xb, pool[s0]), dot(xb, pool[s1]))
            load_ring(b, l + RING, RING, N_RG - 3 + RING)
            load_ring(b, l + 1 + RING, 1 + RING, N_RG - 2 + RING)
            return carry

        with jax.named_scope(f"guring{b}"):
            lax.fori_loop(0, N_RG // 2, step, 0)
        l = N_RG - 1
        s0 = (N_QKV + N_MLP * b + l) % RING
        wait_slot(s0)
        r = dot(x[pl.ds(b * 128, 128), :], pool[s0])
        g = r[:, :128]
        act[:, 3328:3456] = (g * jax.nn.sigmoid(g) * r[:, 128:]).astype(BF16)
        load_ring(b, i32(l + RING), l + RING, l + RING)

    def d_partial(b):
        def partial(j):
            parts = []
            for k in range(4):
                l = N_RG + 4 * j + k
                slot = ring_slot(b, l)
                wait_slot(slot, 3456)
                parts.append(slot)
            parts = [dot(act[...], pool[s, pl.ds(0, 3456), :]) for s in parts]
            for k in range(4):
                l = N_RG + 4 * j + k
                if b == 0:
                    load_ring(b, l + RING, N_RG + RING, N_MLP - 1 + RING)
                else:
                    pl.when(l + RING < N_MLP)(lambda l=l: load_ring(b, l + RING, N_RG + RING, N_MLP - 1))
            return parts
        return partial

    with jax.named_scope("gather00"):
        gather(0, 0)
    with jax.named_scope("norm00"):
        arrive(0, 0)
        norm_hidden(0)
    gu_ring(0)
    gu_keep(0)
    with jax.named_scope("d0"):
        reduce_half(1, 0, d_partial(0))
    with jax.named_scope("gather01"):
        gather(0, 1)
    with jax.named_scope("norm01"):
        arrive(0, 1)
        norm_hidden(1)
    gu_keep(1)
    gu_ring(1)
    with jax.named_scope("d1"):
        reduce_half(1, 1, d_partial(1))
    mcopies = []
    for b in range(2):
        with jax.named_scope(f"gather1{b}"):
            gather(1, b)
        with jax.named_scope(f"arrive1{b}"):
            arrive(1, b)
        mcopies.append(pltpu.make_async_copy(full.at[b], m_hbm.at[b], ysem.at[2 + b]))
        mcopies[-1].start()
    rcopy = pltpu.make_async_copy(rs_out.at[1], rs_hbm, ysem.at[4])
    rcopy.start()
    with jax.named_scope("tail"):
        hcopies = [pltpu.make_async_copy(x.at[pl.ds(b * 128, 128)], h_hbm.at[pl.ds(b * 128, 128)], ysem.at[b]) for b in range(2)]
        for c in [vcopy, kcopy, rcopy] + hcopies + mcopies:
            c.wait()


def finish_kernel(rs_hbm, gm_hbm, h_hbm, m_hbm, k_in, v_in, y_hbm, k_out, v_out, rs, gm, h, m, kb, vb, isem, msem, hsem, osem, ysem):
    copies = [pltpu.make_async_copy(src, dst, isem.at[i]) for i, (src, dst) in enumerate(((rs_hbm, rs), (gm_hbm, gm), (k_in, kb), (v_in, vb)))]
    for c in copies[:2]:
        c.start()

    def inputs(c):
        return [pltpu.make_async_copy(m_hbm.at[:, c], m.at[c], msem.at[c]), pltpu.make_async_copy(h_hbm.at[:, pl.ds(c * 512, 512)], h.at[:, pl.ds(c * 512, 512)], hsem.at[c])]

    for c in range(10):
        for d in inputs(c):
            d.start()
    for c in copies[2:]:
        c.start()
    copies[0].wait()
    copies[1].wait()
    out = []
    for c in range(10):
        for d in inputs(c):
            d.wait()
        for b in range(2):
            rows = pl.ds(b * 128, 128)
            for w in range(4):
                cs = pl.ds(c * 512 + w * 128, 128)
                g = gm[c * 4 + w:c * 4 + w + 1, :].astype(F32)
                h[rows, cs] = (h[rows, cs].astype(F32) + m[c, b, :, pl.ds(w * 128, 128)].astype(F32) * rs[rows, :] * g).astype(BF16)
        cs = pl.ds(c * 512, 512)
        out.append(pltpu.make_async_copy(h.at[:, cs], y_hbm.at[:, cs], ysem.at[c]))
        out[-1].start()
    for i, (src, dst) in enumerate(((kb, k_out), (vb, v_out))):
        copies[2 + i].wait()
        out.append(pltpu.make_async_copy(src, dst, osem.at[i]))
        out[-1].start()
    for d in out:
        d.wait()


def solution(mesh):
    def local_layer(tokens, seq_lens, w_q, w_k, w_v, w_o, g_q, g_k, g_attn, g_mlp, w_gate, w_up, w_down):
        cos_tab, sin_tab = rope_tables(128)
        hbm = pl.BlockSpec(memory_space=pl.ANY)
        gain = lambda g: g.reshape(-1, 128)
        dma = pltpu.SemaphoreType.DMA
        cache = jax.ShapeDtypeStruct((2, 10, 128, 128), BF16)
        hidden = jax.ShapeDtypeStruct((256, 5120), BF16)
        h, m, rs, kc, vc = pl.pallas_call(
            layer_kernel,
            out_shape=(hidden, jax.ShapeDtypeStruct((2, 10, 128, 512), BF16), jax.ShapeDtypeStruct((256, 128), F32), cache, cache),
            in_specs=[pl.BlockSpec(memory_space=pltpu.SMEM)] + [hbm] * 13,
            out_specs=(hbm,) * 5,
            scratch_shapes=[
                pltpu.VMEM((RING + KEEP, 5120, 256), BF16),
                pltpu.VMEM((256, 5120), BF16),
                pltpu.VMEM((2, 10, 128, 128), F32),
                pltpu.VMEM((2, 10, 128, 128), F32),
                pltpu.VMEM((2, 10, 128, 128), BF16),
                pltpu.VMEM((2, 10, 128, 128), BF16),
                pltpu.VMEM((10, 128, 128), BF16),
                pltpu.VMEM((256, 1280), BF16),
                pltpu.VMEM((128, 3456), BF16),
                pltpu.VMEM((2, 128, 512), F32),
                pltpu.VMEM((2, 256, 128), F32),
                pltpu.VMEM((2, 256, 128), F32),
                pltpu.VMEM((8, 256), F32),
                pltpu.VMEM((3, 8, 256), F32),
                pltpu.VMEM((2, 5, 128, 512), BF16),
                pltpu.VMEM((2, 5, 128, 512), BF16),
                pltpu.VMEM((2, 5, 128, 512), BF16),
                pltpu.VMEM((2, 2, 5, 128, 512), BF16),
                pltpu.VMEM((2, 10, 128, 512), BF16),
                pltpu.VMEM((2, 2, 128, 128), F32),
                pltpu.VMEM((2, 256, 128), F32),
                pltpu.VMEM((128, 128), F32),
                pltpu.VMEM((128, 128), F32),
                pltpu.VMEM((10, 128), BF16),
                pltpu.VMEM((10, 128), BF16),
                pltpu.VMEM((40, 128), BF16),
                pltpu.VMEM((10, 128), F32),
                pltpu.VMEM((10, 128), F32),
                pltpu.VMEM((40, 128), F32),
                dma((RING + KEEP,)), dma, dma((2,)), dma((5,)), dma((3,)), dma((3,)), dma((2, 2, 6, 5)), dma((5,)),
            ],
            compiler_params=pltpu.CompilerParams(collective_id=0, has_side_effects=True, vmem_limit_bytes=67043328),
        )(seq_lens, jnp.asarray(cos_tab), jnp.asarray(sin_tab), gain(g_q), gain(g_k), gain(g_attn),
          tokens.reshape(256, 5120), w_q, w_k, w_v, w_o, w_gate, w_up, w_down)
        y, kc, vc = pl.pallas_call(
            finish_kernel,
            out_shape=(hidden, cache, cache),
            in_specs=[hbm] * 6,
            out_specs=(hbm,) * 3,
            scratch_shapes=[
                pltpu.VMEM((256, 128), F32),
                pltpu.VMEM((40, 128), BF16),
                pltpu.VMEM((256, 5120), BF16),
                pltpu.VMEM((10, 2, 128, 512), BF16),
                pltpu.VMEM((2, 10, 128, 128), BF16),
                pltpu.VMEM((2, 10, 128, 128), BF16),
                dma((4,)), dma((10,)), dma((10,)), dma((2,)), dma((10,)),
            ],
            compiler_params=pltpu.CompilerParams(vmem_limit_bytes=60000000),
        )(rs, gain(g_mlp), h, m, kc, vc)
        return y.reshape(2, 128, 5120), kc, vc

    return jax.shard_map(local_layer, mesh=mesh, in_specs=(P('dp', None, None), P('dp'), P(None, 'tp'), P(None, 'tp'), P(None, 'tp'), P('tp', None), P('tp'), P('tp'), P(), P(), P(None, 'tp'), P(None, 'tp'), P('tp', None)), out_specs=(P('dp', None, None), P('dp', 'tp', None, None), P('dp', 'tp', None, None)), check_vma=False)
```

```python
import jax
import jax.numpy as jnp
import numpy as np
from jax import lax
from jax.experimental import pallas as pl
from jax.experimental.pallas import tpu as pltpu
from jax.sharding import PartitionSpec as P

HEAD_DIM = 128
ROPE_BASE = 500000.0
NORM_EPS = 1e-6
F32 = jnp.float32
BF16 = jnp.bfloat16

WIDTH = 5120
RING = 6
KEEP = 12
N_V, N_QKV = 10, 15
N_G = 27
N_RG = N_G - KEEP
N_MLP = N_RG + 20


def rope_tables(seq_len):
    half = HEAD_DIM // 2
    inv_freq = (ROPE_BASE ** (-2.0 * np.arange(half) / HEAD_DIM)).astype(np.float32)
    angles = np.arange(seq_len, dtype=np.float32)[:, None] * inv_freq[None, :]
    cos, sin = np.cos(angles), np.sin(angles)
    return (np.concatenate([cos, cos], -1).astype(np.float32), np.concatenate([-sin, sin], -1).astype(np.float32))


def cols(start, size):
    return pl.ds(pl.multiple_of(start, size), size)


def dot(a, b):
    return jnp.dot(a, b, preferred_element_type=F32)


def layer_kernel(seq_ref, cos_hbm, sin_hbm, gq_hbm, gk_hbm, ga_hbm,
                 x_hbm, wq, wk, wv, wo, wg, wu, wd,
                 h_hbm, m_hbm, rs_hbm, kc_hbm, vc_hbm,
                 pool, x, qk, kb, vb, act, rsc, ssq_send, ssq_recv,
                 sends, rs_recv, xs_recv, other, rs_out,
                 cos_ref, sin_ref, gq16, gk16, ga16, gq_ref, gk_ref, ga_ref,
                 wsem, xsem, csem, ysem, ssq_s, ssq_r, arsem, tsem):
    t = lax.axis_index("tp")
    core = lax.rem(t, 2)
    sib = t + 1 - 2 * core
    xpeer = lax.rem(t + 2, 4)
    diag = 3 - t

    def load(src, dst, slot):
        pltpu.make_async_copy(src, dst, wsem.at[slot]).start()

    def load_qk(n):
        slot = lax.rem(n, RING)

        @pl.when(lax.rem(n, 2) == 0)
        def _():
            load(wq.at[:, cols((n // 2) * 256, 256)], pool.at[slot], slot)

        @pl.when(lax.rem(n, 2) == 1)
        def _():
            load(wk.at[:, cols((n // 2) * 256, 256)], pool.at[slot], slot)

    def load_v(n):
        slot = lax.rem(n, RING)
        load(wv.at[:, cols((n - N_V) * 256, 256)], pool.at[slot], slot)

    def load_o(j):
        slot = RING + j
        for k in range(4):
            half = core if k // 2 else 1 - core
            load(wo.at[:, cols(half * 2560 + j * 512 + (k % 2) * 256, 256)], pool.at[slot, pl.ds(k * 1280, 1280), :], slot)

    def load_g(k, slot):
        @pl.when(jnp.logical_and(lax.rem(k, 2) == 0, k < N_G - 1))
        def _():
            load(wg.at[:, cols((k // 2) * 256, 256)], pool.at[slot], slot)

        @pl.when(lax.rem(k, 2) == 1)
        def _():
            load(wu.at[:, cols((k // 2) * 256, 256)], pool.at[slot], slot)

        @pl.when(k == N_G - 1)
        def _():
            load(wg.at[:, pl.ds(3328, 128)], pool.at[slot, :, pl.ds(0, 128)], slot)
            load(wu.at[:, pl.ds(3328, 128)], pool.at[slot, :, pl.ds(128, 128)], slot)

    def keep_slot(k):
        return RING + lax.rem(k + 5, KEEP)

    def ring_slot(b, l):
        return lax.rem(N_QKV + N_MLP * b + l, RING)

    def load_ring(b, l, lo, hi):
        slot = ring_slot(b, l)

        def g():
            load_g(KEEP + l, slot)

        def d():
            q = l - N_RG
            half = lax.rem(lax.rem(q, 4) // 2 + 1 + core, 2)
            load(wd.at[:, cols(half * 2560 + (q // 4) * 512 + lax.rem(q, 2) * 256, 256)], pool.at[slot, pl.ds(0, 3456), :], slot)

        def nxt():
            load_g(KEEP + l - N_MLP, slot)

        for start, end, fn in ((0, N_RG, g), (N_RG, N_MLP, d), (N_MLP, 2 * N_MLP, nxt if b == 0 else None)):
            if fn is None or hi < start or lo >= end:
                continue
            if lo >= start and hi < end:
                fn()
            else:
                pl.when(jnp.logical_and(l >= start, l < end))(fn)

    def wait_slot(slot, rows=WIDTH):
        src = wq if rows == WIDTH else wd
        pltpu.make_async_copy(src.at[:, pl.ds(0, 256)], pool.at[slot, pl.ds(0, rows), :], wsem.at[slot]).wait()

    def i32(v):
        return jnp.int32(v)

    xcopy = pltpu.make_async_copy(x_hbm, x, xsem)
    xcopy.start()
    for n in range(2):
        load_qk(i32(n))
    small = [pltpu.make_async_copy(src, dst, tsem.at[i]) for i, (src, dst) in enumerate(
        ((cos_hbm, cos_ref), (sin_hbm, sin_ref), (gq_hbm, gq16), (gk_hbm, gk16), (ga_hbm, ga16)))]
    for c in small:
        c.start()

    barrier = pltpu.get_barrier_semaphore()
    for peer in (sib, xpeer, diag):
        pl.semaphore_signal(barrier, inc=1, device_id={"tp": peer}, device_id_type=pl.DeviceIdType.MESH)

    def remote(src, dst, ssem, rsem, peer):
        return pltpu.make_async_remote_copy(src_ref=src, dst_ref=dst, send_sem=ssem, recv_sem=rsem,
                                            device_id={"tp": peer}, device_id_type=pl.DeviceIdType.MESH)

    rsc[...] = jnp.zeros_like(rsc)
    xcopy.wait()
    for n in range(2, 4):
        load_qk(i32(n))

    def qk_step(i, carry):
        n = 2 * i
        s0, s1 = lax.rem(n, RING), lax.rem(n + 1, RING)
        wait_slot(s0)
        wait_slot(s1)
        for m in (n + 4, n + 5):
            pl.when(m < N_V)(lambda m=m: load_qk(m))
            pl.when(m >= N_V)(lambda m=m: load_v(m))
        q = dot(x[...], pool[s0])
        k = dot(x[...], pool[s1])
        for b in range(2):
            for hh in range(2):
                qk[b, 2 * i + hh] = q[b * 128:(b + 1) * 128, hh * 128:(hh + 1) * 128]
                qk[b, 10 + 2 * i + hh] = k[b * 128:(b + 1) * 128, hh * 128:(hh + 1) * 128]
        rsc[0] += q[:, :128] * q[:, :128] + q[:, 128:] * q[:, 128:]
        rsc[1] += k[:, :128] * k[:, :128] + k[:, 128:] * k[:, 128:]
        return carry

    with jax.named_scope("qk"):
        lax.fori_loop(0, 5, qk_step, 0)
    load_v(i32(14))
    load_o(0)

    for r in range(2):
        ssq_send[r:r + 1, :] = jnp.sum(jnp.transpose(rsc[r]), axis=0, keepdims=True)
    ssq_send[2:8, :] = jnp.zeros((6, 256), F32)
    with jax.named_scope("barrier"):
        pl.semaphore_wait(barrier, 3)
    ssq_copies = [remote(ssq_send, ssq_recv.at[j], ssq_s.at[j], ssq_r.at[j], peer) for j, peer in enumerate((sib, xpeer, diag))]
    for c in ssq_copies:
        c.start()

    with jax.named_scope("v"):
        for group in ((10, 11), (12, 13), (14,)):
            for n in group:
                wait_slot(n % RING)
            if group[0] == 10:
                load_o(1)
                load_o(2)
            elif group[0] == 12:
                load_o(3)
                load_o(4)
            else:
                for k in range(KEEP - 5):
                    load_g(i32(k), keep_slot(i32(k)))
            vals = [dot(x[...], pool[n % RING]).astype(BF16) for n in group]
            for n, v in zip(group, vals):
                for b in range(2):
                    for hh in range(2):
                        vb[b, 2 * (n - N_V) + hh] = v[b * 128:(b + 1) * 128, hh * 128:(hh + 1) * 128]
    vcopy = pltpu.make_async_copy(vb, vc_hbm, csem.at[0])
    vcopy.start()
    for l in range(RING):
        load_ring(0, i32(l), l, l)

    with jax.named_scope("ssqwait"):
        for c in ssq_copies:
            c.wait()
    for c in small:
        c.wait()
    for src, dst in ((gq16, gq_ref), (gk16, gk_ref), (ga16, ga_ref)):
        dst[...] = src[...].astype(F32)
    total = ssq_send[...] + ssq_recv[0] + ssq_recv[1] + ssq_recv[2]
    scale = lax.rsqrt(total * (1.0 / WIDTH) + NORM_EPS)
    for r in range(2):
        rsc[r] = jnp.transpose(jnp.broadcast_to(scale[r:r + 1, :], (128, 256)))

    def rope(v):
        return (v * cos_ref[...] + pltpu.roll(v, 64, 1) * sin_ref[...]).astype(BF16)

    def qb(h):
        return act.at[:, pl.ds(h * 128, 128)]

    def attention(b):
        rows = pl.ds(b * 128, 128)
        row = lax.broadcasted_iota(jnp.int32, (128, 128), 0)
        col = lax.broadcasted_iota(jnp.int32, (128, 128), 1)
        allowed = jnp.logical_and(col <= row, col < seq_ref[b])
        for h in range(10):
            qb(h)[...] = rope(qk[b, h] * rsc[0, rows, :] * gq_ref[h:h + 1, :])
            kb[b, h] = rope(qk[b, 10 + h] * rsc[1, rows, :] * gk_ref[h:h + 1, :])
        for h in range(10):
            qk[b, h] = lax.dot_general(qb(h)[...], kb[b, h], (((1,), (1,)), ((), ())), preferred_element_type=F32)
        for h in range(10):
            s = jnp.where(allowed, qk[b, h] * HEAD_DIM ** -0.5, -1e30)
            e = jnp.exp(s - jnp.max(s, axis=-1, keepdims=True))
            qb(h)[...] = (e / jnp.sum(e, axis=-1, keepdims=True)).astype(BF16)
        for h in range(10):
            act[:, pl.ds(1280 + h * 128, 128)] = dot(qb(h)[...], vb[b, h]).astype(BF16)

    def rs_copy(p, b, j):
        return remote(sends.at[b, j], rs_recv.at[b, j], arsem.at[p, b, 0, j], arsem.at[p, b, 1, j], sib)

    def xs_copy(p, b, j):
        return remote(sends.at[b, j], xs_recv.at[p, b, j], arsem.at[p, b, 2, j], arsem.at[p, b, 3, j], xpeer)

    def ag_copy(p, b, j):
        return remote(xs_recv.at[p, b, j], other.at[b, j], arsem.at[p, b, 4, j], arsem.at[p, b, 5, j], sib)

    def send_sib(p, b, j, parts):
        for k in range(2):
            sends[b, j, :, pl.ds(k * 256, 256)] = parts[k].astype(BF16)
        rs_copy(p, b, j).start()

    def keep_own(j, parts):
        for k in range(4):
            qk[0, lax.rem(j, 3) * 4 + k] = parts[k // 2][:, (k % 2) * 128:(k % 2 + 1) * 128]

    def chip_sum(p, b, j):
        rs_copy(p, b, j).wait()
        for k in range(4):
            cs = pl.ds(k * 128, 128)
            sends[b, j, :, cs] = (qk[0, lax.rem(j, 3) * 4 + k] + rs_recv[b, j, :, cs].astype(F32)).astype(BF16)
        if (p, b) != (0, 1):
            xs_copy(p, b, j).start()

    def add_squares(half, b, v):
        v = v.astype(F32)
        rsc[half, pl.ds(b * 128, 128), :] += v[:, :128] * v[:, :128] + v[:, 128:256] * v[:, 128:256] + v[:, 256:384] * v[:, 256:384] + v[:, 384:] * v[:, 384:]

    def gather(p, b):
        for half in range(2):
            rsc[half, pl.ds(b * 128, 128), :] = jnp.zeros((128, 128), F32)

        def step(j, carry):
            with jax.named_scope(f"xwait{p}{b}"):
                xs_copy(p, b, j).wait()
            v = (sends[b, j].astype(F32) + xs_recv[p, b, j].astype(F32)).astype(BF16)
            xs_recv[p, b, j] = v
            ag_copy(p, b, j).start()
            add_squares(0, b, v)
            if (p, b) == (0, 0):
                @pl.when(j == 3)
                def _():
                    for c in range(5):
                        xs_copy(0, 1, c).start()
            return carry

        lax.fori_loop(0, 5, step, 0)

    def arrive(p, b):
        def step(j, carry):
            ag_copy(p, b, j).wait()
            add_squares(1, b, other[b, j])
            return carry

        lax.fori_loop(0, 5, step, 0)
        rs = lax.rsqrt(jnp.sum(rsc[0, pl.ds(b * 128, 128), :] + rsc[1, pl.ds(b * 128, 128), :], axis=-1, keepdims=True) * (1.0 / WIDTH) + NORM_EPS)
        rs_out[p, pl.ds(b * 128, 128), :] = jnp.broadcast_to(rs, (128, 128))

    def norm_hidden(b):
        rows = pl.ds(b * 128, 128)

        def apply(j, carry):
            for half, ref in ((core, xs_recv.at[0]), (1 - core, other)):
                for w in range(4):
                    cs = cols(half * 2560 + j * 512 + w * 128, 128)
                    gain = ga_ref[pl.ds(half * 20 + j * 4 + w, 1), :]
                    x[rows, cs] = (x[rows, cs].astype(F32) + ref[b, j, :, pl.ds(w * 128, 128)].astype(F32) * rs_out[0, rows, :] * gain).astype(BF16)
            return carry

        lax.fori_loop(0, 5, apply, 0)
        pltpu.make_async_copy(x.at[rows], h_hbm.at[rows], ysem.at[b]).start()

    def project(b):
        def step(j, carry):
            slot = RING + j
            if b == 0:
                wait_slot(slot)
            parts = [dot(act[:, pl.ds(1280, 1280)], pool[slot, pl.ds(k * 1280, 1280), :]) for k in range(4)]
            send_sib(0, b, j, parts[:2])
            keep_own(j, parts[2:])
            pl.when(j > 1)(lambda: chip_sum(0, b, j - 2))
            return carry

        lax.fori_loop(0, 5, step, 0)
        chip_sum(0, b, i32(3))
        chip_sum(0, b, i32(4))

    for b in range(2):
        with jax.named_scope(f"attn{b}"):
            attention(b)
        with jax.named_scope(f"o{b}"):
            project(b)
    kcopy = pltpu.make_async_copy(kb, kc_hbm, csem.at[1])
    kcopy.start()
    for k in range(KEEP - 5, KEEP):
        load_g(i32(k), keep_slot(i32(k)))

    def gu_store(i, g, u):
        act[:, cols(i * 256, 256)] = (g * jax.nn.sigmoid(g) * u).astype(BF16)

    def gu_keep(b):
        def step(i, carry):
            s0, s1 = keep_slot(2 * i), keep_slot(2 * i + 1)
            if b == 0:
                wait_slot(s0)
                wait_slot(s1)
            xb = x[pl.ds(b * 128, 128), :]
            gu_store(i, dot(xb, pool[s0]), dot(xb, pool[s1]))
            return carry

        with jax.named_scope(f"gukeep{b}"):
            lax.fori_loop(0, KEEP // 2, step, 0)

    def gu_ring(b):
        def step(i, carry):
            l = 2 * i
            s0, s1 = ring_slot(b, l), ring_slot(b, l + 1)
            wait_slot(s0)
            wait_slot(s1)
            xb = x[pl.ds(b * 128, 128), :]
            gu_store(i + KEEP // 2, dot(xb, pool[s0]), dot(xb, pool[s1]))
            load_ring(b, l + RING, RING, N_RG - 3 + RING)
            load_ring(b, l + 1 + RING, 1 + RING, N_RG - 2 + RING)
            return carry

        with jax.named_scope(f"guring{b}"):
            lax.fori_loop(0, N_RG // 2, step, 0)
        l = N_RG - 1
        s0 = (N_QKV + N_MLP * b + l) % RING
        wait_slot(s0)
        r = dot(x[pl.ds(b * 128, 128), :], pool[s0])
        g = r[:, :128]
        act[:, 3328:3456] = (g * jax.nn.sigmoid(g) * r[:, 128:]).astype(BF16)
        load_ring(b, i32(l + RING), l + RING, l + RING)

    def down(b):
        def blocks(first):
            slots = [ring_slot(b, first + k) for k in range(2)]
            for sl in slots:
                wait_slot(sl, 3456)
            return [dot(act[...], pool[sl, pl.ds(0, 3456), :]) for sl in slots]

        def refill(first):
            for k in range(2):
                l = first + k + RING
                if b == 0:
                    load_ring(b, l, N_RG + RING, N_MLP - 1 + RING)
                else:
                    pl.when(l < N_MLP)(lambda l=l: load_ring(b, l, N_RG + RING, N_MLP - 1))

        def step(j, carry):
            l = N_RG + 4 * j
            send_sib(1, b, j, blocks(l))
            refill(l)
            keep_own(j, blocks(l + 2))
            refill(l + 2)
            chip_sum(1, b, j)
            return carry

        with jax.named_scope(f"d{b}"):
            lax.fori_loop(0, 5, step, 0)

    with jax.named_scope("gather00"):
        gather(0, 0)
    with jax.named_scope("norm00"):
        arrive(0, 0)
        norm_hidden(0)
    gu_ring(0)
    gu_keep(0)
    with jax.named_scope("gather01"):
        gather(0, 1)
    down(0)
    with jax.named_scope("norm01"):
        arrive(0, 1)
        norm_hidden(1)
    gu_ring(1)
    gu_keep(1)
    with jax.named_scope("gather10"):
        gather(1, 0)
    down(1)
    mcopies = []
    for b in range(2):
        if b == 1:
            with jax.named_scope("gather11"):
                gather(1, 1)
        with jax.named_scope(f"arrive1{b}"):
            arrive(1, b)
        for half, ref in ((core, xs_recv.at[1, b]), (1 - core, other.at[b])):
            mcopies.append(pltpu.make_async_copy(ref, m_hbm.at[b, pl.ds(half * 5, 5)], ysem.at[3 + len(mcopies)]))
            mcopies[-1].start()
    rcopy = pltpu.make_async_copy(rs_out.at[1], rs_hbm, ysem.at[2])
    rcopy.start()
    with jax.named_scope("tail"):
        hcopies = [pltpu.make_async_copy(x.at[pl.ds(b * 128, 128)], h_hbm.at[pl.ds(b * 128, 128)], ysem.at[b]) for b in range(2)]
        for c in [vcopy, kcopy, rcopy] + hcopies + mcopies:
            c.wait()


def finish_kernel(rs_hbm, gm_hbm, h_hbm, m_hbm, k_in, v_in, y_hbm, k_out, v_out, rs, gm, h, m, kb, vb, isem, msem, hsem, osem, ysem):
    copies = [pltpu.make_async_copy(src, dst, isem.at[i]) for i, (src, dst) in enumerate(((rs_hbm, rs), (gm_hbm, gm), (k_in, kb), (v_in, vb)))]
    for c in copies[:2]:
        c.start()

    def inputs(c):
        return [pltpu.make_async_copy(m_hbm.at[:, c], m.at[c], msem.at[c]), pltpu.make_async_copy(h_hbm.at[:, pl.ds(c * 512, 512)], h.at[:, pl.ds(c * 512, 512)], hsem.at[c])]

    for c in range(10):
        for d in inputs(c):
            d.start()
    for c in copies[2:]:
        c.start()
    copies[0].wait()
    copies[1].wait()
    out = []
    for c in range(10):
        for d in inputs(c):
            d.wait()
        for b in range(2):
            rows = pl.ds(b * 128, 128)
            for w in range(4):
                cs = pl.ds(c * 512 + w * 128, 128)
                g = gm[c * 4 + w:c * 4 + w + 1, :].astype(F32)
                h[rows, cs] = (h[rows, cs].astype(F32) + m[c, b, :, pl.ds(w * 128, 128)].astype(F32) * rs[rows, :] * g).astype(BF16)
        cs = pl.ds(c * 512, 512)
        out.append(pltpu.make_async_copy(h.at[:, cs], y_hbm.at[:, cs], ysem.at[c]))
        out[-1].start()
    for i, (src, dst) in enumerate(((kb, k_out), (vb, v_out))):
        copies[2 + i].wait()
        out.append(pltpu.make_async_copy(src, dst, osem.at[i]))
        out[-1].start()
    for d in out:
        d.wait()


def solution(mesh):
    def local_layer(tokens, seq_lens, w_q, w_k, w_v, w_o, g_q, g_k, g_attn, g_mlp, w_gate, w_up, w_down):
        cos_tab, sin_tab = rope_tables(128)
        hbm = pl.BlockSpec(memory_space=pl.ANY)
        gain = lambda g: g.reshape(-1, 128)
        dma = pltpu.SemaphoreType.DMA
        cache = jax.ShapeDtypeStruct((2, 10, 128, 128), BF16)
        hidden = jax.ShapeDtypeStruct((256, 5120), BF16)
        h, m, rs, kc, vc = pl.pallas_call(
            layer_kernel,
            out_shape=(hidden, jax.ShapeDtypeStruct((2, 10, 128, 512), BF16), jax.ShapeDtypeStruct((256, 128), F32), cache, cache),
            in_specs=[pl.BlockSpec(memory_space=pltpu.SMEM)] + [hbm] * 13,
            out_specs=(hbm,) * 5,
            scratch_shapes=[
                pltpu.VMEM((RING + KEEP, 5120, 256), BF16),
                pltpu.VMEM((256, 5120), BF16),
                pltpu.VMEM((2, 20, 128, 128), F32),
                pltpu.VMEM((2, 10, 128, 128), BF16),
                pltpu.VMEM((2, 10, 128, 128), BF16),
                pltpu.VMEM((128, 3456), BF16),
                pltpu.VMEM((2, 256, 128), F32),
                pltpu.VMEM((8, 256), F32),
                pltpu.VMEM((3, 8, 256), F32),
                pltpu.VMEM((2, 5, 128, 512), BF16),
                pltpu.VMEM((2, 5, 128, 512), BF16),
                pltpu.VMEM((2, 2, 5, 128, 512), BF16),
                pltpu.VMEM((2, 5, 128, 512), BF16),
                pltpu.VMEM((2, 256, 128), F32),
                pltpu.VMEM((128, 128), F32),
                pltpu.VMEM((128, 128), F32),
                pltpu.VMEM((10, 128), BF16),
                pltpu.VMEM((10, 128), BF16),
                pltpu.VMEM((40, 128), BF16),
                pltpu.VMEM((10, 128), F32),
                pltpu.VMEM((10, 128), F32),
                pltpu.VMEM((40, 128), F32),
                dma((RING + KEEP,)), dma, dma((2,)), dma((7,)), dma((3,)), dma((3,)), dma((2, 2, 6, 5)), dma((5,)),
            ],
            compiler_params=pltpu.CompilerParams(collective_id=0, has_side_effects=True, vmem_limit_bytes=67043328),
        )(seq_lens, jnp.asarray(cos_tab), jnp.asarray(sin_tab), gain(g_q), gain(g_k), gain(g_attn),
          tokens.reshape(256, 5120), w_q, w_k, w_v, w_o, w_gate, w_up, w_down)
        y, kc, vc = pl.pallas_call(
            finish_kernel,
            out_shape=(hidden, cache, cache),
            in_specs=[hbm] * 6,
            out_specs=(hbm,) * 3,
            scratch_shapes=[
                pltpu.VMEM((256, 128), F32),
                pltpu.VMEM((40, 128), BF16),
                pltpu.VMEM((256, 5120), BF16),
                pltpu.VMEM((10, 2, 128, 512), BF16),
                pltpu.VMEM((2, 10, 128, 128), BF16),
                pltpu.VMEM((2, 10, 128, 128), BF16),
                dma((4,)), dma((10,)), dma((10,)), dma((2,)), dma((10,)),
            ],
            compiler_params=pltpu.CompilerParams(vmem_limit_bytes=60000000),
        )(rs, gain(g_mlp), h, m, kc, vc)
        return y.reshape(2, 128, 5120), kc, vc

    return jax.shard_map(local_layer, mesh=mesh, in_specs=(P('dp', None, None), P('dp'), P(None, 'tp'), P(None, 'tp'), P(None, 'tp'), P('tp', None), P('tp'), P('tp'), P(), P(), P(None, 'tp'), P(None, 'tp'), P('tp', None)), out_specs=(P('dp', None, None), P('dp', 'tp', None, None), P('dp', 'tp', None, None)), check_vma=False)
```

```python
import jax
import jax.numpy as jnp
import numpy as np
from jax import lax
from jax.experimental import pallas as pl
from jax.experimental.pallas import tpu as pltpu
from jax.sharding import PartitionSpec as P

HEAD_DIM = 128
ROPE_BASE = 500000.0
NORM_EPS = 1e-6
F32 = jnp.float32
BF16 = jnp.bfloat16

WIDTH = 5120
RING = 6
KEEP = 12
N_V, N_QKV = 10, 15
N_G = 27
N_RG = N_G - KEEP
N_MLP = N_RG + 20


def rope_tables(seq_len):
    half = HEAD_DIM // 2
    inv_freq = (ROPE_BASE ** (-2.0 * np.arange(half) / HEAD_DIM)).astype(np.float32)
    angles = np.arange(seq_len, dtype=np.float32)[:, None] * inv_freq[None, :]
    cos, sin = np.cos(angles), np.sin(angles)
    return (np.concatenate([cos, cos], -1).astype(np.float32), np.concatenate([-sin, sin], -1).astype(np.float32))


def cols(start, size):
    return pl.ds(pl.multiple_of(start, size), size)


def dot(a, b):
    return jnp.dot(a, b, preferred_element_type=F32)


def layer_kernel(seq_ref, cos_hbm, sin_hbm, gq_hbm, gk_hbm, ga_hbm,
                 x_hbm, wq, wk, wv, wo, wg, wu, wd,
                 h_hbm, m_hbm, rs_hbm, kc_hbm, vc_hbm,
                 pool, x, qk, kb, vb, act, rsc, ssq_send, ssq_recv,
                 sends, rs_recv, xs_recv, other, rs_out,
                 cos_ref, sin_ref, gq16, gk16, ga16, gq_ref, gk_ref, ga_ref,
                 wsem, xsem, csem, ysem, ssq_s, ssq_r, arsem, tsem):
    t = lax.axis_index("tp")
    core = lax.rem(t, 2)
    sib = t + 1 - 2 * core
    xpeer = lax.rem(t + 2, 4)
    diag = 3 - t

    def load(src, dst, slot):
        pltpu.make_async_copy(src, dst, wsem.at[slot]).start()

    def load_qk(n):
        slot = lax.rem(n, RING)

        @pl.when(lax.rem(n, 2) == 0)
        def _():
            load(wq.at[:, cols((n // 2) * 256, 256)], pool.at[slot], slot)

        @pl.when(lax.rem(n, 2) == 1)
        def _():
            load(wk.at[:, cols((n // 2) * 256, 256)], pool.at[slot], slot)

    def load_v(n):
        slot = lax.rem(n, RING)
        load(wv.at[:, cols((n - N_V) * 256, 256)], pool.at[slot], slot)

    def load_o(j):
        slot = RING + j
        for k in range(4):
            half = core if k // 2 else 1 - core
            load(wo.at[:, cols(half * 2560 + j * 512 + (k % 2) * 256, 256)], pool.at[slot, pl.ds(k * 1280, 1280), :], slot)

    def load_g(k, slot):
        @pl.when(jnp.logical_and(lax.rem(k, 2) == 0, k < N_G - 1))
        def _():
            load(wg.at[:, cols((k // 2) * 256, 256)], pool.at[slot], slot)

        @pl.when(lax.rem(k, 2) == 1)
        def _():
            load(wu.at[:, cols((k // 2) * 256, 256)], pool.at[slot], slot)

        @pl.when(k == N_G - 1)
        def _():
            load(wg.at[:, pl.ds(3328, 128)], pool.at[slot, :, pl.ds(0, 128)], slot)
            load(wu.at[:, pl.ds(3328, 128)], pool.at[slot, :, pl.ds(128, 128)], slot)

    def keep_slot(k):
        return RING + lax.rem(k + 5, KEEP)

    def ring_slot(b, l):
        return lax.rem(N_QKV + N_MLP * b + l, RING)

    def load_ring(b, l, lo, hi):
        slot = ring_slot(b, l)

        def g():
            load_g(KEEP + l, slot)

        def d():
            q = l - N_RG
            half = lax.rem(lax.rem(q, 4) // 2 + 1 + core, 2)
            load(wd.at[:, cols(half * 2560 + (q // 4) * 512 + lax.rem(q, 2) * 256, 256)], pool.at[slot, pl.ds(0, 3456), :], slot)

        def nxt():
            load_g(KEEP + l - N_MLP, slot)

        for start, end, fn in ((0, N_RG, g), (N_RG, N_MLP, d), (N_MLP, 2 * N_MLP, nxt if b == 0 else None)):
            if fn is None or hi < start or lo >= end:
                continue
            if lo >= start and hi < end:
                fn()
            else:
                pl.when(jnp.logical_and(l >= start, l < end))(fn)

    def wait_slot(slot, rows=WIDTH):
        src = wq if rows == WIDTH else wd
        pltpu.make_async_copy(src.at[:, pl.ds(0, 256)], pool.at[slot, pl.ds(0, rows), :], wsem.at[slot]).wait()

    def i32(v):
        return jnp.int32(v)

    xcopy = pltpu.make_async_copy(x_hbm, x, xsem)
    xcopy.start()
    for n in range(2):
        load_qk(i32(n))
    small = [pltpu.make_async_copy(src, dst, tsem.at[i]) for i, (src, dst) in enumerate(
        ((cos_hbm, cos_ref), (sin_hbm, sin_ref), (gq_hbm, gq16), (gk_hbm, gk16), (ga_hbm, ga16)))]
    for c in small:
        c.start()

    barrier = pltpu.get_barrier_semaphore()
    for peer in (sib, xpeer, diag):
        pl.semaphore_signal(barrier, inc=1, device_id={"tp": peer}, device_id_type=pl.DeviceIdType.MESH)

    def remote(src, dst, ssem, rsem, peer):
        return pltpu.make_async_remote_copy(src_ref=src, dst_ref=dst, send_sem=ssem, recv_sem=rsem,
                                            device_id={"tp": peer}, device_id_type=pl.DeviceIdType.MESH)

    rsc[...] = jnp.zeros_like(rsc)
    xcopy.wait()
    for n in range(2, 4):
        load_qk(i32(n))

    def qk_step(i, carry):
        n = 2 * i
        s0, s1 = lax.rem(n, RING), lax.rem(n + 1, RING)
        wait_slot(s0)
        wait_slot(s1)
        for m in (n + 4, n + 5):
            pl.when(m < N_V)(lambda m=m: load_qk(m))
            pl.when(m >= N_V)(lambda m=m: load_v(m))
        q = dot(x[...], pool[s0])
        k = dot(x[...], pool[s1])
        for b in range(2):
            for hh in range(2):
                qk[b, 2 * i + hh] = q[b * 128:(b + 1) * 128, hh * 128:(hh + 1) * 128]
                qk[b, 10 + 2 * i + hh] = k[b * 128:(b + 1) * 128, hh * 128:(hh + 1) * 128]
        rsc[0] += q[:, :128] * q[:, :128] + q[:, 128:] * q[:, 128:]
        rsc[1] += k[:, :128] * k[:, :128] + k[:, 128:] * k[:, 128:]
        return carry

    with jax.named_scope("qk"):
        lax.fori_loop(0, 5, qk_step, 0)
    load_v(i32(14))
    load_o(0)

    for r in range(2):
        ssq_send[r:r + 1, :] = jnp.sum(jnp.transpose(rsc[r]), axis=0, keepdims=True)
    ssq_send[2:8, :] = jnp.zeros((6, 256), F32)
    with jax.named_scope("barrier"):
        pl.semaphore_wait(barrier, 3)
    ssq_copies = [remote(ssq_send, ssq_recv.at[j], ssq_s.at[j], ssq_r.at[j], peer) for j, peer in enumerate((sib, xpeer, diag))]
    for c in ssq_copies:
        c.start()

    with jax.named_scope("v"):
        for group in ((10, 11), (12, 13), (14,)):
            for n in group:
                wait_slot(n % RING)
            if group[0] == 10:
                load_o(1)
                load_o(2)
            elif group[0] == 12:
                load_o(3)
                load_o(4)
            else:
                for k in range(KEEP - 5):
                    load_g(i32(k), keep_slot(i32(k)))
            vals = [dot(x[...], pool[n % RING]).astype(BF16) for n in group]
            for n, v in zip(group, vals):
                for b in range(2):
                    for hh in range(2):
                        vb[b, 2 * (n - N_V) + hh] = v[b * 128:(b + 1) * 128, hh * 128:(hh + 1) * 128]
    vcopy = pltpu.make_async_copy(vb, vc_hbm, csem.at[0])
    vcopy.start()
    for l in range(RING):
        load_ring(0, i32(l), l, l)

    with jax.named_scope("ssqwait"):
        for c in ssq_copies:
            c.wait()
    for c in small:
        c.wait()
    for src, dst in ((gq16, gq_ref), (gk16, gk_ref), (ga16, ga_ref)):
        dst[...] = src[...].astype(F32)
    total = ssq_send[...] + ssq_recv[0] + ssq_recv[1] + ssq_recv[2]
    scale = lax.rsqrt(total * (1.0 / WIDTH) + NORM_EPS)
    for r in range(2):
        rsc[r] = jnp.transpose(jnp.broadcast_to(scale[r:r + 1, :], (128, 256)))

    def rope(v):
        return (v * cos_ref[...] + pltpu.roll(v, 64, 1) * sin_ref[...]).astype(BF16)

    def qb(h):
        return act.at[:, pl.ds(h * 128, 128)]

    def attention(b):
        rows = pl.ds(b * 128, 128)
        row = lax.broadcasted_iota(jnp.int32, (128, 128), 0)
        col = lax.broadcasted_iota(jnp.int32, (128, 128), 1)
        allowed = jnp.logical_and(col <= row, col < seq_ref[b])
        for h in range(10):
            qb(h)[...] = rope(qk[b, h] * rsc[0, rows, :] * gq_ref[h:h + 1, :])
            kb[b, h] = rope(qk[b, 10 + h] * rsc[1, rows, :] * gk_ref[h:h + 1, :])
        for h in range(10):
            qk[b, h] = lax.dot_general(qb(h)[...], kb[b, h], (((1,), (1,)), ((), ())), preferred_element_type=F32)
        for h in range(10):
            s = jnp.where(allowed, qk[b, h] * HEAD_DIM ** -0.5, -1e30)
            e = jnp.exp(s - jnp.max(s, axis=-1, keepdims=True))
            qb(h)[...] = (e / jnp.sum(e, axis=-1, keepdims=True)).astype(BF16)
        for h in range(10):
            act[:, pl.ds(1280 + h * 128, 128)] = dot(qb(h)[...], vb[b, h]).astype(BF16)

    def rs_copy(p, b, j):
        return remote(sends.at[b, j], rs_recv.at[b, j], arsem.at[p, b, 0, j], arsem.at[p, b, 1, j], sib)

    def xs_copy(p, b, j):
        return remote(sends.at[b, j], xs_recv.at[p, b, j], arsem.at[p, b, 2, j], arsem.at[p, b, 3, j], xpeer)

    def ag_copy(p, b, j):
        return remote(xs_recv.at[p, b, j], other.at[b, j], arsem.at[p, b, 4, j], arsem.at[p, b, 5, j], sib)

    def send_sib(p, b, j, parts):
        for k in range(2):
            sends[b, j, :, pl.ds(k * 256, 256)] = parts[k].astype(BF16)
        rs_copy(p, b, j).start()

    def keep_own(j, parts):
        for k in range(4):
            qk[0, lax.rem(j, 3) * 4 + k] = parts[k // 2][:, (k % 2) * 128:(k % 2 + 1) * 128]

    def chip_sum(p, b, j):
        rs_copy(p, b, j).wait()
        for k in range(4):
            cs = pl.ds(k * 128, 128)
            sends[b, j, :, cs] = (qk[0, lax.rem(j, 3) * 4 + k] + rs_recv[b, j, :, cs].astype(F32)).astype(BF16)
        if (p, b) != (0, 1):
            xs_copy(p, b, j).start()

    def add_squares(half, b, v):
        v = v.astype(F32)
        rsc[half, pl.ds(b * 128, 128), :] += v[:, :128] * v[:, :128] + v[:, 128:256] * v[:, 128:256] + v[:, 256:384] * v[:, 256:384] + v[:, 384:] * v[:, 384:]

    def gather(p, b):
        for half in range(2):
            rsc[half, pl.ds(b * 128, 128), :] = jnp.zeros((128, 128), F32)

        def step(j, carry):
            with jax.named_scope(f"xwait{p}{b}"):
                xs_copy(p, b, j).wait()
            v = (sends[b, j].astype(F32) + xs_recv[p, b, j].astype(F32)).astype(BF16)
            xs_recv[p, b, j] = v
            ag_copy(p, b, j).start()
            add_squares(0, b, v)
            if (p, b) == (0, 0):
                @pl.when(j == 3)
                def _():
                    for c in range(5):
                        xs_copy(0, 1, c).start()
            return carry

        lax.fori_loop(0, 5, step, 0)

    def arrive(p, b):
        def step(j, carry):
            ag_copy(p, b, j).wait()
            add_squares(1, b, other[b, j])
            return carry

        lax.fori_loop(0, 5, step, 0)
        rs = lax.rsqrt(jnp.sum(rsc[0, pl.ds(b * 128, 128), :] + rsc[1, pl.ds(b * 128, 128), :], axis=-1, keepdims=True) * (1.0 / WIDTH) + NORM_EPS)
        rs_out[p, pl.ds(b * 128, 128), :] = jnp.broadcast_to(rs, (128, 128))

    def norm_hidden(b):
        rows = pl.ds(b * 128, 128)

        def apply(j, carry):
            for half, ref in ((core, xs_recv.at[0]), (1 - core, other)):
                for w in range(4):
                    cs = cols(half * 2560 + j * 512 + w * 128, 128)
                    gain = ga_ref[pl.ds(half * 20 + j * 4 + w, 1), :]
                    x[rows, cs] = (x[rows, cs].astype(F32) + ref[b, j, :, pl.ds(w * 128, 128)].astype(F32) * rs_out[0, rows, :] * gain).astype(BF16)
            return carry

        lax.fori_loop(0, 5, apply, 0)
        pltpu.make_async_copy(x.at[rows], h_hbm.at[rows], ysem.at[b]).start()

    def project(b):
        def step(j, carry):
            slot = RING + j
            if b == 0:
                wait_slot(slot)
            parts = [dot(act[:, pl.ds(1280, 1280)], pool[slot, pl.ds(k * 1280, 1280), :]) for k in range(4)]
            send_sib(0, b, j, parts[:2])
            keep_own(j, parts[2:])
            pl.when(j > 1)(lambda: chip_sum(0, b, j - 2))
            return carry

        lax.fori_loop(0, 5, step, 0)
        chip_sum(0, b, i32(3))
        chip_sum(0, b, i32(4))

    for b in range(2):
        with jax.named_scope(f"attn{b}"):
            attention(b)
        with jax.named_scope(f"o{b}"):
            project(b)
    kcopy = pltpu.make_async_copy(kb, kc_hbm, csem.at[1])
    kcopy.start()
    for k in range(KEEP - 5, KEEP):
        load_g(i32(k), keep_slot(i32(k)))

    def gu_store(i, g, u):
        act[:, cols(i * 256, 256)] = (g * jax.nn.sigmoid(g) * u).astype(BF16)

    def gate_up(b):
        xb = x.at[pl.ds(b * 128, 128)]

        def ring_pair(l):
            s0, s1 = ring_slot(b, l), ring_slot(b, l + 1)
            wait_slot(s0)
            wait_slot(s1)
            return s0, s1

        def step(i, carry):
            l = 2 * i
            s0, s1 = ring_pair(l)
            k0, k1 = keep_slot(2 * i), keep_slot(2 * i + 1)
            if b == 0:
                wait_slot(k0)
                wait_slot(k1)
            gu_store(i + KEEP // 2, dot(xb[...], pool[s0]), dot(xb[...], pool[s1]))
            gu_store(i, dot(xb[...], pool[k0]), dot(xb[...], pool[k1]))
            load_ring(b, l + RING, RING, KEEP - 2 + RING)
            load_ring(b, l + 1 + RING, 1 + RING, KEEP - 1 + RING)
            return carry

        with jax.named_scope(f"gu{b}"):
            lax.fori_loop(0, KEEP // 2, step, 0)
            s0, s1 = ring_pair(i32(N_RG - 3))
            s2 = ring_slot(b, i32(N_RG - 1))
            wait_slot(s2)
            gu_store(i32(N_G // 2 - 1), dot(xb[...], pool[s0]), dot(xb[...], pool[s1]))
            r = dot(xb[...], pool[s2])
            g = r[:, :128]
            act[:, 3328:3456] = (g * jax.nn.sigmoid(g) * r[:, 128:]).astype(BF16)
            for l in range(N_RG - 3, N_RG):
                load_ring(b, i32(l + RING), l + RING, l + RING)

    def down(b):
        def blocks(first):
            slots = [ring_slot(b, first + k) for k in range(2)]
            for sl in slots:
                wait_slot(sl, 3456)
            return [dot(act[...], pool[sl, pl.ds(0, 3456), :]) for sl in slots]

        def refill(first):
            for k in range(2):
                l = first + k + RING
                if b == 0:
                    load_ring(b, l, N_RG + RING, N_MLP - 1 + RING)
                else:
                    pl.when(l < N_MLP)(lambda l=l: load_ring(b, l, N_RG + RING, N_MLP - 1))

        def step(j, carry):
            l = N_RG + 4 * j
            send_sib(1, b, j, blocks(l))
            refill(l)
            keep_own(j, blocks(l + 2))
            refill(l + 2)
            chip_sum(1, b, j)
            return carry

        with jax.named_scope(f"d{b}"):
            lax.fori_loop(0, 5, step, 0)

    with jax.named_scope("gather00"):
        gather(0, 0)
    with jax.named_scope("norm00"):
        arrive(0, 0)
        norm_hidden(0)
    gate_up(0)
    with jax.named_scope("gather01"):
        gather(0, 1)
    down(0)
    with jax.named_scope("norm01"):
        arrive(0, 1)
        norm_hidden(1)
    gate_up(1)
    with jax.named_scope("gather10"):
        gather(1, 0)
    down(1)
    mcopies = []
    for b in range(2):
        if b == 1:
            with jax.named_scope("gather11"):
                gather(1, 1)
        with jax.named_scope(f"arrive1{b}"):
            arrive(1, b)
        for half, ref in ((core, xs_recv.at[1, b]), (1 - core, other.at[b])):
            mcopies.append(pltpu.make_async_copy(ref, m_hbm.at[b, pl.ds(half * 5, 5)], ysem.at[3 + len(mcopies)]))
            mcopies[-1].start()
    rcopy = pltpu.make_async_copy(rs_out.at[1], rs_hbm, ysem.at[2])
    rcopy.start()
    with jax.named_scope("tail"):
        hcopies = [pltpu.make_async_copy(x.at[pl.ds(b * 128, 128)], h_hbm.at[pl.ds(b * 128, 128)], ysem.at[b]) for b in range(2)]
        for c in [vcopy, kcopy, rcopy] + hcopies + mcopies:
            c.wait()


def finish_kernel(rs_hbm, gm_hbm, h_hbm, m_hbm, k_in, v_in, y_hbm, k_out, v_out, rs, gm, h, m, kb, vb, isem, msem, hsem, osem, ysem):
    copies = [pltpu.make_async_copy(src, dst, isem.at[i]) for i, (src, dst) in enumerate(((rs_hbm, rs), (gm_hbm, gm), (k_in, kb), (v_in, vb)))]
    for c in copies[:2]:
        c.start()

    def inputs(c):
        return [pltpu.make_async_copy(m_hbm.at[:, c], m.at[c], msem.at[c]), pltpu.make_async_copy(h_hbm.at[:, pl.ds(c * 512, 512)], h.at[:, pl.ds(c * 512, 512)], hsem.at[c])]

    for c in range(10):
        for d in inputs(c):
            d.start()
    for c in copies[2:]:
        c.start()
    copies[0].wait()
    copies[1].wait()
    out = []
    for c in range(10):
        for d in inputs(c):
            d.wait()
        for b in range(2):
            rows = pl.ds(b * 128, 128)
            for w in range(4):
                cs = pl.ds(c * 512 + w * 128, 128)
                g = gm[c * 4 + w:c * 4 + w + 1, :].astype(F32)
                h[rows, cs] = (h[rows, cs].astype(F32) + m[c, b, :, pl.ds(w * 128, 128)].astype(F32) * rs[rows, :] * g).astype(BF16)
        cs = pl.ds(c * 512, 512)
        out.append(pltpu.make_async_copy(h.at[:, cs], y_hbm.at[:, cs], ysem.at[c]))
        out[-1].start()
    for i, (src, dst) in enumerate(((kb, k_out), (vb, v_out))):
        copies[2 + i].wait()
        out.append(pltpu.make_async_copy(src, dst, osem.at[i]))
        out[-1].start()
    for d in out:
        d.wait()


def solution(mesh):
    def local_layer(tokens, seq_lens, w_q, w_k, w_v, w_o, g_q, g_k, g_attn, g_mlp, w_gate, w_up, w_down):
        cos_tab, sin_tab = rope_tables(128)
        hbm = pl.BlockSpec(memory_space=pl.ANY)
        gain = lambda g: g.reshape(-1, 128)
        dma = pltpu.SemaphoreType.DMA
        cache = jax.ShapeDtypeStruct((2, 10, 128, 128), BF16)
        hidden = jax.ShapeDtypeStruct((256, 5120), BF16)
        h, m, rs, kc, vc = pl.pallas_call(
            layer_kernel,
            out_shape=(hidden, jax.ShapeDtypeStruct((2, 10, 128, 512), BF16), jax.ShapeDtypeStruct((256, 128), F32), cache, cache),
            in_specs=[pl.BlockSpec(memory_space=pltpu.SMEM)] + [hbm] * 13,
            out_specs=(hbm,) * 5,
            scratch_shapes=[
                pltpu.VMEM((RING + KEEP, 5120, 256), BF16),
                pltpu.VMEM((256, 5120), BF16),
                pltpu.VMEM((2, 20, 128, 128), F32),
                pltpu.VMEM((2, 10, 128, 128), BF16),
                pltpu.VMEM((2, 10, 128, 128), BF16),
                pltpu.VMEM((128, 3456), BF16),
                pltpu.VMEM((2, 256, 128), F32),
                pltpu.VMEM((8, 256), F32),
                pltpu.VMEM((3, 8, 256), F32),
                pltpu.VMEM((2, 5, 128, 512), BF16),
                pltpu.VMEM((2, 5, 128, 512), BF16),
                pltpu.VMEM((2, 2, 5, 128, 512), BF16),
                pltpu.VMEM((2, 5, 128, 512), BF16),
                pltpu.VMEM((2, 256, 128), F32),
                pltpu.VMEM((128, 128), F32),
                pltpu.VMEM((128, 128), F32),
                pltpu.VMEM((10, 128), BF16),
                pltpu.VMEM((10, 128), BF16),
                pltpu.VMEM((40, 128), BF16),
                pltpu.VMEM((10, 128), F32),
                pltpu.VMEM((10, 128), F32),
                pltpu.VMEM((40, 128), F32),
                dma((RING + KEEP,)), dma, dma((2,)), dma((7,)), dma((3,)), dma((3,)), dma((2, 2, 6, 5)), dma((5,)),
            ],
            compiler_params=pltpu.CompilerParams(collective_id=0, has_side_effects=True, vmem_limit_bytes=67043328),
        )(seq_lens, jnp.asarray(cos_tab), jnp.asarray(sin_tab), gain(g_q), gain(g_k), gain(g_attn),
          tokens.reshape(256, 5120), w_q, w_k, w_v, w_o, w_gate, w_up, w_down)
        y, kc, vc = pl.pallas_call(
            finish_kernel,
            out_shape=(hidden, cache, cache),
            in_specs=[hbm] * 6,
            out_specs=(hbm,) * 3,
            scratch_shapes=[
                pltpu.VMEM((256, 128), F32),
                pltpu.VMEM((40, 128), BF16),
                pltpu.VMEM((256, 5120), BF16),
                pltpu.VMEM((10, 2, 128, 512), BF16),
                pltpu.VMEM((2, 10, 128, 128), BF16),
                pltpu.VMEM((2, 10, 128, 128), BF16),
                dma((4,)), dma((10,)), dma((10,)), dma((2,)), dma((10,)),
            ],
            compiler_params=pltpu.CompilerParams(vmem_limit_bytes=60000000),
        )(rs, gain(g_mlp), h, m, kc, vc)
        return y.reshape(2, 128, 5120), kc, vc

    return jax.shard_map(local_layer, mesh=mesh, in_specs=(P('dp', None, None), P('dp'), P(None, 'tp'), P(None, 'tp'), P(None, 'tp'), P('tp', None), P('tp'), P('tp'), P(), P(), P(None, 'tp'), P(None, 'tp'), P('tp', None)), out_specs=(P('dp', None, None), P('dp', 'tp', None, None), P('dp', 'tp', None, None)), check_vma=False)
```

```python
import jax
import jax.numpy as jnp
import numpy as np
from jax import lax
from jax.experimental import pallas as pl
from jax.experimental.pallas import tpu as pltpu
from jax.sharding import PartitionSpec as P

HEAD_DIM = 128
ROPE_BASE = 500000.0
NORM_EPS = 1e-6
F32 = jnp.float32
BF16 = jnp.bfloat16

WIDTH = 5120
RING = 6
KEEP = 12
N_V, N_QKV = 10, 15
N_G = 27
N_RG = N_G - KEEP
N_MLP = N_RG + 20


def rope_tables(seq_len):
    half = HEAD_DIM // 2
    inv_freq = (ROPE_BASE ** (-2.0 * np.arange(half) / HEAD_DIM)).astype(np.float32)
    angles = np.arange(seq_len, dtype=np.float32)[:, None] * inv_freq[None, :]
    cos, sin = np.cos(angles), np.sin(angles)
    return (np.concatenate([cos, cos], -1).astype(np.float32), np.concatenate([-sin, sin], -1).astype(np.float32))


def cols(start, size):
    return pl.ds(pl.multiple_of(start, size), size)


def dot(a, b):
    return jnp.dot(a, b, preferred_element_type=F32)


def layer_kernel(seq_ref, cos_hbm, sin_hbm, gq_hbm, gk_hbm, ga_hbm, gm_hbm,
                 x_hbm, wq, wk, wv, wo, wg, wu, wd,
                 yh_hbm, m_hbm, rs_hbm, kc_hbm, vc_hbm,
                 pool, x, qk, kb, vb, act, rsc, ssq_send, ssq_recv,
                 sends, rs_recv, xs_recv, other, rs_out,
                 cos_ref, sin_ref, gq16, gk16, ga16, gm16, gq_ref, gk_ref, ga_ref, gm_ref,
                 wsem, xsem, csem, ysem, ssq_s, ssq_r, arsem, tsem):
    t = lax.axis_index("tp")
    core = lax.rem(t, 2)
    sib = t + 1 - 2 * core
    xpeer = lax.rem(t + 2, 4)
    diag = 3 - t

    def load(src, dst, slot):
        pltpu.make_async_copy(src, dst, wsem.at[slot]).start()

    def load_qk(n):
        slot = lax.rem(n, RING)

        @pl.when(lax.rem(n, 2) == 0)
        def _():
            load(wq.at[:, cols((n // 2) * 256, 256)], pool.at[slot], slot)

        @pl.when(lax.rem(n, 2) == 1)
        def _():
            load(wk.at[:, cols((n // 2) * 256, 256)], pool.at[slot], slot)

    def load_v(n):
        slot = lax.rem(n, RING)
        load(wv.at[:, cols((n - N_V) * 256, 256)], pool.at[slot], slot)

    def load_o(j):
        slot = RING + j
        for k in range(4):
            half = core if k // 2 else 1 - core
            load(wo.at[:, cols(half * 2560 + j * 512 + (k % 2) * 256, 256)], pool.at[slot, pl.ds(k * 1280, 1280), :], slot)

    def load_g(k, slot):
        @pl.when(jnp.logical_and(lax.rem(k, 2) == 0, k < N_G - 1))
        def _():
            load(wg.at[:, cols((k // 2) * 256, 256)], pool.at[slot], slot)

        @pl.when(lax.rem(k, 2) == 1)
        def _():
            load(wu.at[:, cols((k // 2) * 256, 256)], pool.at[slot], slot)

        @pl.when(k == N_G - 1)
        def _():
            load(wg.at[:, pl.ds(3328, 128)], pool.at[slot, :, pl.ds(0, 128)], slot)
            load(wu.at[:, pl.ds(3328, 128)], pool.at[slot, :, pl.ds(128, 128)], slot)

    def keep_slot(k):
        return RING + lax.rem(k + 5, KEEP)

    def ring_slot(b, l):
        return lax.rem(N_QKV + N_MLP * b + l, RING)

    def load_ring(b, l, lo, hi):
        slot = ring_slot(b, l)

        def g():
            load_g(KEEP + l, slot)

        def d():
            q = l - N_RG
            half = lax.rem(lax.rem(q, 4) // 2 + 1 + core, 2)
            load(wd.at[:, cols(half * 2560 + (q // 4) * 512 + lax.rem(q, 2) * 256, 256)], pool.at[slot, pl.ds(0, 3456), :], slot)

        def nxt():
            load_g(KEEP + l - N_MLP, slot)

        for start, end, fn in ((0, N_RG, g), (N_RG, N_MLP, d), (N_MLP, 2 * N_MLP, nxt if b == 0 else None)):
            if fn is None or hi < start or lo >= end:
                continue
            if lo >= start and hi < end:
                fn()
            else:
                pl.when(jnp.logical_and(l >= start, l < end))(fn)

    def wait_slot(slot, rows=WIDTH):
        src = wq if rows == WIDTH else wd
        pltpu.make_async_copy(src.at[:, pl.ds(0, 256)], pool.at[slot, pl.ds(0, rows), :], wsem.at[slot]).wait()

    def i32(v):
        return jnp.int32(v)

    xcopies = [pltpu.make_async_copy(x_hbm.at[pl.ds(b * 128, 128)], x.at[pl.ds(b * 128, 128)], xsem.at[b]) for b in range(2)]
    for c in xcopies:
        c.start()
    for n in range(2):
        load_qk(i32(n))
    small = [pltpu.make_async_copy(src, dst, tsem.at[i]) for i, (src, dst) in enumerate(
        ((cos_hbm, cos_ref), (sin_hbm, sin_ref), (gq_hbm, gq16), (gk_hbm, gk16), (ga_hbm, ga16), (gm_hbm, gm16)))]
    for c in small:
        c.start()

    barrier = pltpu.get_barrier_semaphore()
    for peer in (sib, xpeer, diag):
        pl.semaphore_signal(barrier, inc=1, device_id={"tp": peer}, device_id_type=pl.DeviceIdType.MESH)

    def remote(src, dst, ssem, rsem, peer):
        return pltpu.make_async_remote_copy(src_ref=src, dst_ref=dst, send_sem=ssem, recv_sem=rsem,
                                            device_id={"tp": peer}, device_id_type=pl.DeviceIdType.MESH)

    rsc[...] = jnp.zeros_like(rsc)
    for c in xcopies:
        c.wait()
    for n in range(2, 4):
        load_qk(i32(n))

    def qk_step(i, carry):
        n = 2 * i
        s0, s1 = lax.rem(n, RING), lax.rem(n + 1, RING)
        wait_slot(s0)
        wait_slot(s1)
        for m in (n + 4, n + 5):
            pl.when(m < N_V)(lambda m=m: load_qk(m))
            pl.when(m >= N_V)(lambda m=m: load_v(m))
        q = dot(x[...], pool[s0])
        k = dot(x[...], pool[s1])
        for b in range(2):
            for hh in range(2):
                qk[b, 2 * i + hh] = q[b * 128:(b + 1) * 128, hh * 128:(hh + 1) * 128]
                qk[b, 10 + 2 * i + hh] = k[b * 128:(b + 1) * 128, hh * 128:(hh + 1) * 128]
        rsc[0] += q[:, :128] * q[:, :128] + q[:, 128:] * q[:, 128:]
        rsc[1] += k[:, :128] * k[:, :128] + k[:, 128:] * k[:, 128:]
        return carry

    with jax.named_scope("qk"):
        lax.fori_loop(0, 5, qk_step, 0)
    load_v(i32(14))
    load_o(0)

    for r in range(2):
        ssq_send[r:r + 1, :] = jnp.sum(jnp.transpose(rsc[r]), axis=0, keepdims=True)
    ssq_send[2:8, :] = jnp.zeros((6, 256), F32)
    with jax.named_scope("barrier"):
        pl.semaphore_wait(barrier, 3)
    ssq_copies = [remote(ssq_send, ssq_recv.at[j], ssq_s.at[j], ssq_r.at[j], peer) for j, peer in enumerate((sib, xpeer, diag))]
    for c in ssq_copies:
        c.start()

    with jax.named_scope("v"):
        for group in ((10, 11), (12, 13), (14,)):
            for n in group:
                wait_slot(n % RING)
            if group[0] == 10:
                load_o(1)
                load_o(2)
            elif group[0] == 12:
                load_o(3)
                load_o(4)
            else:
                for k in range(KEEP - 5):
                    load_g(i32(k), keep_slot(i32(k)))
            vals = [[dot(x[pl.ds(b * 128, 128), :], pool[n % RING]).astype(BF16) for b in range(2)] for n in group]
            for n, v in zip(group, vals):
                for b in range(2):
                    for hh in range(2):
                        vb[b, 2 * (n - N_V) + hh] = v[b][:, hh * 128:(hh + 1) * 128]
    vcopy = pltpu.make_async_copy(vb, vc_hbm, csem.at[0])
    vcopy.start()
    for l in range(RING):
        load_ring(0, i32(l), l, l)

    with jax.named_scope("ssqwait"):
        for c in ssq_copies:
            c.wait()
    for c in small:
        c.wait()
    for src, dst in ((gq16, gq_ref), (gk16, gk_ref), (ga16, ga_ref), (gm16, gm_ref)):
        dst[...] = src[...].astype(F32)
    total = ssq_send[...] + ssq_recv[0] + ssq_recv[1] + ssq_recv[2]
    scale = lax.rsqrt(total * (1.0 / WIDTH) + NORM_EPS)
    for r in range(2):
        rsc[r] = jnp.transpose(jnp.broadcast_to(scale[r:r + 1, :], (128, 256)))

    def rope(v):
        return (v * cos_ref[...] + pltpu.roll(v, 64, 1) * sin_ref[...]).astype(BF16)

    def qb(h):
        return act.at[:, pl.ds(h * 128, 128)]

    def attention(b):
        rows = pl.ds(b * 128, 128)
        row = lax.broadcasted_iota(jnp.int32, (128, 128), 0)
        col = lax.broadcasted_iota(jnp.int32, (128, 128), 1)
        allowed = jnp.logical_and(col <= row, col < seq_ref[b])
        for h in range(10):
            qb(h)[...] = rope(qk[b, h] * rsc[0, rows, :] * gq_ref[h:h + 1, :])
            kb[b, h] = rope(qk[b, 10 + h] * rsc[1, rows, :] * gk_ref[h:h + 1, :])
        for h in range(10):
            qk[b, h] = lax.dot_general(qb(h)[...], kb[b, h], (((1,), (1,)), ((), ())), preferred_element_type=F32)
        for h in range(10):
            s = jnp.where(allowed, qk[b, h] * HEAD_DIM ** -0.5, -1e30)
            e = jnp.exp(s - jnp.max(s, axis=-1, keepdims=True))
            qb(h)[...] = (e / jnp.sum(e, axis=-1, keepdims=True)).astype(BF16)
        for h in range(10):
            act[:, pl.ds(1280 + h * 128, 128)] = dot(qb(h)[...], vb[b, h]).astype(BF16)

    def rs_copy(p, b, j):
        return remote(sends.at[b, j], rs_recv.at[b, j], arsem.at[p, b, 0, j], arsem.at[p, b, 1, j], sib)

    def xs_copy(p, b, j):
        return remote(sends.at[b, j], xs_recv.at[p, b, j], arsem.at[p, b, 2, j], arsem.at[p, b, 3, j], xpeer)

    def ag_copy(p, b, j):
        return remote(xs_recv.at[p, b, j], other.at[b, j], arsem.at[p, b, 4, j], arsem.at[p, b, 5, j], sib)

    def send_sib(p, b, j, parts):
        for k in range(2):
            sends[b, j, :, pl.ds(k * 256, 256)] = parts[k].astype(BF16)
        rs_copy(p, b, j).start()

    def keep_own(j, parts):
        for k in range(4):
            qk[0, lax.rem(j, 3) * 4 + k] = parts[k // 2][:, (k % 2) * 128:(k % 2 + 1) * 128]

    def chip_sum(p, b, j):
        rs_copy(p, b, j).wait()
        for k in range(4):
            cs = pl.ds(k * 128, 128)
            sends[b, j, :, cs] = (qk[0, lax.rem(j, 3) * 4 + k] + rs_recv[b, j, :, cs].astype(F32)).astype(BF16)
        if (p, b) != (0, 1):
            xs_copy(p, b, j).start()

    def add_squares(half, b, v):
        v = v.astype(F32)
        rsc[half, pl.ds(b * 128, 128), :] += v[:, :128] * v[:, :128] + v[:, 128:256] * v[:, 128:256] + v[:, 256:384] * v[:, 256:384] + v[:, 384:] * v[:, 384:]

    def gather(p, b):
        for half in range(2):
            rsc[half, pl.ds(b * 128, 128), :] = jnp.zeros((128, 128), F32)

        def step(j, carry):
            with jax.named_scope(f"xwait{p}{b}"):
                xs_copy(p, b, j).wait()
            v = (sends[b, j].astype(F32) + xs_recv[p, b, j].astype(F32)).astype(BF16)
            xs_recv[p, b, j] = v
            ag_copy(p, b, j).start()
            add_squares(0, b, v)
            if (p, b) == (0, 0):
                @pl.when(j == 3)
                def _():
                    for c in range(5):
                        xs_copy(0, 1, c).start()
            return carry

        lax.fori_loop(0, 5, step, 0)

    def arrive(p, b):
        def step(j, carry):
            ag_copy(p, b, j).wait()
            add_squares(1, b, other[b, j])
            return carry

        lax.fori_loop(0, 5, step, 0)
        rs = lax.rsqrt(jnp.sum(rsc[0, pl.ds(b * 128, 128), :] + rsc[1, pl.ds(b * 128, 128), :], axis=-1, keepdims=True) * (1.0 / WIDTH) + NORM_EPS)
        rs_out[p, pl.ds(b * 128, 128), :] = jnp.broadcast_to(rs, (128, 128))

    def add_branch(p, b):
        rows = pl.ds(b * 128, 128)
        gain_ref = gm_ref if p else ga_ref

        def apply(j, carry):
            for half, ref in ((core, xs_recv.at[p]), (1 - core, other)):
                for w in range(4):
                    cs = cols(half * 2560 + j * 512 + w * 128, 128)
                    gain = gain_ref[pl.ds(half * 20 + j * 4 + w, 1), :]
                    x[rows, cs] = (x[rows, cs].astype(F32) + ref[b, j, :, pl.ds(w * 128, 128)].astype(F32) * rs_out[p, rows, :] * gain).astype(BF16)
            return carry

        lax.fori_loop(0, 5, apply, 0)

    yhcopies = [pltpu.make_async_copy(x.at[pl.ds(b * 128, 128)], yh_hbm.at[pl.ds(b * 128, 128)], ysem.at[b]) for b in range(2)]

    def project(b):
        def step(j, carry):
            slot = RING + j
            if b == 0:
                wait_slot(slot)
            parts = [dot(act[:, pl.ds(1280, 1280)], pool[slot, pl.ds(k * 1280, 1280), :]) for k in range(4)]
            send_sib(0, b, j, parts[:2])
            keep_own(j, parts[2:])
            pl.when(j > 1)(lambda: chip_sum(0, b, j - 2))
            return carry

        lax.fori_loop(0, 5, step, 0)
        chip_sum(0, b, i32(3))
        chip_sum(0, b, i32(4))

    for b in range(2):
        with jax.named_scope(f"attn{b}"):
            attention(b)
        with jax.named_scope(f"o{b}"):
            project(b)
    kcopy = pltpu.make_async_copy(kb, kc_hbm, csem.at[1])
    kcopy.start()
    for k in range(KEEP - 5, KEEP):
        load_g(i32(k), keep_slot(i32(k)))

    def gu_store(i, g, u):
        act[:, cols(i * 256, 256)] = (g * jax.nn.sigmoid(g) * u).astype(BF16)

    def gate_up(b):
        xb = x.at[pl.ds(b * 128, 128)]

        def ring_pair(l):
            s0, s1 = ring_slot(b, l), ring_slot(b, l + 1)
            wait_slot(s0)
            wait_slot(s1)
            return s0, s1

        def step(i, carry):
            l = 2 * i
            s0, s1 = ring_pair(l)
            k0, k1 = keep_slot(2 * i), keep_slot(2 * i + 1)
            if b == 0:
                wait_slot(k0)
                wait_slot(k1)
            gu_store(i + KEEP // 2, dot(xb[...], pool[s0]), dot(xb[...], pool[s1]))
            gu_store(i, dot(xb[...], pool[k0]), dot(xb[...], pool[k1]))
            load_ring(b, l + RING, RING, KEEP - 2 + RING)
            load_ring(b, l + 1 + RING, 1 + RING, KEEP - 1 + RING)
            return carry

        with jax.named_scope(f"gu{b}"):
            lax.fori_loop(0, KEEP // 2, step, 0)
            s0, s1 = ring_pair(i32(N_RG - 3))
            s2 = ring_slot(b, i32(N_RG - 1))
            wait_slot(s2)
            gu_store(i32(N_G // 2 - 1), dot(xb[...], pool[s0]), dot(xb[...], pool[s1]))
            r = dot(xb[...], pool[s2])
            g = r[:, :128]
            act[:, 3328:3456] = (g * jax.nn.sigmoid(g) * r[:, 128:]).astype(BF16)
            for l in range(N_RG - 3, N_RG):
                load_ring(b, i32(l + RING), l + RING, l + RING)

    def down(b):
        def blocks(first):
            slots = [ring_slot(b, first + k) for k in range(2)]
            for sl in slots:
                wait_slot(sl, 3456)
            return [dot(act[...], pool[sl, pl.ds(0, 3456), :]) for sl in slots]

        def refill(first):
            for k in range(2):
                l = first + k + RING
                if b == 0:
                    load_ring(b, l, N_RG + RING, N_MLP - 1 + RING)
                else:
                    pl.when(l < N_MLP)(lambda l=l: load_ring(b, l, N_RG + RING, N_MLP - 1))

        def step(j, carry):
            l = N_RG + 4 * j
            send_sib(1, b, j, blocks(l))
            refill(l)
            keep_own(j, blocks(l + 2))
            refill(l + 2)
            chip_sum(1, b, j)
            return carry

        with jax.named_scope(f"d{b}"):
            lax.fori_loop(0, 5, step, 0)

    with jax.named_scope("gather00"):
        gather(0, 0)
    with jax.named_scope("norm00"):
        arrive(0, 0)
        add_branch(0, 0)
    gate_up(0)
    with jax.named_scope("gather01"):
        gather(0, 1)
    down(0)
    with jax.named_scope("norm01"):
        arrive(0, 1)
        add_branch(0, 1)
        yhcopies[1].start()
    gate_up(1)
    with jax.named_scope("gather10"):
        gather(1, 0)
    down(1)
    with jax.named_scope("arrive10"):
        arrive(1, 0)
        add_branch(1, 0)
        yhcopies[0].start()
    with jax.named_scope("gather11"):
        gather(1, 1)
    mcopies = [pltpu.make_async_copy(ref, m_hbm.at[pl.ds(half * 5, 5)], ysem.at[3 + i]) for i, (half, ref) in enumerate(((core, xs_recv.at[1, 1]), (1 - core, other.at[1])))]
    mcopies[0].start()
    with jax.named_scope("arrive11"):
        arrive(1, 1)
    mcopies[1].start()
    rcopy = pltpu.make_async_copy(rs_out.at[1, pl.ds(128, 128)], rs_hbm, ysem.at[2])
    rcopy.start()
    with jax.named_scope("tail"):
        for c in [vcopy, kcopy, rcopy] + yhcopies + mcopies:
            c.wait()


def finish_kernel(rs_hbm, gm_hbm, yh_hbm, m_hbm, k_in, v_in, y_hbm, k_out, v_out, rs, gm, yh, m, kb, vb, isem, msem, hsem, psem, osem, ysem):
    def chunk(c):
        cs = pl.ds(c * 512, 512)
        return [pltpu.make_async_copy(m_hbm.at[c], m.at[c], msem.at[c]), pltpu.make_async_copy(yh_hbm.at[pl.ds(128, 128), cs], yh.at[pl.ds(128, 128), cs], hsem.at[c])]

    small = [pltpu.make_async_copy(src, dst, isem.at[i]) for i, (src, dst) in enumerate(((rs_hbm, rs), (gm_hbm, gm)))]
    for d in small:
        d.start()
    for c in range(10):
        for d in chunk(c):
            d.start()
    top = pl.ds(0, 128)
    moves = ((yh_hbm.at[top], yh.at[top], y_hbm.at[top]), (k_in, kb, k_out), (v_in, vb, v_out))
    loads = [pltpu.make_async_copy(src, buf, psem.at[i]) for i, (src, buf, dst) in enumerate(moves)]
    out = [pltpu.make_async_copy(buf, dst, osem.at[i]) for i, (src, buf, dst) in enumerate(moves)]
    for d in loads:
        d.start()
    for d in small:
        d.wait()
    for c in range(10):
        for d in chunk(c):
            d.wait()
        for w in range(4):
            rows, cs = pl.ds(128, 128), pl.ds(c * 512 + w * 128, 128)
            g = gm[c * 4 + w:c * 4 + w + 1, :].astype(F32)
            yh[rows, cs] = (yh[rows, cs].astype(F32) + m[c, :, pl.ds(w * 128, 128)].astype(F32) * rs[...] * g).astype(BF16)
        rows, cs = pl.ds(128, 128), pl.ds(c * 512, 512)
        ycopy = pltpu.make_async_copy(yh.at[rows, cs], y_hbm.at[rows, cs], ysem.at[c])
        ycopy.start()
        out.append(ycopy)
    for i in range(3):
        loads[i].wait()
        out[i].start()
    for d in out:
        d.wait()


def solution(mesh):
    def local_layer(tokens, seq_lens, w_q, w_k, w_v, w_o, g_q, g_k, g_attn, g_mlp, w_gate, w_up, w_down):
        cos_tab, sin_tab = rope_tables(128)
        hbm = pl.BlockSpec(memory_space=pl.ANY)
        gain = lambda g: g.reshape(-1, 128)
        dma = pltpu.SemaphoreType.DMA
        cache = jax.ShapeDtypeStruct((2, 10, 128, 128), BF16)
        hidden = jax.ShapeDtypeStruct((256, 5120), BF16)
        yh, m, rs, kc, vc = pl.pallas_call(
            layer_kernel,
            out_shape=(hidden, jax.ShapeDtypeStruct((10, 128, 512), BF16), jax.ShapeDtypeStruct((128, 128), F32), cache, cache),
            in_specs=[pl.BlockSpec(memory_space=pltpu.SMEM)] + [hbm] * 14,
            out_specs=(hbm,) * 5,
            scratch_shapes=[
                pltpu.VMEM((RING + KEEP, 5120, 256), BF16),
                pltpu.VMEM((256, 5120), BF16),
                pltpu.VMEM((2, 20, 128, 128), F32),
                pltpu.VMEM((2, 10, 128, 128), BF16),
                pltpu.VMEM((2, 10, 128, 128), BF16),
                pltpu.VMEM((128, 3456), BF16),
                pltpu.VMEM((2, 256, 128), F32),
                pltpu.VMEM((8, 256), F32),
                pltpu.VMEM((3, 8, 256), F32),
                pltpu.VMEM((2, 5, 128, 512), BF16),
                pltpu.VMEM((2, 5, 128, 512), BF16),
                pltpu.VMEM((2, 2, 5, 128, 512), BF16),
                pltpu.VMEM((2, 5, 128, 512), BF16),
                pltpu.VMEM((2, 256, 128), F32),
                pltpu.VMEM((128, 128), F32),
                pltpu.VMEM((128, 128), F32),
                pltpu.VMEM((10, 128), BF16),
                pltpu.VMEM((10, 128), BF16),
                pltpu.VMEM((40, 128), BF16),
                pltpu.VMEM((40, 128), BF16),
                pltpu.VMEM((10, 128), F32),
                pltpu.VMEM((10, 128), F32),
                pltpu.VMEM((40, 128), F32),
                pltpu.VMEM((40, 128), F32),
                dma((RING + KEEP,)), dma((2,)), dma((2,)), dma((6,)), dma((3,)), dma((3,)), dma((2, 2, 6, 5)), dma((6,)),
            ],
            compiler_params=pltpu.CompilerParams(collective_id=0, has_side_effects=True, vmem_limit_bytes=67043328),
        )(seq_lens, jnp.asarray(cos_tab), jnp.asarray(sin_tab), gain(g_q), gain(g_k), gain(g_attn), gain(g_mlp),
          tokens.reshape(256, 5120), w_q, w_k, w_v, w_o, w_gate, w_up, w_down)
        y, kc, vc = pl.pallas_call(
            finish_kernel,
            out_shape=(hidden, cache, cache),
            in_specs=[hbm] * 6,
            out_specs=(hbm,) * 3,
            scratch_shapes=[
                pltpu.VMEM((128, 128), F32),
                pltpu.VMEM((40, 128), BF16),
                pltpu.VMEM((256, 5120), BF16),
                pltpu.VMEM((10, 128, 512), BF16),
                pltpu.VMEM((2, 10, 128, 128), BF16),
                pltpu.VMEM((2, 10, 128, 128), BF16),
                dma((2,)), dma((10,)), dma((10,)), dma((3,)), dma((3,)), dma((10,)),
            ],
            compiler_params=pltpu.CompilerParams(vmem_limit_bytes=60000000),
        )(rs, gain(g_mlp), yh, m, kc, vc)
        return y.reshape(2, 128, 5120), kc, vc

    return jax.shard_map(local_layer, mesh=mesh, in_specs=(P('dp', None, None), P('dp'), P(None, 'tp'), P(None, 'tp'), P(None, 'tp'), P('tp', None), P('tp'), P('tp'), P(), P(), P(None, 'tp'), P(None, 'tp'), P('tp', None)), out_specs=(P('dp', None, None), P('dp', 'tp', None, None), P('dp', 'tp', None, None)), check_vma=False)
```

```python
import jax
import jax.numpy as jnp
import numpy as np
from jax import lax
from jax.experimental import pallas as pl
from jax.experimental.pallas import tpu as pltpu
from jax.sharding import PartitionSpec as P

HEAD_DIM = 128
ROPE_BASE = 500000.0
NORM_EPS = 1e-6
F32 = jnp.float32
BF16 = jnp.bfloat16

WIDTH = 5120
RING = 6
KEEP = 12
N_V, N_QKV = 10, 15
N_G = 27
N_RG = N_G - KEEP
N_MLP = N_RG + 20


def rope_tables(seq_len):
    half = HEAD_DIM // 2
    inv_freq = (ROPE_BASE ** (-2.0 * np.arange(half) / HEAD_DIM)).astype(np.float32)
    angles = np.arange(seq_len, dtype=np.float32)[:, None] * inv_freq[None, :]
    cos, sin = np.cos(angles), np.sin(angles)
    return (np.concatenate([cos, cos], -1).astype(np.float32), np.concatenate([-sin, sin], -1).astype(np.float32))


def cols(start, size):
    return pl.ds(pl.multiple_of(start, size), size)


def dot(a, b):
    return jnp.dot(a, b, preferred_element_type=F32)


def layer_kernel(seq_ref, cos_hbm, sin_hbm, gq_hbm, gk_hbm, ga_hbm, gm_hbm,
                 x_hbm, wq, wk, wv, wo, wg, wu, wd,
                 yh_hbm, m_hbm, rs_hbm, kc_hbm, vc_hbm,
                 pool, x, qk, kb, vb, act, rsc, ssq_send, ssq_recv,
                 sends, rs_recv, xs_recv, other, rs_out,
                 gq16, gk16, ga16, gm16, gq_ref, gk_ref, ga_ref, gm_ref,
                 wsem, xsem, csem, ysem, ssq_s, ssq_r, arsem, tsem):
    t = lax.axis_index("tp")
    core = lax.rem(t, 2)
    sib = t + 1 - 2 * core
    xpeer = lax.rem(t + 2, 4)
    diag = 3 - t

    cos_ref, sin_ref = (rs_out.at[r, pl.ds(0, 128)] for r in range(2))

    def load(src, dst, slot):
        pltpu.make_async_copy(src, dst, wsem.at[slot]).start()

    def load_qk(n):
        slot = lax.rem(n, RING)

        @pl.when(lax.rem(n, 2) == 0)
        def _():
            load(wq.at[:, cols((n // 2) * 256, 256)], pool.at[slot], slot)

        @pl.when(lax.rem(n, 2) == 1)
        def _():
            load(wk.at[:, cols((n // 2) * 256, 256)], pool.at[slot], slot)

    def load_v(n):
        slot = lax.rem(n, RING)
        load(wv.at[:, cols((n - N_V) * 256, 256)], pool.at[slot], slot)

    def load_o(j):
        slot = RING + j
        for k in range(4):
            half = core if k // 2 else 1 - core
            load(wo.at[:, cols(half * 2560 + j * 512 + (k % 2) * 256, 256)], pool.at[slot, pl.ds(k * 1280, 1280), :], slot)

    def load_g(k, slot):
        @pl.when(jnp.logical_and(lax.rem(k, 2) == 0, k < N_G - 1))
        def _():
            load(wg.at[:, cols((k // 2) * 256, 256)], pool.at[slot], slot)

        @pl.when(lax.rem(k, 2) == 1)
        def _():
            load(wu.at[:, cols((k // 2) * 256, 256)], pool.at[slot], slot)

        @pl.when(k == N_G - 1)
        def _():
            load(wg.at[:, pl.ds(3328, 128)], pool.at[slot, :, pl.ds(0, 128)], slot)
            load(wu.at[:, pl.ds(3328, 128)], pool.at[slot, :, pl.ds(128, 128)], slot)

    def keep_slot(k):
        return RING + lax.rem(k + 5, KEEP)

    def ring_slot(b, l):
        return lax.rem(N_QKV + N_MLP * b + l, RING)

    def load_ring(b, l, lo, hi):
        slot = ring_slot(b, l)

        def g():
            load_g(KEEP + l, slot)

        def d():
            q = l - N_RG
            half = lax.rem(lax.rem(q, 4) // 2 + 1 + core, 2)
            load(wd.at[:, cols(half * 2560 + (q // 4) * 512 + lax.rem(q, 2) * 256, 256)], pool.at[slot, pl.ds(0, 3456), :], slot)

        def nxt():
            load_g(KEEP + l - N_MLP, slot)

        for start, end, fn in ((0, N_RG, g), (N_RG, N_MLP, d), (N_MLP, 2 * N_MLP, nxt if b == 0 else None)):
            if fn is None or hi < start or lo >= end:
                continue
            if lo >= start and hi < end:
                fn()
            else:
                pl.when(jnp.logical_and(l >= start, l < end))(fn)

    def wait_slot(slot, rows=WIDTH):
        src = wq if rows == WIDTH else wd
        pltpu.make_async_copy(src.at[:, pl.ds(0, 256)], pool.at[slot, pl.ds(0, rows), :], wsem.at[slot]).wait()

    def i32(v):
        return jnp.int32(v)

    xcopies = [pltpu.make_async_copy(x_hbm.at[pl.ds(b * 128, 128)], x.at[pl.ds(b * 128, 128)], xsem.at[b]) for b in range(2)]
    for c in xcopies:
        c.start()
    for n in range(2):
        load_qk(i32(n))
    small = [pltpu.make_async_copy(src, dst, tsem.at[i]) for i, (src, dst) in enumerate(
        ((cos_hbm, cos_ref), (sin_hbm, sin_ref), (gq_hbm, gq16), (gk_hbm, gk16), (ga_hbm, ga16), (gm_hbm, gm16)))]
    for c in small:
        c.start()

    barrier = pltpu.get_barrier_semaphore()
    for peer in (sib, xpeer, diag):
        pl.semaphore_signal(barrier, inc=1, device_id={"tp": peer}, device_id_type=pl.DeviceIdType.MESH)

    def remote(src, dst, ssem, rsem, peer):
        return pltpu.make_async_remote_copy(src_ref=src, dst_ref=dst, send_sem=ssem, recv_sem=rsem,
                                            device_id={"tp": peer}, device_id_type=pl.DeviceIdType.MESH)

    rsc[...] = jnp.zeros_like(rsc)
    for c in xcopies:
        c.wait()
    for n in range(2, 4):
        load_qk(i32(n))

    def qk_step(i, carry):
        n = 2 * i
        s0, s1 = lax.rem(n, RING), lax.rem(n + 1, RING)
        wait_slot(s0)
        wait_slot(s1)
        for m in (n + 4, n + 5):
            pl.when(m < N_V)(lambda m=m: load_qk(m))
            pl.when(m >= N_V)(lambda m=m: load_v(m))
        q = dot(x[...], pool[s0])
        k = dot(x[...], pool[s1])
        for b in range(2):
            for hh in range(2):
                qk[b, 2 * i + hh] = q[b * 128:(b + 1) * 128, hh * 128:(hh + 1) * 128]
                qk[b, 10 + 2 * i + hh] = k[b * 128:(b + 1) * 128, hh * 128:(hh + 1) * 128]
        rsc[0] += q[:, :128] * q[:, :128] + q[:, 128:] * q[:, 128:]
        rsc[1] += k[:, :128] * k[:, :128] + k[:, 128:] * k[:, 128:]
        return carry

    with jax.named_scope("qk"):
        lax.fori_loop(0, 5, qk_step, 0)
    load_v(i32(14))
    load_o(0)

    for r in range(2):
        ssq_send[r:r + 1, :] = jnp.sum(jnp.transpose(rsc[r]), axis=0, keepdims=True)
    ssq_send[2:8, :] = jnp.zeros((6, 256), F32)
    with jax.named_scope("barrier"):
        pl.semaphore_wait(barrier, 3)
    ssq_copies = [remote(ssq_send, ssq_recv.at[j], ssq_s.at[j], ssq_r.at[j], peer) for j, peer in enumerate((sib, xpeer, diag))]
    for c in ssq_copies:
        c.start()

    with jax.named_scope("v"):
        for group in ((10, 11), (12, 13, 14)):
            for n in group:
                wait_slot(n % RING)
            if group[0] == 10:
                load_o(1)
                load_o(2)
            else:
                load_o(3)
                load_o(4)
                for k in range(KEEP - 5):
                    load_g(i32(k), keep_slot(i32(k)))
            vals = [[dot(x[pl.ds(b * 128, 128), :], pool[n % RING]).astype(BF16) for b in range(2)] for n in group]
            for n, v in zip(group, vals):
                for b in range(2):
                    for hh in range(2):
                        vb[b, 2 * (n - N_V) + hh] = v[b][:, hh * 128:(hh + 1) * 128]
    vcopy = pltpu.make_async_copy(vb, vc_hbm, csem.at[0])
    vcopy.start()
    for l in range(RING):
        load_ring(0, i32(l), l, l)

    with jax.named_scope("ssqwait"):
        for c in ssq_copies:
            c.wait()
    for c in small:
        c.wait()
    for src, dst in ((gq16, gq_ref), (gk16, gk_ref), (ga16, ga_ref), (gm16, gm_ref)):
        dst[...] = src[...].astype(F32)
    total = ssq_send[...] + ssq_recv[0] + ssq_recv[1] + ssq_recv[2]
    scale = lax.rsqrt(total * (1.0 / WIDTH) + NORM_EPS)
    for r in range(2):
        rsc[r] = jnp.transpose(jnp.broadcast_to(scale[r:r + 1, :], (128, 256)))

    def rope(v):
        return (v * cos_ref[...] + pltpu.roll(v, 64, 1) * sin_ref[...]).astype(BF16)

    def qb(h):
        return act.at[:, pl.ds(h * 128, 128)]

    def attention(b):
        rows = pl.ds(b * 128, 128)
        row = lax.broadcasted_iota(jnp.int32, (128, 128), 0)
        col = lax.broadcasted_iota(jnp.int32, (128, 128), 1)
        allowed = jnp.logical_and(col <= row, col < seq_ref[b])
        for h in range(10):
            qb(h)[...] = rope(qk[b, h] * rsc[0, rows, :] * gq_ref[h:h + 1, :])
            kb[b, h] = rope(qk[b, 10 + h] * rsc[1, rows, :] * gk_ref[h:h + 1, :])
        for h in range(10):
            qk[b, h] = lax.dot_general(qb(h)[...], kb[b, h], (((1,), (1,)), ((), ())), preferred_element_type=F32)
        for h in range(10):
            s = jnp.where(allowed, qk[b, h] * HEAD_DIM ** -0.5, -1e30)
            e = jnp.exp(s - jnp.max(s, axis=-1, keepdims=True))
            qb(h)[...] = (e / jnp.sum(e, axis=-1, keepdims=True)).astype(BF16)
        for h in range(10):
            act[:, pl.ds(1280 + h * 128, 128)] = dot(qb(h)[...], vb[b, h]).astype(BF16)

    def rs_copy(p, b, j):
        return remote(sends.at[b, j], rs_recv.at[b, j], arsem.at[p, b, 0, j], arsem.at[p, b, 1, j], sib)

    def xs_copy(p, b, j):
        return remote(sends.at[b, j], xs_recv.at[p, b, j], arsem.at[p, b, 2, j], arsem.at[p, b, 3, j], xpeer)

    def ag_copy(p, b, j):
        return remote(xs_recv.at[p, b, j], other.at[b, j], arsem.at[p, b, 4, j], arsem.at[p, b, 5, j], sib)

    def send_sib(p, b, j, parts):
        for k in range(2):
            sends[b, j, :, pl.ds(k * 256, 256)] = parts[k].astype(BF16)
        rs_copy(p, b, j).start()

    def keep_own(j, parts):
        for k in range(4):
            qk[0, lax.rem(j, 3) * 4 + k] = parts[k // 2][:, (k % 2) * 128:(k % 2 + 1) * 128]

    def chip_sum(p, b, j):
        rs_copy(p, b, j).wait()
        for k in range(4):
            cs = pl.ds(k * 128, 128)
            sends[b, j, :, cs] = (qk[0, lax.rem(j, 3) * 4 + k] + rs_recv[b, j, :, cs].astype(F32)).astype(BF16)
        if (p, b) != (0, 1):
            xs_copy(p, b, j).start()

    def add_squares(half, b, v):
        v = v.astype(F32)
        rsc[half, pl.ds(b * 128, 128), :] += v[:, :128] * v[:, :128] + v[:, 128:256] * v[:, 128:256] + v[:, 256:384] * v[:, 256:384] + v[:, 384:] * v[:, 384:]

    def gather(p, b):
        for half in range(2):
            rsc[half, pl.ds(b * 128, 128), :] = jnp.zeros((128, 128), F32)

        def step(j, carry):
            with jax.named_scope(f"xwait{p}{b}"):
                xs_copy(p, b, j).wait()
            v = (sends[b, j].astype(F32) + xs_recv[p, b, j].astype(F32)).astype(BF16)
            xs_recv[p, b, j] = v
            ag_copy(p, b, j).start()
            add_squares(0, b, v)
            if (p, b) == (0, 0):
                @pl.when(j == 3)
                def _():
                    for c in range(5):
                        xs_copy(0, 1, c).start()
            return carry

        lax.fori_loop(0, 5, step, 0)

    def arrive(p, b):
        def step(j, carry):
            ag_copy(p, b, j).wait()
            add_squares(1, b, other[b, j])
            return carry

        lax.fori_loop(0, 5, step, 0)
        rs = lax.rsqrt(jnp.sum(rsc[0, pl.ds(b * 128, 128), :] + rsc[1, pl.ds(b * 128, 128), :], axis=-1, keepdims=True) * (1.0 / WIDTH) + NORM_EPS)
        rs_out[p, pl.ds(b * 128, 128), :] = jnp.broadcast_to(rs, (128, 128))

    def add_branch(p, b):
        rows = pl.ds(b * 128, 128)
        gain_ref = gm_ref if p else ga_ref

        def apply(j, carry):
            for half, ref in ((core, xs_recv.at[p]), (1 - core, other)):
                for w in range(4):
                    cs = cols(half * 2560 + j * 512 + w * 128, 128)
                    gain = gain_ref[pl.ds(half * 20 + j * 4 + w, 1), :]
                    x[rows, cs] = (x[rows, cs].astype(F32) + ref[b, j, :, pl.ds(w * 128, 128)].astype(F32) * rs_out[p, rows, :] * gain).astype(BF16)
            return carry

        lax.fori_loop(0, 5, apply, 0)

    yhcopies = [pltpu.make_async_copy(x.at[pl.ds(b * 128, 128)], yh_hbm.at[pl.ds(b * 128, 128)], ysem.at[b]) for b in range(2)]

    def project(b):
        def step(j, carry):
            slot = RING + j
            if b == 0:
                wait_slot(slot)
            parts = [dot(act[:, pl.ds(1280, 1280)], pool[slot, pl.ds(k * 1280, 1280), :]) for k in range(4)]
            send_sib(0, b, j, parts[:2])
            keep_own(j, parts[2:])
            pl.when(j > 1)(lambda: chip_sum(0, b, j - 2))
            return carry

        lax.fori_loop(0, 5, step, 0)
        chip_sum(0, b, i32(3))
        chip_sum(0, b, i32(4))

    for b in range(2):
        with jax.named_scope(f"attn{b}"):
            attention(b)
        with jax.named_scope(f"o{b}"):
            project(b)
    kcopy = pltpu.make_async_copy(kb, kc_hbm, csem.at[1])
    kcopy.start()
    for k in range(KEEP - 5, KEEP):
        load_g(i32(k), keep_slot(i32(k)))

    def gu_store(i, g, u):
        act[:, cols(i * 256, 256)] = (g * jax.nn.sigmoid(g) * u).astype(BF16)

    def gate_up(b):
        xb = x.at[pl.ds(b * 128, 128)]

        def ring_pair(l):
            s0, s1 = ring_slot(b, l), ring_slot(b, l + 1)
            wait_slot(s0)
            wait_slot(s1)
            return s0, s1

        def step(i, carry):
            l = 2 * i
            s0, s1 = ring_pair(l)
            k0, k1 = keep_slot(2 * i), keep_slot(2 * i + 1)
            if b == 0:
                wait_slot(k0)
                wait_slot(k1)
            gu_store(i + KEEP // 2, dot(xb[...], pool[s0]), dot(xb[...], pool[s1]))
            gu_store(i, dot(xb[...], pool[k0]), dot(xb[...], pool[k1]))
            load_ring(b, l + RING, RING, KEEP - 2 + RING)
            load_ring(b, l + 1 + RING, 1 + RING, KEEP - 1 + RING)
            return carry

        with jax.named_scope(f"gu{b}"):
            lax.fori_loop(0, KEEP // 2, step, 0)
            s0, s1 = ring_pair(i32(N_RG - 3))
            s2 = ring_slot(b, i32(N_RG - 1))
            wait_slot(s2)
            gu_store(i32(N_G // 2 - 1), dot(xb[...], pool[s0]), dot(xb[...], pool[s1]))
            r = dot(xb[...], pool[s2])
            g = r[:, :128]
            act[:, 3328:3456] = (g * jax.nn.sigmoid(g) * r[:, 128:]).astype(BF16)
            for l in range(N_RG - 3, N_RG):
                load_ring(b, i32(l + RING), l + RING, l + RING)

    def down(b):
        def blocks(first):
            slots = [ring_slot(b, first + k) for k in range(2)]
            for sl in slots:
                wait_slot(sl, 3456)
            return [dot(act[...], pool[sl, pl.ds(0, 3456), :]) for sl in slots]

        def refill(first):
            for k in range(2):
                l = first + k + RING
                if b == 0:
                    load_ring(b, l, N_RG + RING, N_MLP - 1 + RING)
                else:
                    pl.when(l < N_MLP)(lambda l=l: load_ring(b, l, N_RG + RING, N_MLP - 1))

        def step(j, carry):
            l = N_RG + 4 * j
            send_sib(1, b, j, blocks(l))
            refill(l)
            keep_own(j, blocks(l + 2))
            refill(l + 2)
            chip_sum(1, b, j)
            return carry

        with jax.named_scope(f"d{b}"):
            lax.fori_loop(0, 5, step, 0)

    with jax.named_scope("gather00"):
        gather(0, 0)
    with jax.named_scope("norm00"):
        arrive(0, 0)
        add_branch(0, 0)
    gate_up(0)
    with jax.named_scope("gather01"):
        gather(0, 1)
    down(0)
    with jax.named_scope("norm01"):
        arrive(0, 1)
        add_branch(0, 1)
        yhcopies[1].start()
    gate_up(1)
    with jax.named_scope("gather10"):
        gather(1, 0)
    down(1)
    with jax.named_scope("arrive10"):
        arrive(1, 0)
        add_branch(1, 0)
        yhcopies[0].start()
    with jax.named_scope("gather11"):
        gather(1, 1)
    mcopies = [pltpu.make_async_copy(ref, m_hbm.at[pl.ds(half * 5, 5)], ysem.at[3 + i]) for i, (half, ref) in enumerate(((core, xs_recv.at[1, 1]), (1 - core, other.at[1])))]
    mcopies[0].start()
    with jax.named_scope("arrive11"):
        arrive(1, 1)
    mcopies[1].start()
    rcopy = pltpu.make_async_copy(rs_out.at[1, pl.ds(128, 128)], rs_hbm, ysem.at[2])
    rcopy.start()
    with jax.named_scope("tail"):
        for c in [vcopy, kcopy, rcopy] + yhcopies + mcopies:
            c.wait()


def finish_kernel(rs_hbm, gm_hbm, yh_hbm, m_hbm, k_in, v_in, y_hbm, k_out, v_out, rs, gm, yh, m, kb, vb, isem, msem, hsem, psem, osem, ysem):
    def chunk(c):
        cs = pl.ds(c * 512, 512)
        return [pltpu.make_async_copy(m_hbm.at[c], m.at[c], msem.at[c]), pltpu.make_async_copy(yh_hbm.at[pl.ds(128, 128), cs], yh.at[pl.ds(128, 128), cs], hsem.at[c])]

    top = pl.ds(0, 128)
    moves = ((yh_hbm.at[top], yh.at[top], y_hbm.at[top]), (k_in, kb, k_out), (v_in, vb, v_out))
    loads = [pltpu.make_async_copy(src, buf, psem.at[i]) for i, (src, buf, dst) in enumerate(moves)]
    out = [pltpu.make_async_copy(buf, dst, osem.at[i]) for i, (src, buf, dst) in enumerate(moves)]
    for d in loads:
        d.start()
    small = [pltpu.make_async_copy(src, dst, isem.at[i]) for i, (src, dst) in enumerate(((rs_hbm, rs), (gm_hbm, gm)))]
    for d in small:
        d.start()
    for c in range(10):
        for d in chunk(c):
            d.start()
    for i in range(3):
        loads[i].wait()
        out[i].start()
    for d in small:
        d.wait()
    for c in range(10):
        for d in chunk(c):
            d.wait()
        for w in range(4):
            rows, cs = pl.ds(128, 128), pl.ds(c * 512 + w * 128, 128)
            g = gm[c * 4 + w:c * 4 + w + 1, :].astype(F32)
            yh[rows, cs] = (yh[rows, cs].astype(F32) + m[c, :, pl.ds(w * 128, 128)].astype(F32) * rs[...] * g).astype(BF16)
        rows, cs = pl.ds(128, 128), pl.ds(c * 512, 512)
        ycopy = pltpu.make_async_copy(yh.at[rows, cs], y_hbm.at[rows, cs], ysem.at[c])
        ycopy.start()
        out.append(ycopy)
    for d in out:
        d.wait()


def solution(mesh):
    def local_layer(tokens, seq_lens, w_q, w_k, w_v, w_o, g_q, g_k, g_attn, g_mlp, w_gate, w_up, w_down):
        cos_tab, sin_tab = rope_tables(128)
        hbm = pl.BlockSpec(memory_space=pl.ANY)
        gain = lambda g: g.reshape(-1, 128)
        dma = pltpu.SemaphoreType.DMA
        cache = jax.ShapeDtypeStruct((2, 10, 128, 128), BF16)
        hidden = jax.ShapeDtypeStruct((256, 5120), BF16)
        yh, m, rs, kc, vc = pl.pallas_call(
            layer_kernel,
            out_shape=(hidden, jax.ShapeDtypeStruct((10, 128, 512), BF16), jax.ShapeDtypeStruct((128, 128), F32), cache, cache),
            in_specs=[pl.BlockSpec(memory_space=pltpu.SMEM)] + [hbm] * 14,
            out_specs=(hbm,) * 5,
            scratch_shapes=[
                pltpu.VMEM((RING + KEEP, 5120, 256), BF16),
                pltpu.VMEM((256, 5120), BF16),
                pltpu.VMEM((2, 20, 128, 128), F32),
                pltpu.VMEM((2, 10, 128, 128), BF16),
                pltpu.VMEM((2, 10, 128, 128), BF16),
                pltpu.VMEM((128, 3456), BF16),
                pltpu.VMEM((2, 256, 128), F32),
                pltpu.VMEM((8, 256), F32),
                pltpu.VMEM((3, 8, 256), F32),
                pltpu.VMEM((2, 5, 128, 512), BF16),
                pltpu.VMEM((2, 5, 128, 512), BF16),
                pltpu.VMEM((2, 2, 5, 128, 512), BF16),
                pltpu.VMEM((2, 5, 128, 512), BF16),
                pltpu.VMEM((2, 256, 128), F32),
                pltpu.VMEM((10, 128), BF16),
                pltpu.VMEM((10, 128), BF16),
                pltpu.VMEM((40, 128), BF16),
                pltpu.VMEM((40, 128), BF16),
                pltpu.VMEM((10, 128), F32),
                pltpu.VMEM((10, 128), F32),
                pltpu.VMEM((40, 128), F32),
                pltpu.VMEM((40, 128), F32),
                dma((RING + KEEP,)), dma((2,)), dma((2,)), dma((6,)), dma((3,)), dma((3,)), dma((2, 2, 6, 5)), dma((6,)),
            ],
            compiler_params=pltpu.CompilerParams(collective_id=0, has_side_effects=True, vmem_limit_bytes=67043328),
        )(seq_lens, jnp.asarray(cos_tab), jnp.asarray(sin_tab), gain(g_q), gain(g_k), gain(g_attn), gain(g_mlp),
          tokens.reshape(256, 5120), w_q, w_k, w_v, w_o, w_gate, w_up, w_down)
        y, kc, vc = pl.pallas_call(
            finish_kernel,
            out_shape=(hidden, cache, cache),
            in_specs=[hbm] * 6,
            out_specs=(hbm,) * 3,
            scratch_shapes=[
                pltpu.VMEM((128, 128), F32),
                pltpu.VMEM((40, 128), BF16),
                pltpu.VMEM((256, 5120), BF16),
                pltpu.VMEM((10, 128, 512), BF16),
                pltpu.VMEM((2, 10, 128, 128), BF16),
                pltpu.VMEM((2, 10, 128, 128), BF16),
                dma((2,)), dma((10,)), dma((10,)), dma((3,)), dma((3,)), dma((10,)),
            ],
            compiler_params=pltpu.CompilerParams(vmem_limit_bytes=60000000),
        )(rs, gain(g_mlp), yh, m, kc, vc)
        return y.reshape(2, 128, 5120), kc, vc

    return jax.shard_map(local_layer, mesh=mesh, in_specs=(P('dp', None, None), P('dp'), P(None, 'tp'), P(None, 'tp'), P(None, 'tp'), P('tp', None), P('tp'), P('tp'), P(), P(), P(None, 'tp'), P(None, 'tp'), P('tp', None)), out_specs=(P('dp', None, None), P('dp', 'tp', None, None), P('dp', 'tp', None, None)), check_vma=False)
```

```python
import jax
import jax.numpy as jnp
import numpy as np
from jax import lax
from jax.experimental import pallas as pl
from jax.experimental.pallas import tpu as pltpu
from jax.sharding import PartitionSpec as P

HEAD_DIM = 128
ROPE_BASE = 500000.0
NORM_EPS = 1e-6
F32 = jnp.float32
BF16 = jnp.bfloat16

WIDTH = 5120
RING = 6
KEEP = 12
N_V, N_QKV = 10, 15
N_G = 27
N_RG = N_G - KEEP
N_MLP = N_RG + 20


def rope_tables(seq_len):
    half = HEAD_DIM // 2
    inv_freq = (ROPE_BASE ** (-2.0 * np.arange(half) / HEAD_DIM)).astype(np.float32)
    angles = np.arange(seq_len, dtype=np.float32)[:, None] * inv_freq[None, :]
    cos, sin = np.cos(angles), np.sin(angles)
    return (np.concatenate([cos, cos], -1).astype(np.float32), np.concatenate([-sin, sin], -1).astype(np.float32))


def cols(start, size):
    return pl.ds(pl.multiple_of(start, size), size)


def dot(a, b):
    return jnp.dot(a, b, preferred_element_type=F32)


def layer_kernel(seq_ref, cos_hbm, sin_hbm, gq_hbm, gk_hbm, ga_hbm, gm_hbm,
                 x_hbm, wq, wk, wv, wo, wg, wu, wd,
                 yh_hbm, m_hbm, rs_hbm, kc_hbm, vc_hbm,
                 pool, x, qk, kb, vb, act, rsc, ssq_send, ssq_recv,
                 sends, rs_recv, xs_recv, other, rs_out,
                 gq16, gk16, ga16, gm16, gq_ref, gk_ref, ga_ref, gm_ref,
                 wsem, xsem, csem, ysem, ssq_s, ssq_r, arsem, tsem):
    t = lax.axis_index("tp")
    core = lax.rem(t, 2)
    sib = t + 1 - 2 * core
    xpeer = lax.rem(t + 2, 4)
    diag = 3 - t

    cos_ref, sin_ref = (rs_out.at[r, pl.ds(0, 128)] for r in range(2))

    def load(src, dst, slot):
        pltpu.make_async_copy(src, dst, wsem.at[slot]).start()

    def load_qk(n):
        slot = lax.rem(n, RING)

        @pl.when(lax.rem(n, 2) == 0)
        def _():
            load(wq.at[:, cols((n // 2) * 256, 256)], pool.at[slot], slot)

        @pl.when(lax.rem(n, 2) == 1)
        def _():
            load(wk.at[:, cols((n // 2) * 256, 256)], pool.at[slot], slot)

    def load_v(n):
        slot = lax.rem(n, RING)
        load(wv.at[:, cols((n - N_V) * 256, 256)], pool.at[slot], slot)

    def load_o(j):
        slot = RING + j
        for k in range(4):
            half = core if k // 2 else 1 - core
            load(wo.at[:, cols(half * 2560 + j * 512 + (k % 2) * 256, 256)], pool.at[slot, pl.ds(k * 1280, 1280), :], slot)

    def load_g(k, slot):
        @pl.when(jnp.logical_and(lax.rem(k, 2) == 0, k < N_G - 1))
        def _():
            load(wg.at[:, cols((k // 2) * 256, 256)], pool.at[slot], slot)

        @pl.when(lax.rem(k, 2) == 1)
        def _():
            load(wu.at[:, cols((k // 2) * 256, 256)], pool.at[slot], slot)

        @pl.when(k == N_G - 1)
        def _():
            load(wg.at[:, pl.ds(3328, 128)], pool.at[slot, :, pl.ds(0, 128)], slot)
            load(wu.at[:, pl.ds(3328, 128)], pool.at[slot, :, pl.ds(128, 128)], slot)

    def keep_slot(k):
        return RING + lax.rem(k + 5, KEEP)

    def ring_slot(b, l):
        return lax.rem(N_QKV + N_MLP * b + l, RING)

    def load_ring(b, l, lo, hi):
        slot = ring_slot(b, l)

        def g():
            load_g(KEEP + l, slot)

        def d():
            q = l - N_RG
            half = lax.rem(lax.rem(q, 4) // 2 + 1 + core, 2)
            load(wd.at[:, cols(half * 2560 + (q // 4) * 512 + lax.rem(q, 2) * 256, 256)], pool.at[slot, pl.ds(0, 3456), :], slot)

        def nxt():
            load_g(KEEP + l - N_MLP, slot)

        for start, end, fn in ((0, N_RG, g), (N_RG, N_MLP, d), (N_MLP, 2 * N_MLP, nxt if b == 0 else None)):
            if fn is None or hi < start or lo >= end:
                continue
            if lo >= start and hi < end:
                fn()
            else:
                pl.when(jnp.logical_and(l >= start, l < end))(fn)

    def wait_slot(slot, rows=WIDTH):
        src = wq if rows == WIDTH else wd
        pltpu.make_async_copy(src.at[:, pl.ds(0, 256)], pool.at[slot, pl.ds(0, rows), :], wsem.at[slot]).wait()

    def i32(v):
        return jnp.int32(v)

    xcopies = [pltpu.make_async_copy(x_hbm.at[pl.ds(b * 128, 128)], x.at[pl.ds(b * 128, 128)], xsem.at[b]) for b in range(2)]
    for c in xcopies:
        c.start()
    for n in range(2):
        load_qk(i32(n))
    small = [pltpu.make_async_copy(src, dst, tsem.at[i]) for i, (src, dst) in enumerate(
        ((cos_hbm, cos_ref), (sin_hbm, sin_ref), (gq_hbm, gq16), (gk_hbm, gk16), (ga_hbm, ga16), (gm_hbm, gm16)))]
    for c in small:
        c.start()

    barrier = pltpu.get_barrier_semaphore()
    for peer in (sib, xpeer, diag):
        pl.semaphore_signal(barrier, inc=1, device_id={"tp": peer}, device_id_type=pl.DeviceIdType.MESH)

    def remote(src, dst, ssem, rsem, peer):
        return pltpu.make_async_remote_copy(src_ref=src, dst_ref=dst, send_sem=ssem, recv_sem=rsem,
                                            device_id={"tp": peer}, device_id_type=pl.DeviceIdType.MESH)

    rsc[...] = jnp.zeros_like(rsc)
    for c in xcopies:
        c.wait()
    for n in range(2, 4):
        load_qk(i32(n))

    def qk_step(i, carry):
        n = 2 * i
        s0, s1 = lax.rem(n, RING), lax.rem(n + 1, RING)
        wait_slot(s0)
        wait_slot(s1)
        for m in (n + 4, n + 5):
            pl.when(m < N_V)(lambda m=m: load_qk(m))
            pl.when(m >= N_V)(lambda m=m: load_v(m))
        q = dot(x[...], pool[s0])
        k = dot(x[...], pool[s1])
        for b in range(2):
            for hh in range(2):
                qk[b, 2 * i + hh] = q[b * 128:(b + 1) * 128, hh * 128:(hh + 1) * 128]
                qk[b, 10 + 2 * i + hh] = k[b * 128:(b + 1) * 128, hh * 128:(hh + 1) * 128]
        rsc[0] += q[:, :128] * q[:, :128] + q[:, 128:] * q[:, 128:]
        rsc[1] += k[:, :128] * k[:, :128] + k[:, 128:] * k[:, 128:]
        return carry

    with jax.named_scope("qk"):
        lax.fori_loop(0, 5, qk_step, 0)
    load_v(i32(14))
    load_o(0)

    for r in range(2):
        ssq_send[r:r + 1, :] = jnp.sum(jnp.transpose(rsc[r]), axis=0, keepdims=True)
    ssq_send[2:8, :] = jnp.zeros((6, 256), F32)
    with jax.named_scope("barrier"):
        pl.semaphore_wait(barrier, 3)
    ssq_copies = [remote(ssq_send, ssq_recv.at[j], ssq_s.at[j], ssq_r.at[j], peer) for j, peer in enumerate((sib, xpeer, diag))]
    for c in ssq_copies:
        c.start()

    with jax.named_scope("v"):
        for group in ((10, 11), (12, 13, 14)):
            for n in group:
                wait_slot(n % RING)
            if group[0] == 10:
                load_o(1)
                load_o(2)
            else:
                load_o(3)
                load_o(4)
                for k in range(KEEP - 5):
                    load_g(i32(k), keep_slot(i32(k)))
            vals = [[dot(x[pl.ds(b * 128, 128), :], pool[n % RING]).astype(BF16) for b in range(2)] for n in group]
            for n, v in zip(group, vals):
                for b in range(2):
                    for hh in range(2):
                        vb[b, 2 * (n - N_V) + hh] = v[b][:, hh * 128:(hh + 1) * 128]
    vcopy = pltpu.make_async_copy(vb, vc_hbm, csem.at[0])
    vcopy.start()
    for l in range(RING):
        load_ring(0, i32(l), l, l)

    with jax.named_scope("ssqwait"):
        for c in ssq_copies:
            c.wait()
    for c in small:
        c.wait()
    for src, dst in ((gq16, gq_ref), (gk16, gk_ref), (ga16, ga_ref), (gm16, gm_ref)):
        dst[...] = src[...].astype(F32)
    total = ssq_send[...] + ssq_recv[0] + ssq_recv[1] + ssq_recv[2]
    scale = lax.rsqrt(total * (1.0 / WIDTH) + NORM_EPS)
    for r in range(2):
        rsc[r] = jnp.transpose(jnp.broadcast_to(scale[r:r + 1, :], (128, 256)))

    def rope(v):
        return (v * cos_ref[...] + pltpu.roll(v, 64, 1) * sin_ref[...]).astype(BF16)

    def qb(h):
        return act.at[:, pl.ds(h * 128, 128)]

    def attention(b):
        rows = pl.ds(b * 128, 128)
        row = lax.broadcasted_iota(jnp.int32, (128, 128), 0)
        col = lax.broadcasted_iota(jnp.int32, (128, 128), 1)
        allowed = jnp.logical_and(col <= row, col < seq_ref[b])
        for h in range(10):
            qb(h)[...] = rope(qk[b, h] * rsc[0, rows, :] * gq_ref[h:h + 1, :])
            kb[b, h] = rope(qk[b, 10 + h] * rsc[1, rows, :] * gk_ref[h:h + 1, :])
        for h in range(10):
            qk[b, h] = lax.dot_general(qb(h)[...], kb[b, h], (((1,), (1,)), ((), ())), preferred_element_type=F32)
        for h in range(10):
            s = jnp.where(allowed, qk[b, h] * HEAD_DIM ** -0.5, -1e30)
            e = jnp.exp(s - jnp.max(s, axis=-1, keepdims=True))
            qb(h)[...] = (e / jnp.sum(e, axis=-1, keepdims=True)).astype(BF16)
        for h in range(10):
            act[:, pl.ds(1280 + h * 128, 128)] = dot(qb(h)[...], vb[b, h]).astype(BF16)

    def rs_copy(p, b, j):
        return remote(sends.at[b, j], rs_recv.at[b, j], arsem.at[p, b, 0, j], arsem.at[p, b, 1, j], sib)

    def xs_copy(p, b, j):
        return remote(sends.at[b, j], xs_recv.at[p, b, j], arsem.at[p, b, 2, j], arsem.at[p, b, 3, j], xpeer)

    def ag_copy(p, b, j):
        return remote(xs_recv.at[p, b, j], other.at[b, j], arsem.at[p, b, 4, j], arsem.at[p, b, 5, j], sib)

    def send_sib(p, b, j, parts):
        for k in range(2):
            sends[b, j, :, pl.ds(k * 256, 256)] = parts[k].astype(BF16)
        rs_copy(p, b, j).start()

    def keep_own(j, parts):
        for k in range(4):
            qk[0, lax.rem(j, 3) * 4 + k] = parts[k // 2][:, (k % 2) * 128:(k % 2 + 1) * 128]

    def chip_sum(p, b, j):
        rs_copy(p, b, j).wait()
        for k in range(4):
            cs = pl.ds(k * 128, 128)
            sends[b, j, :, cs] = (qk[0, lax.rem(j, 3) * 4 + k] + rs_recv[b, j, :, cs].astype(F32)).astype(BF16)
        if (p, b) != (0, 1):
            xs_copy(p, b, j).start()

    def add_squares(half, b, v):
        v = v.astype(F32)
        rsc[half, pl.ds(b * 128, 128), :] += v[:, :128] * v[:, :128] + v[:, 128:256] * v[:, 128:256] + v[:, 256:384] * v[:, 256:384] + v[:, 384:] * v[:, 384:]

    def gather(p, b):
        for half in range(2):
            rsc[half, pl.ds(b * 128, 128), :] = jnp.zeros((128, 128), F32)

        def step(j, carry):
            with jax.named_scope(f"xwait{p}{b}"):
                xs_copy(p, b, j).wait()
            v = (sends[b, j].astype(F32) + xs_recv[p, b, j].astype(F32)).astype(BF16)
            xs_recv[p, b, j] = v
            ag_copy(p, b, j).start()
            add_squares(0, b, v)
            if (p, b) == (0, 0):
                @pl.when(j == 3)
                def _():
                    for c in range(5):
                        xs_copy(0, 1, c).start()
            return carry

        lax.fori_loop(0, 5, step, 0)

    def arrive(p, b):
        def step(j, carry):
            ag_copy(p, b, j).wait()
            add_squares(1, b, other[b, j])
            return carry

        lax.fori_loop(0, 5, step, 0)
        rs = lax.rsqrt(jnp.sum(rsc[0, pl.ds(b * 128, 128), :] + rsc[1, pl.ds(b * 128, 128), :], axis=-1, keepdims=True) * (1.0 / WIDTH) + NORM_EPS)
        rs_out[p, pl.ds(b * 128, 128), :] = jnp.broadcast_to(rs, (128, 128))

    def add_branch(p, b):
        rows = pl.ds(b * 128, 128)
        gain_ref = gm_ref if p else ga_ref

        def apply(j, carry):
            for half, ref in ((core, xs_recv.at[p]), (1 - core, other)):
                for w in range(4):
                    cs = cols(half * 2560 + j * 512 + w * 128, 128)
                    gain = gain_ref[pl.ds(half * 20 + j * 4 + w, 1), :]
                    x[rows, cs] = (x[rows, cs].astype(F32) + ref[b, j, :, pl.ds(w * 128, 128)].astype(F32) * rs_out[p, rows, :] * gain).astype(BF16)
            return carry

        lax.fori_loop(0, 5, apply, 0)

    yhcopies = [pltpu.make_async_copy(x.at[pl.ds(b * 128, 128)], yh_hbm.at[pl.ds(b * 128, 128)], ysem.at[b]) for b in range(2)]

    def project(b):
        def step(j, carry):
            slot = RING + j
            if b == 0:
                wait_slot(slot)
            def blocks(first):
                return [dot(act[:, pl.ds(1280, 1280)], pool[slot, pl.ds(k * 1280, 1280), :]) for k in (first, first + 1)]

            send_sib(0, b, j, blocks(0))
            keep_own(j, blocks(2))
            if b == 0:
                chip_sum(0, b, j)
            else:
                pl.when(j > 1)(lambda: chip_sum(0, b, j - 2))
            return carry

        lax.fori_loop(0, 5, step, 0)
        if b == 1:
            chip_sum(0, b, i32(3))
            chip_sum(0, b, i32(4))

    for b in range(2):
        with jax.named_scope(f"attn{b}"):
            attention(b)
        with jax.named_scope(f"o{b}"):
            project(b)
    kcopy = pltpu.make_async_copy(kb, kc_hbm, csem.at[1])
    kcopy.start()
    for k in range(KEEP - 5, KEEP):
        load_g(i32(k), keep_slot(i32(k)))

    def gu_store(i, g, u):
        act[:, cols(i * 256, 256)] = (g * jax.nn.sigmoid(g) * u).astype(BF16)

    def gate_up(b):
        xb = x.at[pl.ds(b * 128, 128)]

        def ring_pair(l):
            s0, s1 = ring_slot(b, l), ring_slot(b, l + 1)
            wait_slot(s0)
            wait_slot(s1)
            return s0, s1

        def step(i, carry):
            l = 2 * i
            s0, s1 = ring_pair(l)
            k0, k1 = keep_slot(2 * i), keep_slot(2 * i + 1)
            if b == 0:
                wait_slot(k0)
                wait_slot(k1)
            gu_store(i + KEEP // 2, dot(xb[...], pool[s0]), dot(xb[...], pool[s1]))
            gu_store(i, dot(xb[...], pool[k0]), dot(xb[...], pool[k1]))
            load_ring(b, l + RING, RING, KEEP - 2 + RING)
            load_ring(b, l + 1 + RING, 1 + RING, KEEP - 1 + RING)
            return carry

        with jax.named_scope(f"gu{b}"):
            lax.fori_loop(0, KEEP // 2, step, 0)
            s0, s1 = ring_pair(i32(N_RG - 3))
            s2 = ring_slot(b, i32(N_RG - 1))
            wait_slot(s2)
            gu_store(i32(N_G // 2 - 1), dot(xb[...], pool[s0]), dot(xb[...], pool[s1]))
            r = dot(xb[...], pool[s2])
            g = r[:, :128]
            act[:, 3328:3456] = (g * jax.nn.sigmoid(g) * r[:, 128:]).astype(BF16)
            for l in range(N_RG - 3, N_RG):
                load_ring(b, i32(l + RING), l + RING, l + RING)

    def down(b):
        def blocks(first):
            slots = [ring_slot(b, first + k) for k in range(2)]
            for sl in slots:
                wait_slot(sl, 3456)
            return [dot(act[...], pool[sl, pl.ds(0, 3456), :]) for sl in slots]

        def refill(first):
            for k in range(2):
                l = first + k + RING
                if b == 0:
                    load_ring(b, l, N_RG + RING, N_MLP - 1 + RING)
                else:
                    pl.when(l < N_MLP)(lambda l=l: load_ring(b, l, N_RG + RING, N_MLP - 1))

        def step(j, carry):
            l = N_RG + 4 * j
            send_sib(1, b, j, blocks(l))
            refill(l)
            keep_own(j, blocks(l + 2))
            refill(l + 2)
            if b == 1:
                chip_sum(1, b, j)
            else:
                pl.when(j > 0)(lambda: chip_sum(1, b, j - 1))
            return carry

        with jax.named_scope(f"d{b}"):
            lax.fori_loop(0, 5, step, 0)
            if b == 0:
                chip_sum(1, b, i32(4))

    with jax.named_scope("gather00"):
        gather(0, 0)
    with jax.named_scope("norm00"):
        arrive(0, 0)
        add_branch(0, 0)
    gate_up(0)
    with jax.named_scope("gather01"):
        gather(0, 1)
    down(0)
    with jax.named_scope("norm01"):
        arrive(0, 1)
        add_branch(0, 1)
        yhcopies[1].start()
    gate_up(1)
    with jax.named_scope("gather10"):
        gather(1, 0)
    down(1)
    with jax.named_scope("arrive10"):
        arrive(1, 0)
        add_branch(1, 0)
        yhcopies[0].start()
    with jax.named_scope("gather11"):
        gather(1, 1)
    mcopies = [pltpu.make_async_copy(ref, m_hbm.at[pl.ds(half * 5, 5)], ysem.at[3 + i]) for i, (half, ref) in enumerate(((core, xs_recv.at[1, 1]), (1 - core, other.at[1])))]
    mcopies[0].start()
    with jax.named_scope("arrive11"):
        arrive(1, 1)
    mcopies[1].start()
    rcopy = pltpu.make_async_copy(rs_out.at[1, pl.ds(128, 128)], rs_hbm, ysem.at[2])
    rcopy.start()
    with jax.named_scope("tail"):
        for c in [vcopy, kcopy, rcopy] + yhcopies + mcopies:
            c.wait()


def finish_kernel(rs_hbm, gm_hbm, yh_hbm, m_hbm, k_in, v_in, y_hbm, k_out, v_out, rs, gm, yh, m, kb, vb, isem, msem, hsem, psem, osem, ysem):
    def chunk(c):
        cs = pl.ds(c * 512, 512)
        return [pltpu.make_async_copy(m_hbm.at[c], m.at[c], msem.at[c]), pltpu.make_async_copy(yh_hbm.at[pl.ds(128, 128), cs], yh.at[pl.ds(128, 128), cs], hsem.at[c])]

    top = pl.ds(0, 128)
    moves = ((yh_hbm.at[top], yh.at[top], y_hbm.at[top]), (k_in, kb, k_out), (v_in, vb, v_out))
    loads = [pltpu.make_async_copy(src, buf, psem.at[i]) for i, (src, buf, dst) in enumerate(moves)]
    out = [pltpu.make_async_copy(buf, dst, osem.at[i]) for i, (src, buf, dst) in enumerate(moves)]
    for d in loads:
        d.start()
    small = [pltpu.make_async_copy(src, dst, isem.at[i]) for i, (src, dst) in enumerate(((rs_hbm, rs), (gm_hbm, gm)))]
    for d in small:
        d.start()
    for c in range(10):
        for d in chunk(c):
            d.start()
    for i in range(3):
        loads[i].wait()
        out[i].start()
    for d in small:
        d.wait()
    for c in range(10):
        for d in chunk(c):
            d.wait()
        for w in range(4):
            rows, cs = pl.ds(128, 128), pl.ds(c * 512 + w * 128, 128)
            g = gm[c * 4 + w:c * 4 + w + 1, :].astype(F32)
            yh[rows, cs] = (yh[rows, cs].astype(F32) + m[c, :, pl.ds(w * 128, 128)].astype(F32) * rs[...] * g).astype(BF16)
        rows, cs = pl.ds(128, 128), pl.ds(c * 512, 512)
        ycopy = pltpu.make_async_copy(yh.at[rows, cs], y_hbm.at[rows, cs], ysem.at[c])
        ycopy.start()
        out.append(ycopy)
    for d in out:
        d.wait()


def solution(mesh):
    def local_layer(tokens, seq_lens, w_q, w_k, w_v, w_o, g_q, g_k, g_attn, g_mlp, w_gate, w_up, w_down):
        cos_tab, sin_tab = rope_tables(128)
        hbm = pl.BlockSpec(memory_space=pl.ANY)
        gain = lambda g: g.reshape(-1, 128)
        dma = pltpu.SemaphoreType.DMA
        cache = jax.ShapeDtypeStruct((2, 10, 128, 128), BF16)
        hidden = jax.ShapeDtypeStruct((256, 5120), BF16)
        yh, m, rs, kc, vc = pl.pallas_call(
            layer_kernel,
            out_shape=(hidden, jax.ShapeDtypeStruct((10, 128, 512), BF16), jax.ShapeDtypeStruct((128, 128), F32), cache, cache),
            in_specs=[pl.BlockSpec(memory_space=pltpu.SMEM)] + [hbm] * 14,
            out_specs=(hbm,) * 5,
            scratch_shapes=[
                pltpu.VMEM((RING + KEEP, 5120, 256), BF16),
                pltpu.VMEM((256, 5120), BF16),
                pltpu.VMEM((2, 20, 128, 128), F32),
                pltpu.VMEM((2, 10, 128, 128), BF16),
                pltpu.VMEM((2, 10, 128, 128), BF16),
                pltpu.VMEM((128, 3456), BF16),
                pltpu.VMEM((2, 256, 128), F32),
                pltpu.VMEM((8, 256), F32),
                pltpu.VMEM((3, 8, 256), F32),
                pltpu.VMEM((2, 5, 128, 512), BF16),
                pltpu.VMEM((2, 5, 128, 512), BF16),
                pltpu.VMEM((2, 2, 5, 128, 512), BF16),
                pltpu.VMEM((2, 5, 128, 512), BF16),
                pltpu.VMEM((2, 256, 128), F32),
                pltpu.VMEM((10, 128), BF16),
                pltpu.VMEM((10, 128), BF16),
                pltpu.VMEM((40, 128), BF16),
                pltpu.VMEM((40, 128), BF16),
                pltpu.VMEM((10, 128), F32),
                pltpu.VMEM((10, 128), F32),
                pltpu.VMEM((40, 128), F32),
                pltpu.VMEM((40, 128), F32),
                dma((RING + KEEP,)), dma((2,)), dma((2,)), dma((6,)), dma((3,)), dma((3,)), dma((2, 2, 6, 5)), dma((6,)),
            ],
            compiler_params=pltpu.CompilerParams(collective_id=0, has_side_effects=True, vmem_limit_bytes=67043328),
        )(seq_lens, jnp.asarray(cos_tab), jnp.asarray(sin_tab), gain(g_q), gain(g_k), gain(g_attn), gain(g_mlp),
          tokens.reshape(256, 5120), w_q, w_k, w_v, w_o, w_gate, w_up, w_down)
        y, kc, vc = pl.pallas_call(
            finish_kernel,
            out_shape=(hidden, cache, cache),
            in_specs=[hbm] * 6,
            out_specs=(hbm,) * 3,
            scratch_shapes=[
                pltpu.VMEM((128, 128), F32),
                pltpu.VMEM((40, 128), BF16),
                pltpu.VMEM((256, 5120), BF16),
                pltpu.VMEM((10, 128, 512), BF16),
                pltpu.VMEM((2, 10, 128, 128), BF16),
                pltpu.VMEM((2, 10, 128, 128), BF16),
                dma((2,)), dma((10,)), dma((10,)), dma((3,)), dma((3,)), dma((10,)),
            ],
            compiler_params=pltpu.CompilerParams(vmem_limit_bytes=60000000),
        )(rs, gain(g_mlp), yh, m, kc, vc)
        return y.reshape(2, 128, 5120), kc, vc

    return jax.shard_map(local_layer, mesh=mesh, in_specs=(P('dp', None, None), P('dp'), P(None, 'tp'), P(None, 'tp'), P(None, 'tp'), P('tp', None), P('tp'), P('tp'), P(), P(), P(None, 'tp'), P(None, 'tp'), P('tp', None)), out_specs=(P('dp', None, None), P('dp', 'tp', None, None), P('dp', 'tp', None, None)), check_vma=False)
```

```python
import jax
import jax.numpy as jnp
import numpy as np
from jax import lax
from jax.experimental import pallas as pl
from jax.experimental.pallas import tpu as pltpu
from jax.sharding import PartitionSpec as P

HEAD_DIM = 128
ROPE_BASE = 500000.0
NORM_EPS = 1e-6
F32 = jnp.float32
BF16 = jnp.bfloat16

WIDTH = 5120
RING = 6
KEEP = 12
N_V, N_QKV = 10, 15
N_G = 27
N_RG = N_G - KEEP
N_MLP = N_RG + 20


def rope_tables(seq_len):
    half = HEAD_DIM // 2
    inv_freq = (ROPE_BASE ** (-2.0 * np.arange(half) / HEAD_DIM)).astype(np.float32)
    angles = np.arange(seq_len, dtype=np.float32)[:, None] * inv_freq[None, :]
    cos, sin = np.cos(angles), np.sin(angles)
    return (np.concatenate([cos, cos], -1).astype(np.float32), np.concatenate([-sin, sin], -1).astype(np.float32))


def cols(start, size):
    return pl.ds(pl.multiple_of(start, size), size)


def dot(a, b):
    return jnp.dot(a, b, preferred_element_type=F32)


def layer_kernel(seq_ref, cos_hbm, sin_hbm, gq_hbm, gk_hbm, ga_hbm, gm_hbm,
                 x_hbm, wq, wk, wv, wo, wg, wu, wd,
                 yh_hbm, m_hbm, rs_hbm, kc_hbm, vc_hbm,
                 pool, x, qk, kb, vb, act, rsc, ssq_send, ssq_recv,
                 sends, rs_recv, xs_recv, other, rs_out,
                 gq16, gk16, ga16, gm16, gq_ref, gk_ref, ga_ref, gm_ref,
                 wsem, xsem, csem, ysem, ssq_s, ssq_r, arsem, tsem):
    t = lax.axis_index("tp")
    core = lax.rem(t, 2)
    sib = t + 1 - 2 * core
    xpeer = lax.rem(t + 2, 4)
    diag = 3 - t

    cos_ref, sin_ref = (rs_out.at[r, pl.ds(0, 128)] for r in range(2))

    def load(src, dst, slot):
        pltpu.make_async_copy(src, dst, wsem.at[slot]).start()

    def load_qk(n):
        slot = lax.rem(n, RING)

        @pl.when(lax.rem(n, 2) == 0)
        def _():
            load(wq.at[:, cols((n // 2) * 256, 256)], pool.at[slot], slot)

        @pl.when(lax.rem(n, 2) == 1)
        def _():
            load(wk.at[:, cols((n // 2) * 256, 256)], pool.at[slot], slot)

    def load_v(n):
        slot = lax.rem(n, RING)
        load(wv.at[:, cols((n - N_V) * 256, 256)], pool.at[slot], slot)

    def load_o(j):
        slot = RING + j
        for k in range(4):
            half = core if k // 2 else 1 - core
            load(wo.at[:, cols(half * 2560 + j * 512 + (k % 2) * 256, 256)], pool.at[slot, pl.ds(k * 1280, 1280), :], slot)

    def load_g(k, slot):
        @pl.when(jnp.logical_and(lax.rem(k, 2) == 0, k < N_G - 1))
        def _():
            load(wg.at[:, cols((k // 2) * 256, 256)], pool.at[slot], slot)

        @pl.when(lax.rem(k, 2) == 1)
        def _():
            load(wu.at[:, cols((k // 2) * 256, 256)], pool.at[slot], slot)

        @pl.when(k == N_G - 1)
        def _():
            load(wg.at[:, pl.ds(3328, 128)], pool.at[slot, :, pl.ds(0, 128)], slot)
            load(wu.at[:, pl.ds(3328, 128)], pool.at[slot, :, pl.ds(128, 128)], slot)

    def keep_slot(k):
        return RING + lax.rem(k + 5, KEEP)

    def ring_slot(b, l):
        return lax.rem(N_QKV + N_MLP * b + l, RING)

    def load_ring(b, l, lo, hi):
        slot = ring_slot(b, l)

        def g():
            load_g(KEEP + l, slot)

        def d():
            q = l - N_RG
            half = lax.rem(lax.rem(q, 4) // 2 + 1 + core, 2)
            load(wd.at[:, cols(half * 2560 + (q // 4) * 512 + lax.rem(q, 2) * 256, 256)], pool.at[slot, pl.ds(0, 3456), :], slot)

        def nxt():
            load_g(KEEP + l - N_MLP, slot)

        for start, end, fn in ((0, N_RG, g), (N_RG, N_MLP, d), (N_MLP, 2 * N_MLP, nxt if b == 0 else None)):
            if fn is None or hi < start or lo >= end:
                continue
            if lo >= start and hi < end:
                fn()
            else:
                pl.when(jnp.logical_and(l >= start, l < end))(fn)

    def wait_slot(slot, rows=WIDTH):
        src = wq if rows == WIDTH else wd
        pltpu.make_async_copy(src.at[:, pl.ds(0, 256)], pool.at[slot, pl.ds(0, rows), :], wsem.at[slot]).wait()

    def i32(v):
        return jnp.int32(v)

    xcopies = [pltpu.make_async_copy(x_hbm.at[pl.ds(b * 128, 128)], x.at[pl.ds(b * 128, 128)], xsem.at[b]) for b in range(2)]
    for c in xcopies:
        c.start()
    for n in range(2):
        load_qk(i32(n))
    small = [pltpu.make_async_copy(src, dst, tsem.at[i]) for i, (src, dst) in enumerate(
        ((cos_hbm, cos_ref), (sin_hbm, sin_ref), (gq_hbm, gq16), (gk_hbm, gk16), (ga_hbm, ga16), (gm_hbm, gm16)))]
    for c in small:
        c.start()

    barrier = pltpu.get_barrier_semaphore()
    for peer in (sib, xpeer, diag):
        pl.semaphore_signal(barrier, inc=1, device_id={"tp": peer}, device_id_type=pl.DeviceIdType.MESH)

    def remote(src, dst, ssem, rsem, peer):
        return pltpu.make_async_remote_copy(src_ref=src, dst_ref=dst, send_sem=ssem, recv_sem=rsem,
                                            device_id={"tp": peer}, device_id_type=pl.DeviceIdType.MESH)

    rsc[...] = jnp.zeros_like(rsc)
    for c in xcopies:
        c.wait()
    for n in range(2, 4):
        load_qk(i32(n))

    def qk_step(i, carry):
        n = 2 * i
        s0, s1 = lax.rem(n, RING), lax.rem(n + 1, RING)
        wait_slot(s0)
        wait_slot(s1)
        for m in (n + 4, n + 5):
            pl.when(m < N_V)(lambda m=m: load_qk(m))
            pl.when(m >= N_V)(lambda m=m: load_v(m))
        q = dot(x[...], pool[s0])
        k = dot(x[...], pool[s1])
        for b in range(2):
            for hh in range(2):
                qk[b, 2 * i + hh] = q[b * 128:(b + 1) * 128, hh * 128:(hh + 1) * 128]
                qk[b, 10 + 2 * i + hh] = k[b * 128:(b + 1) * 128, hh * 128:(hh + 1) * 128]
        rsc[0] += q[:, :128] * q[:, :128] + q[:, 128:] * q[:, 128:]
        rsc[1] += k[:, :128] * k[:, :128] + k[:, 128:] * k[:, 128:]
        return carry

    with jax.named_scope("qk"):
        lax.fori_loop(0, 5, qk_step, 0)
    load_v(i32(14))
    load_o(0)

    for r in range(2):
        ssq_send[r:r + 1, :] = jnp.sum(jnp.transpose(rsc[r]), axis=0, keepdims=True)
    ssq_send[2:8, :] = jnp.zeros((6, 256), F32)
    with jax.named_scope("barrier"):
        pl.semaphore_wait(barrier, 3)
    ssq_copies = [remote(ssq_send, ssq_recv.at[j], ssq_s.at[j], ssq_r.at[j], peer) for j, peer in enumerate((sib, xpeer, diag))]
    for c in ssq_copies:
        c.start()

    with jax.named_scope("v"):
        for group in ((10, 11), (12, 13), (14,)):
            for n in group:
                wait_slot(n % RING)
            if group[0] == 10:
                load_o(1)
                load_o(2)
            elif group[0] == 12:
                load_o(3)
                load_o(4)
            else:
                for k in range(KEEP - 5):
                    load_g(i32(k), keep_slot(i32(k)))
            vals = [[dot(x[pl.ds(b * 128, 128), :], pool[n % RING]).astype(BF16) for b in range(2)] for n in group]
            for n, v in zip(group, vals):
                for b in range(2):
                    for hh in range(2):
                        vb[b, 2 * (n - N_V) + hh] = v[b][:, hh * 128:(hh + 1) * 128]
    vcopy = pltpu.make_async_copy(vb, vc_hbm, csem.at[0])
    vcopy.start()
    for l in range(RING):
        load_ring(0, i32(l), l, l)

    with jax.named_scope("ssqwait"):
        for c in ssq_copies:
            c.wait()
    for c in small:
        c.wait()
    for src, dst in ((gq16, gq_ref), (gk16, gk_ref), (ga16, ga_ref), (gm16, gm_ref)):
        dst[...] = src[...].astype(F32)
    total = ssq_send[...] + ssq_recv[0] + ssq_recv[1] + ssq_recv[2]
    scale = lax.rsqrt(total * (1.0 / WIDTH) + NORM_EPS)
    for r in range(2):
        rsc[r] = jnp.transpose(jnp.broadcast_to(scale[r:r + 1, :], (128, 256)))

    def rope(v):
        return (v * cos_ref[...] + pltpu.roll(v, 64, 1) * sin_ref[...]).astype(BF16)

    def qb(h):
        return act.at[:, pl.ds(h * 128, 128)]

    def attention(b):
        rows = pl.ds(b * 128, 128)
        row = lax.broadcasted_iota(jnp.int32, (128, 128), 0)
        col = lax.broadcasted_iota(jnp.int32, (128, 128), 1)
        allowed = jnp.logical_and(col <= row, col < seq_ref[b])
        for h in range(10):
            qb(h)[...] = rope(qk[b, h] * rsc[0, rows, :] * gq_ref[h:h + 1, :])
            kb[b, h] = rope(qk[b, 10 + h] * rsc[1, rows, :] * gk_ref[h:h + 1, :])
        for h in range(10):
            qk[b, h] = lax.dot_general(qb(h)[...], kb[b, h], (((1,), (1,)), ((), ())), preferred_element_type=F32)
        for h in range(10):
            s = jnp.where(allowed, qk[b, h] * HEAD_DIM ** -0.5, -1e30)
            e = jnp.exp(s - jnp.max(s, axis=-1, keepdims=True))
            qb(h)[...] = (e / jnp.sum(e, axis=-1, keepdims=True)).astype(BF16)
        for h in range(10):
            act[:, pl.ds(1280 + h * 128, 128)] = dot(qb(h)[...], vb[b, h]).astype(BF16)

    def rs_copy(p, b, j):
        return remote(sends.at[b, j], rs_recv.at[b, j], arsem.at[p, b, 0, j], arsem.at[p, b, 1, j], sib)

    def xs_copy(p, b, j):
        return remote(sends.at[b, j], xs_recv.at[p, b, j], arsem.at[p, b, 2, j], arsem.at[p, b, 3, j], xpeer)

    def ag_copy(p, b, j):
        return remote(xs_recv.at[p, b, j], other.at[b, j], arsem.at[p, b, 4, j], arsem.at[p, b, 5, j], sib)

    def send_sib(p, b, j, parts):
        for k in range(2):
            sends[b, j, :, pl.ds(k * 256, 256)] = parts[k].astype(BF16)
        rs_copy(p, b, j).start()

    def keep_own(j, parts):
        for k in range(4):
            qk[0, lax.rem(j, 3) * 4 + k] = parts[k // 2][:, (k % 2) * 128:(k % 2 + 1) * 128]

    def chip_sum(p, b, j):
        rs_copy(p, b, j).wait()
        for k in range(4):
            cs = pl.ds(k * 128, 128)
            sends[b, j, :, cs] = (qk[0, lax.rem(j, 3) * 4 + k] + rs_recv[b, j, :, cs].astype(F32)).astype(BF16)
        if (p, b) != (0, 1):
            xs_copy(p, b, j).start()

    def add_squares(half, b, v):
        v = v.astype(F32)
        rsc[half, pl.ds(b * 128, 128), :] += v[:, :128] * v[:, :128] + v[:, 128:256] * v[:, 128:256] + v[:, 256:384] * v[:, 256:384] + v[:, 384:] * v[:, 384:]

    def gather(p, b):
        for half in range(2):
            rsc[half, pl.ds(b * 128, 128), :] = jnp.zeros((128, 128), F32)

        def step(j, carry):
            with jax.named_scope(f"xwait{p}{b}"):
                xs_copy(p, b, j).wait()
            v = (sends[b, j].astype(F32) + xs_recv[p, b, j].astype(F32)).astype(BF16)
            xs_recv[p, b, j] = v
            ag_copy(p, b, j).start()
            add_squares(0, b, v)
            if (p, b) == (0, 0):
                @pl.when(j == 3)
                def _():
                    for c in range(5):
                        xs_copy(0, 1, c).start()
            return carry

        lax.fori_loop(0, 5, step, 0)

    def arrive(p, b):
        def step(j, carry):
            ag_copy(p, b, j).wait()
            add_squares(1, b, other[b, j])
            return carry

        lax.fori_loop(0, 5, step, 0)
        rs = lax.rsqrt(jnp.sum(rsc[0, pl.ds(b * 128, 128), :] + rsc[1, pl.ds(b * 128, 128), :], axis=-1, keepdims=True) * (1.0 / WIDTH) + NORM_EPS)
        rs_out[p, pl.ds(b * 128, 128), :] = jnp.broadcast_to(rs, (128, 128))

    def add_branch(p, b):
        rows = pl.ds(b * 128, 128)
        gain_ref = gm_ref if p else ga_ref

        def apply(j, carry):
            for half, ref in ((core, xs_recv.at[p]), (1 - core, other)):
                for w in range(4):
                    cs = cols(half * 2560 + j * 512 + w * 128, 128)
                    gain = gain_ref[pl.ds(half * 20 + j * 4 + w, 1), :]
                    x[rows, cs] = (x[rows, cs].astype(F32) + ref[b, j, :, pl.ds(w * 128, 128)].astype(F32) * rs_out[p, rows, :] * gain).astype(BF16)
            return carry

        lax.fori_loop(0, 5, apply, 0)

    yhcopies = [pltpu.make_async_copy(x.at[pl.ds(b * 128, 128)], yh_hbm.at[pl.ds(b * 128, 128)], ysem.at[b]) for b in range(2)]

    def project(b):
        def step(j, carry):
            slot = RING + j
            if b == 0:
                wait_slot(slot)
            def blocks(first):
                return [dot(act[:, pl.ds(1280, 1280)], pool[slot, pl.ds(k * 1280, 1280), :]) for k in (first, first + 1)]

            send_sib(0, b, j, blocks(0))
            keep_own(j, blocks(2))
            if b == 0:
                chip_sum(0, b, j)
            else:
                pl.when(j > 1)(lambda: chip_sum(0, b, j - 2))
            return carry

        lax.fori_loop(0, 5, step, 0)
        if b == 1:
            chip_sum(0, b, i32(3))
            chip_sum(0, b, i32(4))

    for b in range(2):
        with jax.named_scope(f"attn{b}"):
            attention(b)
        with jax.named_scope(f"o{b}"):
            project(b)
    kcopy = pltpu.make_async_copy(kb, kc_hbm, csem.at[1])
    kcopy.start()
    for k in range(KEEP - 5, KEEP):
        load_g(i32(k), keep_slot(i32(k)))

    def gu_store(i, g, u):
        act[:, cols(i * 256, 256)] = (g * jax.nn.sigmoid(g) * u).astype(BF16)

    def gate_up(b):
        xb = x.at[pl.ds(b * 128, 128)]

        def ring_pair(l):
            s0, s1 = ring_slot(b, l), ring_slot(b, l + 1)
            wait_slot(s0)
            wait_slot(s1)
            return s0, s1

        def step(i, carry):
            l = 2 * i
            s0, s1 = ring_pair(l)
            k0, k1 = keep_slot(2 * i), keep_slot(2 * i + 1)
            if b == 0:
                wait_slot(k0)
                wait_slot(k1)
            gu_store(i + KEEP // 2, dot(xb[...], pool[s0]), dot(xb[...], pool[s1]))
            gu_store(i, dot(xb[...], pool[k0]), dot(xb[...], pool[k1]))
            load_ring(b, l + RING, RING, KEEP - 2 + RING)
            load_ring(b, l + 1 + RING, 1 + RING, KEEP - 1 + RING)
            return carry

        with jax.named_scope(f"gu{b}"):
            lax.fori_loop(0, KEEP // 2, step, 0)
            s0, s1 = ring_pair(i32(N_RG - 3))
            s2 = ring_slot(b, i32(N_RG - 1))
            wait_slot(s2)
            gu_store(i32(N_G // 2 - 1), dot(xb[...], pool[s0]), dot(xb[...], pool[s1]))
            r = dot(xb[...], pool[s2])
            g = r[:, :128]
            act[:, 3328:3456] = (g * jax.nn.sigmoid(g) * r[:, 128:]).astype(BF16)
            for l in range(N_RG - 3, N_RG):
                load_ring(b, i32(l + RING), l + RING, l + RING)

    def down(b):
        def blocks(first):
            slots = [ring_slot(b, first + k) for k in range(2)]
            for sl in slots:
                wait_slot(sl, 3456)
            return [dot(act[...], pool[sl, pl.ds(0, 3456), :]) for sl in slots]

        def refill(first):
            for k in range(2):
                l = first + k + RING
                if b == 0:
                    load_ring(b, l, N_RG + RING, N_MLP - 1 + RING)
                else:
                    pl.when(l < N_MLP)(lambda l=l: load_ring(b, l, N_RG + RING, N_MLP - 1))

        def step(j, carry):
            l = N_RG + 4 * j
            send_sib(1, b, j, blocks(l))
            refill(l)
            keep_own(j, blocks(l + 2))
            refill(l + 2)
            chip_sum(1, b, j)
            return carry

        with jax.named_scope(f"d{b}"):
            lax.fori_loop(0, 5, step, 0)

    with jax.named_scope("gather00"):
        gather(0, 0)
    with jax.named_scope("norm00"):
        arrive(0, 0)
        add_branch(0, 0)
    gate_up(0)
    with jax.named_scope("gather01"):
        gather(0, 1)
    down(0)
    with jax.named_scope("norm01"):
        arrive(0, 1)
        add_branch(0, 1)
        yhcopies[1].start()
    gate_up(1)
    with jax.named_scope("gather10"):
        gather(1, 0)
    down(1)
    with jax.named_scope("arrive10"):
        arrive(1, 0)
        add_branch(1, 0)
        yhcopies[0].start()
    with jax.named_scope("gather11"):
        gather(1, 1)
    mcopies = [pltpu.make_async_copy(ref, m_hbm.at[pl.ds(half * 5, 5)], ysem.at[3 + i]) for i, (half, ref) in enumerate(((core, xs_recv.at[1, 1]), (1 - core, other.at[1])))]
    mcopies[0].start()
    with jax.named_scope("arrive11"):
        arrive(1, 1)
    mcopies[1].start()
    rcopy = pltpu.make_async_copy(rs_out.at[1, pl.ds(128, 128)], rs_hbm, ysem.at[2])
    rcopy.start()
    with jax.named_scope("tail"):
        for c in [vcopy, kcopy, rcopy] + yhcopies + mcopies:
            c.wait()


def finish_kernel(rs_hbm, gm_hbm, yh_hbm, m_hbm, k_in, v_in, y_hbm, k_out, v_out, rs, gm, yh, m, kb, vb, isem, msem, hsem, psem, osem, ysem):
    def chunk(c):
        cs = pl.ds(c * 512, 512)
        return [pltpu.make_async_copy(m_hbm.at[c], m.at[c], msem.at[c]), pltpu.make_async_copy(yh_hbm.at[pl.ds(128, 128), cs], yh.at[pl.ds(128, 128), cs], hsem.at[c])]

    top = pl.ds(0, 128)
    moves = ((yh_hbm.at[top], yh.at[top], y_hbm.at[top]), (k_in, kb, k_out), (v_in, vb, v_out))
    loads = [pltpu.make_async_copy(src, buf, psem.at[i]) for i, (src, buf, dst) in enumerate(moves)]
    out = [pltpu.make_async_copy(buf, dst, osem.at[i]) for i, (src, buf, dst) in enumerate(moves)]
    for d in loads:
        d.start()
    small = [pltpu.make_async_copy(src, dst, isem.at[i]) for i, (src, dst) in enumerate(((rs_hbm, rs), (gm_hbm, gm)))]
    for d in small:
        d.start()
    for c in range(10):
        for d in chunk(c):
            d.start()
    for i in range(3):
        loads[i].wait()
        out[i].start()
    for d in small:
        d.wait()
    for c in range(10):
        for d in chunk(c):
            d.wait()
        for w in range(4):
            rows, cs = pl.ds(128, 128), pl.ds(c * 512 + w * 128, 128)
            g = gm[c * 4 + w:c * 4 + w + 1, :].astype(F32)
            yh[rows, cs] = (yh[rows, cs].astype(F32) + m[c, :, pl.ds(w * 128, 128)].astype(F32) * rs[...] * g).astype(BF16)
        rows, cs = pl.ds(128, 128), pl.ds(c * 512, 512)
        ycopy = pltpu.make_async_copy(yh.at[rows, cs], y_hbm.at[rows, cs], ysem.at[c])
        ycopy.start()
        out.append(ycopy)
    for d in out:
        d.wait()


def solution(mesh):
    def local_layer(tokens, seq_lens, w_q, w_k, w_v, w_o, g_q, g_k, g_attn, g_mlp, w_gate, w_up, w_down):
        cos_tab, sin_tab = rope_tables(128)
        hbm = pl.BlockSpec(memory_space=pl.ANY)
        gain = lambda g: g.reshape(-1, 128)
        dma = pltpu.SemaphoreType.DMA
        cache = jax.ShapeDtypeStruct((2, 10, 128, 128), BF16)
        hidden = jax.ShapeDtypeStruct((256, 5120), BF16)
        yh, m, rs, kc, vc = pl.pallas_call(
            layer_kernel,
            out_shape=(hidden, jax.ShapeDtypeStruct((10, 128, 512), BF16), jax.ShapeDtypeStruct((128, 128), F32), cache, cache),
            in_specs=[pl.BlockSpec(memory_space=pltpu.SMEM)] + [hbm] * 14,
            out_specs=(hbm,) * 5,
            scratch_shapes=[
                pltpu.VMEM((RING + KEEP, 5120, 256), BF16),
                pltpu.VMEM((256, 5120), BF16),
                pltpu.VMEM((2, 20, 128, 128), F32),
                pltpu.VMEM((2, 10, 128, 128), BF16),
                pltpu.VMEM((2, 10, 128, 128), BF16),
                pltpu.VMEM((128, 3456), BF16),
                pltpu.VMEM((2, 256, 128), F32),
                pltpu.VMEM((8, 256), F32),
                pltpu.VMEM((3, 8, 256), F32),
                pltpu.VMEM((2, 5, 128, 512), BF16),
                pltpu.VMEM((2, 5, 128, 512), BF16),
                pltpu.VMEM((2, 2, 5, 128, 512), BF16),
                pltpu.VMEM((2, 5, 128, 512), BF16),
                pltpu.VMEM((2, 256, 128), F32),
                pltpu.VMEM((10, 128), BF16),
                pltpu.VMEM((10, 128), BF16),
                pltpu.VMEM((40, 128), BF16),
                pltpu.VMEM((40, 128), BF16),
                pltpu.VMEM((10, 128), F32),
                pltpu.VMEM((10, 128), F32),
                pltpu.VMEM((40, 128), F32),
                pltpu.VMEM((40, 128), F32),
                dma((RING + KEEP,)), dma((2,)), dma((2,)), dma((6,)), dma((3,)), dma((3,)), dma((2, 2, 6, 5)), dma((6,)),
            ],
            compiler_params=pltpu.CompilerParams(collective_id=0, has_side_effects=True, vmem_limit_bytes=67043328),
        )(seq_lens, jnp.asarray(cos_tab), jnp.asarray(sin_tab), gain(g_q), gain(g_k), gain(g_attn), gain(g_mlp),
          tokens.reshape(256, 5120), w_q, w_k, w_v, w_o, w_gate, w_up, w_down)
        y, kc, vc = pl.pallas_call(
            finish_kernel,
            out_shape=(hidden, cache, cache),
            in_specs=[hbm] * 6,
            out_specs=(hbm,) * 3,
            scratch_shapes=[
                pltpu.VMEM((128, 128), F32),
                pltpu.VMEM((40, 128), BF16),
                pltpu.VMEM((256, 5120), BF16),
                pltpu.VMEM((10, 128, 512), BF16),
                pltpu.VMEM((2, 10, 128, 128), BF16),
                pltpu.VMEM((2, 10, 128, 128), BF16),
                dma((2,)), dma((10,)), dma((10,)), dma((3,)), dma((3,)), dma((10,)),
            ],
            compiler_params=pltpu.CompilerParams(vmem_limit_bytes=60000000),
        )(rs, gain(g_mlp), yh, m, kc, vc)
        return y.reshape(2, 128, 5120), kc, vc

    return jax.shard_map(local_layer, mesh=mesh, in_specs=(P('dp', None, None), P('dp'), P(None, 'tp'), P(None, 'tp'), P(None, 'tp'), P('tp', None), P('tp'), P('tp'), P(), P(), P(None, 'tp'), P(None, 'tp'), P('tp', None)), out_specs=(P('dp', None, None), P('dp', 'tp', None, None), P('dp', 'tp', None, None)), check_vma=False)
```
